32 devices in a mesh: dp: 2 (over x), yax: 4 (over z), xax: 4 (over y, core).
Axes of the slice: x: 2, y: 2, z: 4, core: 2. Of those that a mesh axis runs over, the one named last changes fastest.
Arguments:
- hidden: bfloat16 [128, 2048], P('dp', 'xax'), parts along dimension 0
- cache_len: int32 [128], P('dp'), parts along dimension 0
- k_cache: bfloat16 [128, 8192, 256], P(('dp', 'yax', 'xax')), parts along dimension 0
- v_cache: bfloat16 [128, 8192, 256], P(('dp', 'yax', 'xax')), parts along dimension 0
- g_attn: float32 [2048], P('xax')
- w_query: bfloat16 [2048, 2048], P('xax', 'yax')
- w_key: bfloat16 [2048, 256], P('xax')
- w_value: bfloat16 [2048, 256], P('xax')
- w_gate: bfloat16 [2048, 8192], P('xax', 'yax')
- w_up: bfloat16 [2048, 8192], P('xax', 'yax')
- w_out: bfloat16 [2048, 2048], P('yax', 'xax')
- w_down: bfloat16 [8192, 2048], P('yax', 'xax')
- g_final: float32 [2048], P('xax')
- embedding: bfloat16 [50304, 2048], P('yax', 'xax')
Outputs:
- output 1: bfloat16 [128, 256], P(('dp', 'yax', 'xax')), parts along dimension 0
- output 2: bfloat16 [128, 256], P(('dp', 'yax', 'xax')), parts along dimension 0
- output 3: float32 [128, 50304], P('dp', ('yax', 'xax')), parts along dimension 0
- output 4: float32 [128], P('dp'), parts along dimension 0
There are 2 independent parts. The reference program is written for one: setup_inputs(seed, part) draws one part's arguments, and reference() takes and returns one part's arrays. A program takes and returns all parts, laid end to end along the dimension named above; an argument that names none is the same for every part.
All inputs are finite; a program needn't handle non-finite values.
Results may differ from the reference program's by a relative error of at most 0.001.
Values are sent between devices in bfloat16 or wider.
A program may use at most 1 GiB of HBM per device.

```python
import jax
import jax.numpy as jnp
from jax import lax

D = 2048
HEADS = 8
HEAD = 256
FF = 8192
VOCAB = 50304
BATCH = 64
SEQ = 8192
ROW_BLOCK = 16

EPS = 1e-6
ROPE_BASE = 10000.0


def draw_lengths(key):
    drawn = jax.random.randint(key, (BATCH,), 1, SEQ, dtype=jnp.int32)
    row_ids = jnp.arange(BATCH)
    return jnp.where(row_ids == 0, SEQ - 1, jnp.where(row_ids == 1, 1, drawn)).astype(jnp.int32)


def setup_inputs(seed: int = 0, part: int = 0) -> dict:
    base_key = jax.random.key(seed)
    shared = jax.random.split(base_key, 10)
    own = jax.random.split(jax.random.fold_in(base_key, part), 5)

    def weight(key, shape, fan_in, gain):
        return (gain * fan_in ** -0.5 * jax.random.normal(key, shape, jnp.float32)).astype(jnp.bfloat16)

    col_scale = jnp.exp(0.5 * jax.random.normal(own[0], (D,), jnp.float32))
    hidden = jax.random.normal(own[1], (BATCH, D), jnp.float32) * col_scale
    k_cache = 2.5 * jax.random.normal(own[3], (BATCH, SEQ, HEAD), jnp.float32)
    v_cache = 2.0 * jax.random.normal(own[4], (BATCH, SEQ, HEAD), jnp.float32)
    return {
        "hidden": hidden.astype(jnp.bfloat16),
        "cache_len": draw_lengths(own[2]),
        "k_cache": k_cache.astype(jnp.bfloat16),
        "v_cache": v_cache.astype(jnp.bfloat16),
        "g_attn": 1.0 + 0.3 * jax.random.normal(shared[0], (D,), jnp.float32),
        "w_query": weight(shared[1], (D, HEADS * HEAD), D, 1.0),
        "w_key": weight(shared[2], (D, HEAD), D, 1.0),
        "w_value": weight(shared[3], (D, HEAD), D, 1.0),
        "w_gate": weight(shared[4], (D, FF), D, 1.0),
        "w_up": weight(shared[5], (D, FF), D, 1.0),
        "w_out": weight(shared[6], (HEADS * HEAD, D), HEADS * HEAD, 1.0),
        "w_down": weight(shared[7], (FF, D), FF, 1.0),
        "g_final": 1.0 + 0.3 * jax.random.normal(shared[8], (D,), jnp.float32),
        "embedding": weight(shared[9], (VOCAB, D), D, 2.0),
    }


def layer_norm(values_in, gain):
    row_mean = jnp.mean(values_in, axis=-1, keepdims=True)
    row_var = jnp.mean(jnp.square(values_in - row_mean), axis=-1, keepdims=True)
    return (values_in - row_mean) * lax.rsqrt(row_var + EPS) * gain


def rope_angle(positions):
    half_dim = HEAD // 2
    inv_freq = ROPE_BASE ** (-(jnp.arange(half_dim, dtype=jnp.float32) * 2.0) / HEAD)
    return positions.astype(jnp.float32)[:, None] * inv_freq[None, :]


def rotary(values_in, angles):
    half_dim = values_in.shape[-1] // 2
    cos_a = jnp.cos(angles)
    sin_a = jnp.sin(angles)
    first = values_in[..., :half_dim]
    second = values_in[..., half_dim:]
    return jnp.concatenate([first * cos_a - second * sin_a, second * cos_a + first * sin_a], axis=-1)


def attend_block(block):
    q_blk, kc_blk, vc_blk, kn_blk, vn_blk, len_blk = block
    positions = jnp.arange(SEQ)
    at_slot = positions[None, :, None] == len_blk[:, None, None]
    keys_all = jnp.where(at_slot, kn_blk[:, None, :], kc_blk)
    values_all = jnp.where(at_slot, vn_blk[:, None, :], vc_blk)
    scores = jnp.einsum("rhe,rse->rhs", q_blk.astype(jnp.float32), keys_all.astype(jnp.float32)) * HEAD ** -0.5
    valid = positions[None, None, :] <= len_blk[:, None, None]
    scores = jnp.where(valid, scores, -jnp.inf)
    prob_all = jax.nn.softmax(scores, axis=-1).astype(jnp.bfloat16)
    mixed = jnp.einsum("rhs,rse->rhe", prob_all.astype(jnp.float32), values_all.astype(jnp.float32))
    return mixed.astype(jnp.bfloat16)


def reference(hidden, cache_len, k_cache, v_cache, g_attn, w_query, w_key, w_value,
              w_gate, w_up, w_out, w_down, g_final, embedding):
    residual = hidden.astype(jnp.float32)
    normed = layer_norm(residual, g_attn).astype(jnp.bfloat16)
    query = jnp.dot(normed, w_query, preferred_element_type=jnp.float32).astype(jnp.bfloat16)
    key_new = jnp.dot(normed, w_key, preferred_element_type=jnp.float32).astype(jnp.bfloat16)
    value_new = jnp.dot(normed, w_value, preferred_element_type=jnp.float32).astype(jnp.bfloat16)
    gate = jnp.dot(normed, w_gate, preferred_element_type=jnp.float32).astype(jnp.bfloat16)
    up_val = jnp.dot(normed, w_up, preferred_element_type=jnp.float32).astype(jnp.bfloat16)
    angles = rope_angle(cache_len)
    query = rotary(query.astype(jnp.float32).reshape(BATCH, HEADS, HEAD), angles[:, None, :]).astype(jnp.bfloat16)
    key_new = rotary(key_new.astype(jnp.float32), angles).astype(jnp.bfloat16)
    blocks = BATCH // ROW_BLOCK
    attn_out = lax.map(attend_block, (
        query.reshape(blocks, ROW_BLOCK, HEADS, HEAD),
        k_cache.reshape(blocks, ROW_BLOCK, SEQ, HEAD),
        v_cache.reshape(blocks, ROW_BLOCK, SEQ, HEAD),
        key_new.reshape(blocks, ROW_BLOCK, HEAD),
        value_new.reshape(blocks, ROW_BLOCK, HEAD),
        cache_len.reshape(blocks, ROW_BLOCK)))
    attn_out = attn_out.reshape(BATCH, HEADS * HEAD)
    mlp_act = (jax.nn.silu(gate.astype(jnp.float32)) * up_val.astype(jnp.float32)).astype(jnp.bfloat16)
    branch_sum = (jnp.dot(attn_out, w_out, preferred_element_type=jnp.float32)
                  + jnp.dot(mlp_act, w_down, preferred_element_type=jnp.float32))
    residual_out = residual + branch_sum
    final_norm = layer_norm(residual_out, g_final).astype(jnp.bfloat16)
    logits = jnp.dot(final_norm, embedding.T, preferred_element_type=jnp.float32)
    log_norm = jax.nn.logsumexp(logits, axis=-1)
    return key_new, value_new, logits - log_norm[:, None], log_norm
```

```python
import functools

import jax
import jax.numpy as jnp
from jax import lax
from jax.experimental import pallas as pl
from jax.experimental.pallas import tpu as pltpu
from jax.sharding import PartitionSpec as P

EPS = 1e-6
ROPE_BASE = 10000.0
F32 = jnp.float32
BF16 = jnp.bfloat16
MESH = pl.DeviceIdType.MESH


def rope_angle(positions, head_dim):
    half_dim = head_dim // 2
    inv_freq = ROPE_BASE ** (-(jnp.arange(half_dim, dtype=jnp.float32) * 2.0) / head_dim)
    return positions.astype(jnp.float32)[:, None] * inv_freq[None, :]


def dot(a, b):
    return jnp.dot(a, b, preferred_element_type=F32)


def dot_t(a, b):
    return lax.dot_general(a, b, (((1,), (1,)), ((), ())), preferred_element_type=F32)


def one_hot_rows(rows, cols, source):
    r = lax.broadcasted_iota(jnp.int32, (rows, cols), 0)
    c = lax.broadcasted_iota(jnp.int32, (rows, cols), 1)
    return jnp.where(c == source(r), 1.0, 0.0).astype(BF16)


def step_kernel(sizes,
                lens, hidden_hbm, table_hbm, k_hbm, v_hbm, ga_hbm, wq_hbm, wk_hbm, wv_hbm, wg_hbm, wu_hbm,
                wo_hbm, wd_hbm, gf_hbm, emb_hbm,
                kn_out, vn_out, z_out, ln_out,
                hid, table, ga, gf, kbuf, vbuf, wq, wkv, wg, wu, wo, wd,
                st_send, st_recv, qkv, qkv_recv, q_send, q_recv, qs, kns, vns, os_, o_send, o_recv,
                gup, gu_recv, gux, gux_recv, m_all, mdown, bpart, b_recv, s2_send, s2_recv, fbuf,
                lsend1, lrecv1, hold, xrecv, lsend2, lrecv2, own, l_send, l_recv,
                ld_sem, kv_sem, e_sem, send_sem, st_sem, qkv_sem, q_sem, gu_sem, gux_sem, m_sem, o_sem,
                b_sem, s2_sem, f_sem, l1_sem, lx_sem, l2_sem, lse_sem):
    rows, wid, seq, hd, ffc, vb, chunks = sizes
    yi = lax.axis_index("yax")
    xi = lax.axis_index("xax")
    x1 = xi + 1 - 2 * (xi % 2)
    x2 = (xi + 2) % 4
    x3 = (x1 + 2) % 4
    me = yi * 4 + xi
    ypeers = [(yi + d) % 4 for d in (1, 2, 3)]
    xpeers = [x1, x2, x3]

    loads = {}

    def load(name, i, src, dst):
        loads[name] = pltpu.make_async_copy(src, dst, ld_sem.at[i])
        loads[name].start()

    load("hid", 0, hidden_hbm, hid)
    load("ga", 1, ga_hbm, ga)
    load("table", 2, table_hbm, table)
    load("wq", 3, wq_hbm, wq)
    load("wk", 4, wk_hbm, wkv.at[0])
    load("wv", 5, wv_hbm, wkv.at[1])
    n_id = 6
    for i, xx in enumerate((x1, x3, x2, xi)):
        cols = pl.ds(pl.multiple_of(xx * ffc, ffc), ffc)
        load(f"wg{i}", n_id, wg_hbm.at[:, cols], wg.at[xx])
        load(f"wu{i}", n_id + 1, wu_hbm.at[:, cols], wu.at[xx])
        n_id += 2
    barrier = pltpu.get_barrier_semaphore()
    for dy in range(4):
        for dx in range(4):
            if dy or dx:
                pl.semaphore_signal(barrier, inc=1,
                                    device_id={"yax": (yi + dy) % 4, "xax": (xi + dx) % 4}, device_id_type=MESH)
    for j in range(4):
        pltpu.make_async_copy(k_hbm.at[j], kbuf.at[j], kv_sem.at[j]).start()
        pltpu.make_async_copy(v_hbm.at[j], vbuf.at[j], kv_sem.at[4 + j]).start()
    load("wd", n_id, wd_hbm, wd)
    load("wo", n_id + 1, wo_hbm, wo)
    load("gf", n_id + 2, gf_hbm, gf)

    sends = []

    def send(src, dst, rsem, yy, xx):
        cp = pltpu.make_async_remote_copy(src_ref=src, dst_ref=dst, send_sem=send_sem.at[len(sends)], recv_sem=rsem,
                                          device_id={"yax": yy, "xax": xx}, device_id_type=MESH)
        cp.start()
        sends.append(cp)

    def recv(dst, rsem):
        pltpu.make_async_copy(dst, dst, rsem).wait()

    loads["hid"].wait()
    loads["ga"].wait()
    h = hid[...].astype(F32)
    mean_l = jnp.sum(h, axis=1, keepdims=True) * (1.0 / wid)
    dev = h - mean_l
    m2_l = jnp.sum(dev * dev, axis=1, keepdims=True)
    lane = lax.broadcasted_iota(jnp.int32, (rows, 128), 1)
    stat = jnp.where(lane == 0, mean_l, m2_l)
    stat_t = jnp.concatenate([stat, stat], axis=0).T[:8]
    st_send[...] = stat_t
    pl.semaphore_wait(barrier, 15)
    for xx in xpeers:
        send(st_send, st_recv.at[xi], st_sem.at[xi], yi, xx)
    perm = one_hot_rows(96, 64, lambda r: jnp.where(
        r % 24 < 16, ((r % 24) // 4) * 16 + (r // 24) * 4 + r % 4,
        jnp.where(r % 24 < 20, yi * 16 + (r // 24) * 4 + r % 4, -1)))
    for xx in xpeers:
        recv(st_recv.at[xx], st_sem.at[xx])
    parts = [stat_t] + [st_recv[xx] for xx in xpeers]
    means = [p[0:1] for p in parts]
    mu = (means[0] + means[1] + means[2] + means[3]) * 0.25
    m2 = sum([p[1:2] for p in parts]) + wid * sum([(m - mu) * (m - mu) for m in means])
    rstd = lax.rsqrt(m2 * (1.0 / (4 * wid)) + EPS)
    sub = lax.broadcasted_iota(jnp.int32, (128, 128), 0)
    cols_t = jnp.where(sub == 0, mu, rstd).T
    mu_c = cols_t[:rows, 0:1]
    rstd_c = cols_t[:rows, 1:2]
    normed = ((h - mu_c) * rstd_c * ga[...]).astype(BF16)
    n_perm = dot(perm, normed).astype(BF16)

    loads["wq"].wait()
    loads["wk"].wait()
    loads["wv"].wait()
    q_part = dot(n_perm, wq[...])
    kv_part = jnp.concatenate([dot(n_perm, wkv[0]), dot(n_perm, wkv[1])], axis=1)
    prow = lax.broadcasted_iota(jnp.int32, (96, 2 * hd), 0)
    qkv[...] = jnp.where(prow % 24 < 16, q_part, kv_part).reshape(4, 24, 2 * hd)
    for xx in (x2, x3, x1):
        send(qkv.at[xx], qkv_recv.at[xi], qkv_sem.at[xi], yi, xx)

    for i, xx in enumerate((x1, x3, x2, xi)):
        loads[f"wg{i}"].wait()
        loads[f"wu{i}"].wait()
        gup[xx, 0] = dot(normed, wg[xx])
        gup[xx, 1] = dot(normed, wu[xx])
        if i < 2:
            send(gup.at[xx], gu_recv.at[i], gu_sem.at[i], yi, x1)

    loads["table"].wait()
    for xx in (x1, x2, x3):
        recv(qkv_recv.at[xx], qkv_sem.at[xx])
    tot = ((qkv[xi] + qkv_recv[x1]) + (qkv_recv[x2] + qkv_recv[x3])).astype(BF16).astype(F32)
    half = hd // 2
    cos_a = table[:, :half]
    sin_a = table[:, half:]
    lo0, hi0, lo1, hi1 = [tot[:, i * half:(i + 1) * half] for i in range(4)]
    r0 = (lo0 * cos_a - hi0 * sin_a).astype(BF16)
    r1 = (hi0 * cos_a + lo0 * sin_a).astype(BF16)
    r2 = (lo1 * cos_a - hi1 * sin_a).astype(BF16)
    r3 = (hi1 * cos_a + lo1 * sin_a).astype(BF16)
    kns[:, :half] = r0[16:].astype(F32)
    kns[:, half:] = r1[16:].astype(F32)
    vns[...] = tot[16:, hd:]
    stacked = jnp.concatenate([r0[:16], r1[:16], r2[:16], r3[:16]], axis=0)
    s1 = one_hot_rows(64, 64, lambda r: ((r // 4) % 4) * 16 + (r // 16) * 4 + r % 4)
    q_send[...] = dot(s1, stacked).astype(BF16).reshape(4, 16, 128)
    for yy in ypeers:
        send(q_send.at[yy], q_recv.at[yi], q_sem.at[yi], yy, xi)
    q_recv[yi] = q_send[yi]
    kn_out[...] = kns[...].astype(BF16)[:4]
    vn_out[...] = vns[...].astype(BF16)[:4]

    recv(gu_recv.at[1], gu_sem.at[1])
    gux[...] = gup[x2] + gu_recv[1]
    send(gux, gux_recv, gux_sem, yi, x2)
    recv(gu_recv.at[0], gu_sem.at[0])

    for yy in ypeers:
        recv(q_recv.at[yy], q_sem.at[yy])
    s2 = one_hot_rows(64, 64, lambda r: ((r // 2) % 4) * 16 + (r % 2) * 8 + (r // 32) * 4 + (r // 8) % 4)
    q_all = dot(s2, q_recv[...].reshape(64, 128))
    qs[...] = jnp.concatenate([q_all[:32], q_all[32:]], axis=1).reshape(4, 8, hd)

    scale = hd ** -0.5
    pos = lax.broadcasted_iota(jnp.int32, (8, seq), 1)

    def attend(j, carry):
        qj = qs[j]
        length = lens[me * 4 + j]
        pltpu.make_async_copy(k_hbm.at[j], kbuf.at[j], kv_sem.at[j]).wait()
        s = dot_t(qj.astype(BF16), kbuf[j]) * scale
        s_new = jnp.sum(qj * kns[pl.ds(j, 1), :], axis=1, keepdims=True) * scale
        s = jnp.where(pos < length, s, -jnp.inf)
        top = jnp.maximum(jnp.max(s, axis=1, keepdims=True), s_new)
        w = jnp.exp(s - top)
        w_new = jnp.exp(s_new - top)
        inv = 1.0 / (jnp.sum(w, axis=1, keepdims=True) + w_new)
        prob = (w * inv).astype(BF16)
        p_new = (w_new * inv).astype(BF16).astype(F32)
        pltpu.make_async_copy(v_hbm.at[j], vbuf.at[j], kv_sem.at[4 + j]).wait()
        os_[j] = dot(prob, vbuf[j]) + p_new * vns[pl.ds(j, 1), :]
        voc = pl.ds(pl.multiple_of(j * vb, 8), vb)
        pltpu.make_async_copy(emb_hbm.at[voc, pl.ds(0, hd)], kbuf.at[j, pl.ds(0, vb)], e_sem.at[j]).start()
        pltpu.make_async_copy(emb_hbm.at[voc, pl.ds(hd, hd)], vbuf.at[j, pl.ds(0, vb)], e_sem.at[4 + j]).start()
        return carry

    lax.fori_loop(0, 2, attend, 0)
    recv(gux_recv, gux_sem)
    gu = gup[xi] + gu_recv[0] + gux_recv[...]
    gate = gu[0].astype(BF16).astype(F32)
    up_val = gu[1].astype(BF16).astype(F32)
    m_all[xi] = (gate * jax.nn.sigmoid(gate) * up_val).astype(BF16)
    for xx in (x2, x3, x1):
        send(m_all.at[xi], m_all.at[xi], m_sem.at[xi], yi, xx)
    lax.fori_loop(2, 4, attend, 0)

    o_bf = os_[...].reshape(32, hd).astype(BF16)
    s3 = one_hot_rows(64, 64, lambda r: ((r // 4) % 2) * 32 + (r % 4) * 8 + (r // 16) * 2 + (r // 8) % 2)
    o_send[...] = dot(s3, jnp.concatenate([o_bf[:, :half], o_bf[:, half:]], axis=0)).astype(BF16).reshape(4, 16, 128)
    for yy in ypeers:
        for xx in (x3, x2, x1, xi):
            send(o_send.at[yy], o_recv.at[me], o_sem.at[me], yy, xx)
    for xx in xpeers:
        send(o_send.at[yi], o_recv.at[me], o_sem.at[me], yi, xx)
    o_recv[me] = o_send[yi]

    loads["wd"].wait()
    loads["wo"].wait()
    loads["gf"].wait()
    for xx in xpeers:
        recv(m_all.at[xx], m_sem.at[xx])
    mdown[...] = sum([dot(m_all[i], wd[pl.ds(i * ffc, ffc)]) for i in range(4)])
    s4 = one_hot_rows(256, 256, lambda r: ((r % 64) // 4) * 16 + (r // 64) * 4 + r % 4)
    for xx in xpeers:
        recv(o_recv.at[yi * 4 + xx], o_sem.at[yi * 4 + xx])
    for yy in ypeers:
        for xx in (xi, x1, x2, x3):
            recv(o_recv.at[yy * 4 + xx], o_sem.at[yy * 4 + xx])
    a_all = dot(s4, o_recv[...].reshape(256, 128)).astype(BF16)
    attn = jnp.concatenate([a_all[i * 64:(i + 1) * 64] for i in range(4)], axis=1)
    bpart[...] = (dot(attn, wo[...]) + mdown[...]).reshape(4, 16, wid)
    for yy in (ypeers[1], ypeers[0], ypeers[2]):
        send(bpart.at[yy], b_recv.at[yi], b_sem.at[yi], yy, xi)
    res = hid[pl.ds(pl.multiple_of(yi * 16, 16), 16), :].astype(F32)
    for yy in ypeers:
        recv(b_recv.at[yy], b_sem.at[yy])
    res = res + ((bpart[yi] + b_recv[ypeers[0]]) + (b_recv[ypeers[1]] + b_recv[ypeers[2]]))

    mean_l = jnp.sum(res, axis=1, keepdims=True) * (1.0 / wid)
    dev = res - mean_l
    m2_l = jnp.sum(dev * dev, axis=1, keepdims=True)
    lane = lax.broadcasted_iota(jnp.int32, (16, 128), 1)
    s2_send[...] = jnp.where(lane < 64, mean_l, m2_l)
    for xx in xpeers:
        send(s2_send, s2_recv.at[xi], s2_sem.at[xi], yi, xx)
    for xx in xpeers:
        recv(s2_recv.at[xx], s2_sem.at[xx])
    parts = [s2_recv[xx] for xx in xpeers]
    means = [mean_l] + [p[:, 0:1] for p in parts]
    mu = (means[0] + means[1] + means[2] + means[3]) * 0.25
    m2 = m2_l + sum([p[:, 64:65] for p in parts]) + wid * sum([(m - mu) * (m - mu) for m in means])
    rstd = lax.rsqrt(m2 * (1.0 / (4 * wid)) + EPS)
    fbuf[yi] = ((res - mu) * rstd * gf[...]).astype(BF16)
    for yy in ypeers:
        send(fbuf.at[yi], fbuf.at[yi], f_sem.at[yi], yy, xi)
    for j in range(4):
        pltpu.make_async_copy(emb_hbm.at[pl.ds(0, vb), pl.ds(0, hd)], kbuf.at[j, pl.ds(0, vb)], e_sem.at[j]).wait()
        pltpu.make_async_copy(emb_hbm.at[pl.ds(0, vb), pl.ds(0, hd)], vbuf.at[j, pl.ds(0, vb)], e_sem.at[4 + j]).wait()
    for yy in ypeers:
        recv(fbuf.at[yy], f_sem.at[yy])
    f = fbuf[...].reshape(rows, wid)
    f0 = f[:, :hd]
    f1 = f[:, hd:]

    def logit_part(xx, c0, cn):
        voc = pl.ds(c0, cn)
        return dot_t(f0, kbuf[xx, voc]) + dot_t(f1, vbuf[xx, voc])

    def cross(i):
        c0, cn = chunks[i]
        cs = pl.ds(c0, cn)
        recv(lrecv1.at[:, cs], l1_sem.at[i])
        hold[:, cs] = hold[:, cs] + lrecv1[:, cs]
        send(hold.at[:, cs], xrecv.at[:, cs], lx_sem.at[i], yi, x2)

    for i, (c0, cn) in enumerate(chunks):
        cs = pl.ds(c0, cn)
        lsend1[:, cs] = logit_part(x3, c0, cn)
        send(lsend1.at[:, cs], lrecv1.at[:, cs], l1_sem.at[i], yi, x1)
        hold[:, cs] = logit_part(x2, c0, cn)
        if i >= 1:
            cross(i - 1)
    cross(len(chunks) - 1)
    for i, (c0, cn) in enumerate(chunks):
        cs = pl.ds(c0, cn)
        lsend2[:, cs] = logit_part(x1, c0, cn)
        send(lsend2.at[:, cs], lrecv2.at[:, cs], l2_sem.at[i], yi, x1)
        own[:, cs] = logit_part(xi, c0, cn)
    m_run = jnp.full((rows, 1), -jnp.inf, F32)
    s_run = jnp.zeros((rows, 1), F32)
    for i, (c0, cn) in enumerate(chunks):
        cs = pl.ds(c0, cn)
        recv(lrecv2.at[:, cs], l2_sem.at[i])
        recv(xrecv.at[:, cs], lx_sem.at[i])
        z = own[:, cs] + lrecv2[:, cs] + xrecv[:, cs]
        if c0 + cn > vb:
            z_out[:, c0:vb] = z[:, :vb - c0]
            z = jnp.where(lax.broadcasted_iota(jnp.int32, (rows, cn), 1) < vb - c0, z, -jnp.inf)
        else:
            z_out[:, cs] = z
        m_new = jnp.maximum(m_run, jnp.max(z, axis=1, keepdims=True))
        s_run = s_run * jnp.exp(m_run - m_new) + jnp.sum(jnp.exp(z - m_new), axis=1, keepdims=True)
        m_run = m_new

    lane = lax.broadcasted_iota(jnp.int32, (rows, 128), 1)
    stat = jnp.where(lane == 0, m_run, s_run)
    mine = jnp.concatenate([stat, stat], axis=0).T[0:2]
    l_send[...] = mine
    for yy in ypeers:
        for xx in (x3, x2, x1, xi):
            send(l_send, l_recv.at[me], lse_sem.at[me], yy, xx)
    for xx in xpeers:
        send(l_send, l_recv.at[me], lse_sem.at[me], yi, xx)
    l_recv[me] = mine
    for xx in xpeers:
        recv(l_recv.at[yi * 4 + xx], lse_sem.at[yi * 4 + xx])
    for yy in ypeers:
        for xx in (xi, x1, x2, x3):
            recv(l_recv.at[yy * 4 + xx], lse_sem.at[yy * 4 + xx])
    tops = [l_recv[i, 0:1, :] for i in range(16)]
    top = functools.reduce(jnp.maximum, tops)
    total = sum([l_recv[i, 1:2, :] * jnp.exp(tops[i] - top) for i in range(16)])
    log_norm = top + jnp.log(total)
    ln_out[...] = jnp.broadcast_to(log_norm, (128, 128)).T[:rows, 0:1]
    for cp in sends:
        cp.wait_send()


def solution(mesh):
    row_spec = P(("dp", "yax", "xax"))

    def local_step(hidden, cache_len, k_cache, v_cache, g_attn, w_query, w_key, w_value,
                   w_gate, w_up, w_out, w_down, g_final, embedding):
        rows, wid = hidden.shape
        own_rows, seq, hd = k_cache.shape
        ffc = w_gate.shape[1] // 4
        vb = embedding.shape[0] // 4
        y_idx = lax.axis_index("yax")
        x_idx = lax.axis_index("xax")
        lens3 = cache_len.reshape(4, 4, 4)
        lens_x = lax.dynamic_index_in_dim(lens3, x_idx, axis=1, keepdims=False)
        lens_me = lax.dynamic_index_in_dim(lens_x, y_idx, axis=0, keepdims=False)
        angles = rope_angle(jnp.concatenate([lens_x.reshape(16), lens_me, lens_me]), hd)
        table = jnp.concatenate([jnp.cos(angles), jnp.sin(angles)], axis=1)
        vbp = -(-vb // 128) * 128
        chunks = [(c, min(512, vbp - c)) for c in range(0, vbp, 512)]
        nch = len(chunks)
        sizes = (rows, wid, seq, hd, ffc, vb, chunks)
        any_spec = pl.BlockSpec(memory_space=pl.ANY)
        vmem = pl.BlockSpec(memory_space=pltpu.VMEM)
        v = pltpu.VMEM
        dma = pltpu.SemaphoreType.DMA
        scratch = [
            v((rows, wid), BF16), v((24, hd), F32), v((1, wid), F32), v((1, wid), F32),
            v((4, seq, hd), BF16), v((4, seq, hd), BF16),
            v((wid, 2 * hd), BF16), v((2, wid, hd), BF16), v((4, wid, ffc), BF16), v((4, wid, ffc), BF16),
            v((2 * hd, wid), BF16), v((4 * ffc, wid), BF16),
            v((8, 128), F32), v((4, 8, 128), F32), v((4, 24, 2 * hd), F32), v((4, 24, 2 * hd), F32),
            v((4, 16, 128), BF16), v((4, 16, 128), BF16), v((4, 8, hd), F32), v((8, hd), F32), v((8, hd), F32),
            v((4, 8, hd), F32), v((4, 16, 128), BF16), v((16, 16, 128), BF16),
            v((4, 2, rows, ffc), F32), v((2, 2, rows, ffc), F32), v((2, rows, ffc), F32), v((2, rows, ffc), F32),
            v((4, rows, ffc), BF16), v((rows, wid), F32), v((4, 16, wid), F32), v((4, 16, wid), F32),
            v((16, 128), F32), v((4, 16, 128), F32), v((4, 16, wid), BF16),
            v((rows, vbp), F32), v((rows, vbp), F32), v((rows, vbp), F32), v((rows, vbp), F32),
            v((rows, vbp), F32), v((rows, vbp), F32), v((rows, vbp), F32),
            v((2, 128), F32), v((16, 2, 128), F32),
            dma((20,)), dma((8,)), dma((8,)), dma((100,)), dma((4,)), dma((4,)), dma((4,)), dma((2,)), dma(()),
            dma((4,)), dma((16,)), dma((4,)), dma((4,)), dma((4,)), dma((nch,)), dma((nch,)), dma((nch,)), dma((16,)),
        ]
        k_new, v_new, z, ln = pl.pallas_call(
            functools.partial(step_kernel, sizes),
            name="decode_step",
            out_shape=(jax.ShapeDtypeStruct((own_rows, hd), BF16), jax.ShapeDtypeStruct((own_rows, hd), BF16),
                       jax.ShapeDtypeStruct((rows, vb), F32), jax.ShapeDtypeStruct((rows, 1), F32)),
            in_specs=[pl.BlockSpec(memory_space=pltpu.SMEM)] + [any_spec] * 14,
            out_specs=(vmem, vmem, vmem, vmem),
            scratch_shapes=scratch,
            compiler_params=pltpu.CompilerParams(collective_id=0, has_side_effects=True,
                                                 vmem_limit_bytes=60 * 1024 * 1024),
        )(cache_len, hidden, table, k_cache, v_cache, g_attn.reshape(1, wid), w_query, w_key, w_value,
          w_gate, w_up, w_out, w_down, g_final.reshape(1, wid), embedding)
        return k_new, v_new, z - ln, ln[:, 0]

    in_specs = (P("dp", "xax"), P("dp"), row_spec, row_spec, P("xax"), P("xax", "yax"),
                P("xax", None), P("xax", None), P("xax", "yax"), P("xax", "yax"),
                P("yax", "xax"), P("yax", "xax"), P("xax"), P("yax", "xax"))
    out_specs = (row_spec, row_spec, P("dp", ("yax", "xax")), P("dp"))
    return jax.shard_map(local_step, mesh=mesh, in_specs=in_specs, out_specs=out_specs, check_vma=False)
```

```python
import functools

import jax
import jax.numpy as jnp
from jax import lax
from jax.experimental import pallas as pl
from jax.experimental.pallas import tpu as pltpu
from jax.sharding import PartitionSpec as P

EPS = 1e-6
ROPE_BASE = 10000.0
F32 = jnp.float32
BF16 = jnp.bfloat16
MESH = pl.DeviceIdType.MESH


def dot(a, b):
    return jnp.dot(a, b, preferred_element_type=F32)


def dot_t(a, b):
    return lax.dot_general(a, b, (((1,), (1,)), ((), ())), preferred_element_type=F32)


def one_hot_rows(rows, cols, source):
    r = lax.broadcasted_iota(jnp.int32, (rows, cols), 0)
    c = lax.broadcasted_iota(jnp.int32, (rows, cols), 1)
    return jnp.where(c == source(r), 1.0, 0.0).astype(BF16)


def step_kernel(sizes,
                lens, hidden_hbm, freq_hbm, k_hbm, v_hbm, ga_hbm, wq_hbm, wk_hbm, wv_hbm, wg_hbm, wu_hbm,
                wo_hbm, wd_hbm, gf_hbm, emb_hbm,
                kv_out, z_out, ln_out, lr_out,
                hid, freq, table, ga, gf, kbuf, vbuf, wq, wkv, wgu, wo, wd,
                st_send, st_recv, qkv, qkv_recv, q_send, q_recv, qs, kns, vns, os_, sbuf, o_send, o_recv,
                gup, gu_recv, gux, gux_recv, m_all, mdown, bpart, b_recv, s2_send, s2_recv, fbuf,
                lsend1, lrecv1, hold, xrecv, lsend2, lrecv2, own, lcol, l_send, l_recv,
                ld_sem, snd_sem, rcv_sem, l1_sem, lx_sem, l2_sem):
    rows, wid, seq, hd, ffc, vb, chunks_a, chunks_b, chunks_c = sizes
    yi = lax.axis_index("yax")
    xi = lax.axis_index("xax")
    x1 = xi + 1 - 2 * (xi % 2)
    x2 = (xi + 2) % 4
    x3 = (x1 + 2) % 4
    me = yi * 4 + xi
    ypeers = [(yi + d) % 4 for d in (1, 2, 3)]
    xpeers = [x1, x2, x3]

    def load(i, *pairs):
        for src, dst in pairs:
            pltpu.make_async_copy(src, dst, ld_sem.at[i]).start()

    def loaded(i, dst):
        pltpu.make_async_copy(dst, dst, ld_sem.at[i]).wait()

    HID, GA, FREQ, WQ, WKV, WGU, WD, WO, GF, KEY, VAL, EK, EV = 0, 1, 2, 3, 4, 5, 9, 10, 11, 12, 13, 14, 15
    load(HID, (hidden_hbm, hid))
    load(GA, (ga_hbm, ga))
    barrier = pltpu.get_barrier_semaphore()
    for dy in range(4):
        for dx in range(4):
            if dy or dx:
                pl.semaphore_signal(barrier, inc=1,
                                    device_id={"yax": (yi + dy) % 4, "xax": (xi + dx) % 4}, device_id_type=MESH)
    load(FREQ, (freq_hbm, freq))
    load(WQ, (wq_hbm, wq))
    load(WKV, (wk_hbm, wkv.at[0]), (wv_hbm, wkv.at[1]))
    for i, xx in enumerate((x1, x3, x2, xi)):
        cols = pl.ds(pl.multiple_of(xx * ffc, ffc), ffc)
        load(WGU + i, (wg_hbm.at[:, cols], wgu.at[xx, 0]), (wu_hbm.at[:, cols], wgu.at[xx, 1]))
    load(KEY, *[(k_hbm.at[j], kbuf.at[j]) for j in range(4)])
    load(VAL, *[(v_hbm.at[j], vbuf.at[j]) for j in range(4)])
    load(WD, (wd_hbm, wd))
    load(WO, (wo_hbm, wo))
    load(GF, (gf_hbm, gf))

    ST, QKV, Q, GU, GUX, M, O, B, S2, FN, LSE, L1, LX, L2 = range(14)

    def send(src, dst, i, yy, xx, rsem=None):
        pltpu.make_async_remote_copy(src_ref=src, dst_ref=dst, send_sem=snd_sem.at[i],
                                     recv_sem=rcv_sem.at[i] if rsem is None else rsem,
                                     device_id={"yax": yy, "xax": xx}, device_id_type=MESH).start()

    def recv(dst, i):
        pltpu.make_async_copy(dst, dst, rcv_sem.at[i]).wait()

    def recv_chunk(dst, sem):
        pltpu.make_async_copy(dst, dst, sem).wait()

    def sent(src, i):
        pltpu.make_async_copy(src, src, snd_sem.at[i]).wait()

    three = pl.ds(0, 3)
    most = pl.ds(0, 15)

    loaded(HID, hid)
    loaded(GA, ga)
    h = hid[...].astype(F32)
    mean_l = jnp.sum(h, axis=1, keepdims=True) * (1.0 / wid)
    dev = h - mean_l
    m2_l = jnp.sum(dev * dev, axis=1, keepdims=True)
    lane = lax.broadcasted_iota(jnp.int32, (rows, 128), 1)
    stat = jnp.where(lane == 0, mean_l, m2_l)
    stat_t = jnp.concatenate([stat, stat], axis=0).T[:8]
    st_send[...] = stat_t
    pl.semaphore_wait(barrier, 15)
    for xx in xpeers:
        send(st_send, st_recv.at[xi], ST, yi, xx)
    perm = one_hot_rows(96, 64, lambda r: jnp.where(
        r % 24 < 16, ((r % 24) // 4) * 16 + (r // 24) * 4 + r % 4,
        jnp.where(r % 24 < 20, yi * 16 + (r // 24) * 4 + r % 4, -1)))
    loaded(FREQ, freq)
    prow = lax.broadcasted_iota(jnp.int32, (24, 128), 0)
    posn = jnp.zeros((24, 128), jnp.int32)
    for r in range(20):
        at = (r // 4) * 16 + xi * 4 + r % 4 if r < 16 else me * 4 + r - 16
        posn = jnp.where(prow == r, lens[at], posn)
    angle = posn.astype(F32) * freq[...]
    table[0] = jnp.cos(angle)
    table[1] = jnp.sin(angle)
    recv(st_recv.at[three], ST)
    parts = [stat_t] + [st_recv[xx] for xx in xpeers]
    means = [p[0:1] for p in parts]
    mu = (means[0] + means[1] + means[2] + means[3]) * 0.25
    m2 = sum([p[1:2] for p in parts]) + wid * sum([(m - mu) * (m - mu) for m in means])
    rstd = lax.rsqrt(m2 * (1.0 / (4 * wid)) + EPS)
    sub = lax.broadcasted_iota(jnp.int32, (128, 128), 0)
    cols_t = jnp.where(sub == 0, mu, rstd).T
    mu_c = cols_t[:rows, 0:1]
    rstd_c = cols_t[:rows, 1:2]
    normed = ((h - mu_c) * rstd_c * ga[...]).astype(BF16)
    n_perm = dot(perm, normed).astype(BF16)

    loaded(WQ, wq)
    loaded(WKV, wkv)
    q_part = dot(n_perm, wq[...])
    kv_part = jnp.concatenate([dot(n_perm, wkv[0]), dot(n_perm, wkv[1])], axis=1)
    prow = lax.broadcasted_iota(jnp.int32, (96, 2 * hd), 0)
    qkv[...] = jnp.where(prow % 24 < 16, q_part, kv_part).reshape(4, 24, 2 * hd)
    for xx in (x2, x3, x1):
        send(qkv.at[xx], qkv_recv.at[xi], QKV, yi, xx)

    for i, xx in enumerate((x1, x3, x2, xi)):
        loaded(WGU + i, wgu.at[xx])
        gup[xx, 0] = dot(normed, wgu[xx, 0])
        gup[xx, 1] = dot(normed, wgu[xx, 1])
        if i < 2:
            send(gup.at[xx], gu_recv.at[i], GU, yi, x1)

    recv(qkv_recv.at[three], QKV)
    tot = ((qkv[xi] + qkv_recv[x1]) + (qkv_recv[x2] + qkv_recv[x3])).astype(BF16).astype(F32)
    half = hd // 2
    cos_a = table[0]
    sin_a = table[1]
    lo0, hi0, lo1, hi1 = [tot[:, i * half:(i + 1) * half] for i in range(4)]
    r0 = (lo0 * cos_a - hi0 * sin_a).astype(BF16)
    r1 = (hi0 * cos_a + lo0 * sin_a).astype(BF16)
    r2 = (lo1 * cos_a - hi1 * sin_a).astype(BF16)
    r3 = (hi1 * cos_a + lo1 * sin_a).astype(BF16)
    kns[:, :half] = r0[16:].astype(F32)
    kns[:, half:] = r1[16:].astype(F32)
    vns[...] = tot[16:, hd:]
    stacked = jnp.concatenate([r0[:16], r1[:16], r2[:16], r3[:16]], axis=0)
    s1 = one_hot_rows(64, 64, lambda r: ((r // 4) % 4) * 16 + (r // 16) * 4 + r % 4)
    q_send[...] = dot(s1, stacked).astype(BF16).reshape(4, 16, 128)
    for yy in ypeers:
        send(q_send.at[yy], q_recv.at[yi], Q, yy, xi)
    q_recv[yi] = q_send[yi]
    kv_out[0] = kns[...]
    kv_out[1] = vns[...]

    recv(gu_recv, GU)
    gux[...] = gup[x2] + gu_recv[1]
    send(gux, gux_recv, GUX, yi, x2)
    recv(q_recv.at[three], Q)
    s2 = one_hot_rows(64, 64, lambda r: ((r // 2) % 4) * 16 + (r % 2) * 8 + (r // 32) * 4 + (r // 8) % 4)
    q_all = dot(s2, q_recv[...].reshape(64, 128))
    qs[...] = jnp.concatenate([q_all[:32], q_all[32:]], axis=1).reshape(4, 8, hd)

    loaded(KEY, kbuf)
    loaded(VAL, vbuf)
    scale = hd ** -0.5
    pos = lax.broadcasted_iota(jnp.int32, (8, seq), 1)

    def scores(j):
        qj = qs[j].astype(BF16)
        for t in range(seq // 256):
            at = pl.ds(t * 256, 256)
            sbuf[j % 2, :, at] = dot_t(qj, kbuf[j, at])

    def mix(j):
        s_new = jnp.sum(qs[j] * kns[j:j + 1, :], axis=1, keepdims=True) * scale
        s = jnp.where(pos < lens[me * 4 + j], sbuf[j % 2] * scale, -jnp.inf)
        top = jnp.maximum(jnp.max(s, axis=1, keepdims=True), s_new)
        w = jnp.exp(s - top)
        w_new = jnp.exp(s_new - top)
        inv = 1.0 / (jnp.sum(w, axis=1, keepdims=True) + w_new)
        prob = (w * inv).astype(BF16)
        p_new = (w_new * inv).astype(BF16).astype(F32)
        os_[j] = dot(prob, vbuf[j]) + p_new * vns[j:j + 1, :]

    def load_embedding(j):
        voc = pl.ds(j * vb, vb)
        load(EK, (emb_hbm.at[voc, pl.ds(0, hd)], kbuf.at[j, pl.ds(0, vb)]))
        load(EV, (emb_hbm.at[voc, pl.ds(hd, hd)], vbuf.at[j, pl.ds(0, vb)]))

    scores(0)
    scores(1)
    mix(0)
    load_embedding(0)
    scores(2)
    mix(1)
    load_embedding(1)
    recv(gux_recv, GUX)
    gu = gup[xi] + gu_recv[0] + gux_recv[...]
    gate = gu[0].astype(BF16).astype(F32)
    up_val = gu[1].astype(BF16).astype(F32)
    m_all[xi] = (gate * jax.nn.sigmoid(gate) * up_val).astype(BF16)
    for xx in (x2, x3, x1):
        send(m_all.at[xi], m_all.at[xi], M, yi, xx)
    scores(3)
    mix(2)
    load_embedding(2)
    mix(3)
    load_embedding(3)

    o_bf = os_[...].reshape(32, hd).astype(BF16)
    s3 = one_hot_rows(64, 64, lambda r: ((r // 4) % 2) * 32 + (r % 4) * 8 + (r // 16) * 2 + (r // 8) % 2)
    o_send[...] = dot(s3, jnp.concatenate([o_bf[:, :half], o_bf[:, half:]], axis=0)).astype(BF16).reshape(4, 16, 128)
    for yy in ypeers:
        for xx in (x3, x2, x1, xi):
            send(o_send.at[yy], o_recv.at[me], O, yy, xx)
    for xx in xpeers:
        send(o_send.at[yi], o_recv.at[me], O, yi, xx)
    o_recv[me] = o_send[yi]

    loaded(WD, wd)
    loaded(WO, wo)
    loaded(GF, gf)
    recv(m_all.at[three], M)
    mdown[...] = sum([dot(m_all[i], wd[pl.ds(i * ffc, ffc)]) for i in range(4)])
    s4 = one_hot_rows(256, 256, lambda r: ((r % 64) // 4) * 16 + (r // 64) * 4 + r % 4)
    recv(o_recv.at[most], O)
    a_all = dot(s4, o_recv[...].reshape(256, 128)).astype(BF16)
    attn = jnp.concatenate([a_all[i * 64:(i + 1) * 64] for i in range(4)], axis=1)
    bpart[...] = (dot(attn, wo[...]) + mdown[...]).reshape(4, 16, wid)
    for yy in (ypeers[1], ypeers[0], ypeers[2]):
        send(bpart.at[yy], b_recv.at[yi], B, yy, xi)
    res = hid[pl.ds(pl.multiple_of(yi * 16, 16), 16), :].astype(F32)
    recv(b_recv.at[three], B)
    res = res + ((bpart[yi] + b_recv[ypeers[0]]) + (b_recv[ypeers[1]] + b_recv[ypeers[2]]))

    mean_l = jnp.sum(res, axis=1, keepdims=True) * (1.0 / wid)
    dev = res - mean_l
    m2_l = jnp.sum(dev * dev, axis=1, keepdims=True)
    lane = lax.broadcasted_iota(jnp.int32, (16, 128), 1)
    s2_send[...] = jnp.where(lane < 64, mean_l, m2_l)
    for xx in xpeers:
        send(s2_send, s2_recv.at[xi], S2, yi, xx)
    recv(s2_recv.at[three], S2)
    parts = [s2_recv[xx] for xx in xpeers]
    means = [mean_l] + [p[:, 0:1] for p in parts]
    mu = (means[0] + means[1] + means[2] + means[3]) * 0.25
    m2 = m2_l + sum([p[:, 64:65] for p in parts]) + wid * sum([(m - mu) * (m - mu) for m in means])
    rstd = lax.rsqrt(m2 * (1.0 / (4 * wid)) + EPS)
    f_own = ((res - mu) * rstd * gf[...]).astype(BF16)
    fbuf[yi] = f_own
    for yy in ypeers:
        send(fbuf.at[yi], fbuf.at[yi], FN, yy, xi)
    loaded(EK, kbuf.at[:, pl.ds(0, vb)])
    loaded(EV, vbuf.at[:, pl.ds(0, vb)])

    def logit_part(f, xx, c0, cn):
        voc = pl.ds(c0, cn)
        return dot_t(f[:, :hd], kbuf[xx, voc]) + dot_t(f[:, hd:], vbuf[xx, voc])

    def cross(i, at):
        recv_chunk(lrecv1.at[at], l1_sem.at[i])
        hold[at] = hold[at] + lrecv1[at]
        send(hold.at[at], xrecv.at[at], LX, yi, x2, lx_sem.at[i])

    def cross_blocks(f, slots, chunks, first):
        n = f.shape[0] // 16
        prev = None
        for i, (c0, cn) in enumerate(chunks):
            at = (slots, slice(None), pl.ds(c0, cn))
            lsend1[at] = logit_part(f, x3, c0, cn).reshape(n, 16, cn)
            send(lsend1.at[at], lrecv1.at[at], L1, yi, x1, l1_sem.at[first + i])
            hold[at] = logit_part(f, x2, c0, cn).reshape(n, 16, cn)
            if prev is not None:
                cross(*prev)
            prev = (first + i, at)
        cross(*prev)

    slot_a = pl.ds(0, 1)
    slot_b = pl.ds(1, 3)
    na = len(chunks_a)
    cross_blocks(f_own, slot_a, chunks_a, 0)
    recv(fbuf.at[three], FN)
    f_rest = jnp.concatenate([fbuf[yy] for yy in ypeers], axis=0)
    cross_blocks(f_rest, slot_b, chunks_b, na)
    f_all = jnp.concatenate([f_own, f_rest], axis=0)
    for i, (c0, cn) in enumerate(chunks_c):
        at = (slice(None), slice(None), pl.ds(c0, cn))
        lsend2[at] = logit_part(f_all, x1, c0, cn).reshape(4, 16, cn)
        send(lsend2.at[at], lrecv2.at[at], L2, yi, x1, l2_sem.at[i])
        own[at] = logit_part(f_all, xi, c0, cn).reshape(4, 16, cn)
    recv_chunk(lrecv2, l2_sem.at[0]) if len(chunks_c) == 1 else [
        recv_chunk(lrecv2.at[:, :, pl.ds(c0, cn)], l2_sem.at[i]) for i, (c0, cn) in enumerate(chunks_c)]
    tops, totals = {}, {}
    for d in range(4):
        tops[d] = jnp.full((16, 1), -jnp.inf, F32)
        totals[d] = jnp.zeros((16, 1), F32)
    for chunks, slots, ds, first in ((chunks_a, slot_a, (0,), 0), (chunks_b, slot_b, (1, 2, 3), na)):
        for i, (c0, cn) in enumerate(chunks):
            recv_chunk(xrecv.at[slots, :, pl.ds(c0, cn)], lx_sem.at[first + i])
            cs = pl.ds(c0, cn)
            for d in ds:
                row = pl.ds(pl.multiple_of(((yi + d) % 4) * 16, 16), 16)
                z = own[d, :, cs] + lrecv2[d, :, cs] + xrecv[d, :, cs]
                if c0 + cn > vb:
                    z_out[row, c0:vb] = z[:, :vb - c0]
                    z = jnp.where(lax.broadcasted_iota(jnp.int32, (16, cn), 1) < vb - c0, z, -jnp.inf)
                else:
                    z_out[row, cs] = z
                m_new = jnp.maximum(tops[d], jnp.max(z, axis=1, keepdims=True))
                totals[d] = totals[d] * jnp.exp(tops[d] - m_new) + jnp.sum(jnp.exp(z - m_new), axis=1, keepdims=True)
                tops[d] = m_new
    lane = lax.broadcasted_iota(jnp.int32, (16, 128), 1)
    for d in range(4):
        lcol[(yi + d) % 4] = jnp.where(lane == 0, tops[d], totals[d])

    stat = lcol[...].reshape(rows, 128)
    mine = jnp.concatenate([stat, stat], axis=0).T[0:2]
    l_send[...] = mine
    for yy in ypeers:
        for xx in (x3, x2, x1, xi):
            send(l_send, l_recv.at[me], LSE, yy, xx)
    for xx in xpeers:
        send(l_send, l_recv.at[me], LSE, yi, xx)
    l_recv[me] = mine
    sent(st_recv.at[three], ST)
    sent(qkv.at[three], QKV)
    sent(q_send.at[three], Q)
    sent(gu_recv, GU)
    sent(gux, GUX)
    sent(m_all.at[three], M)
    sent(o_recv.at[most], O)
    sent(bpart.at[three], B)
    sent(s2_recv.at[three], S2)
    sent(fbuf.at[three], FN)
    sent(lsend1, L1)
    sent(hold, LX)
    sent(lsend2, L2)
    recv(l_recv.at[most], LSE)
    tops = [l_recv[i, 0:1, :] for i in range(16)]
    top = functools.reduce(jnp.maximum, tops)
    total = sum([l_recv[i, 1:2, :] * jnp.exp(tops[i] - top) for i in range(16)])
    log_norm = top + jnp.log(total)
    lr_out[...] = log_norm[:, :rows]
    ln_out[...] = jnp.broadcast_to(log_norm, (128, 128)).T[:rows, 0:1]
    sent(l_recv.at[most], LSE)


def finish_kernel(own_rows, kv, z, ln, lr, k_out, v_out, lp_out, ln_out, k_s, v_s, lp_s, sem):
    k_s[...] = kv[0].astype(BF16)[:own_rows]
    v_s[...] = kv[1].astype(BF16)[:own_rows]
    copies = [pltpu.make_async_copy(k_s, k_out, sem.at[0]), pltpu.make_async_copy(v_s, v_out, sem.at[1]),
              pltpu.make_async_copy(lr, ln_out, sem.at[2])]
    for cp in copies:
        cp.start()
    for i in range(z.shape[0] // 8):
        at = pl.ds(i * 8, 8)
        lp_s[at] = z[at] - ln[at]
        copies.append(pltpu.make_async_copy(lp_s.at[at], lp_out.at[at], sem.at[3 + i]))
        copies[-1].start()
    for cp in copies:
        cp.wait()


def solution(mesh):
    row_spec = P(("dp", "yax", "xax"))

    def local_step(hidden, cache_len, k_cache, v_cache, g_attn, w_query, w_key, w_value,
                   w_gate, w_up, w_out, w_down, g_final, embedding):
        rows, wid = hidden.shape
        own_rows, seq, hd = k_cache.shape
        ffc = w_gate.shape[1] // 4
        vb = embedding.shape[0] // 4
        half_dim = hd // 2
        inv_freq = ROPE_BASE ** (-(jnp.arange(half_dim, dtype=jnp.float32) * 2.0) / hd)
        vbp = -(-vb // 128) * 128
        def cut(step):
            return [(c, min(step, vbp - c)) for c in range(0, vbp, step)]

        chunks_a, chunks_b, chunks_c = cut(1024), cut(512), cut(1024)
        nx, nc = len(chunks_a) + len(chunks_b), len(chunks_c)
        sizes = (rows, wid, seq, hd, ffc, vb, chunks_a, chunks_b, chunks_c)
        any_spec = pl.BlockSpec(memory_space=pltpu.HBM)
        vmem = pl.BlockSpec(memory_space=pltpu.VMEM)
        v = pltpu.VMEM
        dma = pltpu.SemaphoreType.DMA
        scratch = [
            v((rows, wid), BF16), v((1, hd // 2), F32), v((2, 24, hd // 2), F32), v((1, wid), F32), v((1, wid), F32),
            v((4, seq, hd), BF16), v((4, seq, hd), BF16),
            v((wid, 2 * hd), BF16), v((2, wid, hd), BF16), v((4, 2, wid, ffc), BF16),
            v((2 * hd, wid), BF16), v((4 * ffc, wid), BF16),
            v((8, 128), F32), v((4, 8, 128), F32), v((4, 24, 2 * hd), F32), v((4, 24, 2 * hd), F32),
            v((4, 16, 128), BF16), v((4, 16, 128), BF16), v((4, 8, hd), F32), v((8, hd), F32), v((8, hd), F32),
            v((4, 8, hd), F32), v((2, 8, seq), F32), v((4, 16, 128), BF16), v((16, 16, 128), BF16),
            v((4, 2, rows, ffc), F32), v((2, 2, rows, ffc), F32), v((2, rows, ffc), F32), v((2, rows, ffc), F32),
            v((4, rows, ffc), BF16), v((rows, wid), F32), v((4, 16, wid), F32), v((4, 16, wid), F32),
            v((16, 128), F32), v((4, 16, 128), F32), v((4, 16, wid), BF16),
            v((4, 16, vbp), F32), v((4, 16, vbp), F32), v((4, 16, vbp), F32), v((4, 16, vbp), F32),
            v((4, 16, vbp), F32), v((4, 16, vbp), F32), v((4, 16, vbp), F32), v((4, 16, 128), F32),
            v((2, 128), F32), v((16, 2, 128), F32),
            dma((16,)), dma((14,)), dma((11,)), dma((nx,)), dma((nx,)), dma((nc,)),
        ]
        kv, z, ln, lr = pl.pallas_call(
            functools.partial(step_kernel, sizes),
            name="decode_step",
            out_shape=(v((2, 8, hd), F32), v((rows, vb), F32), v((rows, 1), F32), v((1, rows), F32)),
            in_specs=[pl.BlockSpec(memory_space=pltpu.SMEM)] + [any_spec] * 14,
            out_specs=(vmem, vmem, vmem, vmem),
            scratch_shapes=scratch,
            compiler_params=pltpu.CompilerParams(collective_id=0, has_side_effects=True,
                                                 vmem_limit_bytes=67043328 - 900 * 1024),
        )(cache_len, hidden, inv_freq.reshape(1, half_dim), k_cache, v_cache, g_attn.reshape(1, wid), w_query, w_key, w_value,
          w_gate, w_up, w_out, w_down, g_final.reshape(1, wid), embedding)
        k_new, v_new, log_probs, log_norm = pl.pallas_call(
            functools.partial(finish_kernel, own_rows),
            name="finish_step",
            out_shape=(jax.ShapeDtypeStruct((own_rows, hd), BF16), jax.ShapeDtypeStruct((own_rows, hd), BF16),
                       jax.ShapeDtypeStruct((rows, vb), F32), jax.ShapeDtypeStruct((1, rows), F32)),
            in_specs=[vmem] * 4,
            out_specs=(any_spec,) * 4,
            scratch_shapes=[v((own_rows, hd), BF16), v((own_rows, hd), BF16), v((rows, vb), F32), dma((11,))],
            compiler_params=pltpu.CompilerParams(vmem_limit_bytes=4 * 1024 * 1024),
        )(kv, z, ln, lr)
        return k_new, v_new, log_probs, log_norm[0]

    in_specs = (P("dp", "xax"), P("dp"), row_spec, row_spec, P("xax"), P("xax", "yax"),
                P("xax", None), P("xax", None), P("xax", "yax"), P("xax", "yax"),
                P("yax", "xax"), P("yax", "xax"), P("xax"), P("yax", "xax"))
    out_specs = (row_spec, row_spec, P("dp", ("yax", "xax")), P("dp"))
    return jax.shard_map(local_step, mesh=mesh, in_specs=in_specs, out_specs=out_specs, check_vma=False)
```

```python
import functools

import jax
import jax.numpy as jnp
import numpy as np
from jax import lax
from jax.experimental import pallas as pl
from jax.experimental.pallas import tpu as pltpu
from jax.sharding import PartitionSpec as P

EPS = 1e-6
ROPE_BASE = 10000.0
F32 = jnp.float32
BF16 = jnp.bfloat16
MESH = pl.DeviceIdType.MESH


def dot(a, b):
    return jnp.dot(a, b, preferred_element_type=F32)


def dot_t(a, b):
    return lax.dot_general(a, b, (((1,), (1,)), ((), ())), preferred_element_type=F32)


def one_hot_rows(rows, cols, source):
    r = lax.broadcasted_iota(jnp.int32, (rows, cols), 0)
    c = lax.broadcasted_iota(jnp.int32, (rows, cols), 1)
    return jnp.where(c == source(r), 1.0, 0.0).astype(BF16)


def step_kernel(sizes,
                lens, hidden_hbm, freq_hbm, k_hbm, v_hbm, ga_hbm, wq_hbm, wk_hbm, wv_hbm, wg_hbm, wu_hbm,
                wo_hbm, wd_hbm, gf_hbm, emb_hbm,
                kv_out, z_out, ln_out, lr_out,
                hid, freq, table, ga, gf, kb0, kb1, kb2, kb3, kb4, vbuf, wq, wkv, wgu, wo, wd,
                st_send, st_recv, qkv, qkv_recv, q_send, q_recv, qs, kns, vns, os_, sbuf, o_send, o_recv,
                gup, gu_recv, gux, gux_recv, m_all, mdown, bpart, b_recv, s2_send, s2_recv, fbuf,
                lsend1, lrecv1, hold, xrecv, lsend2, lrecv2, own, lcol, l_send, l_recv,
                ld_sem, snd_sem, rcv_sem, l1_sem, lx_sem, l2_sem):
    rows, wid, seq, hd, ffc, vb, chunks_a, chunks_b, chunks_c = sizes
    yi = lax.axis_index("yax")
    xi = lax.axis_index("xax")
    x1 = xi + 1 - 2 * (xi % 2)
    x2 = (xi + 2) % 4
    x3 = (x1 + 2) % 4
    me = yi * 4 + xi
    ypeers = [(yi + d) % 4 for d in (1, 2, 3)]
    xpeers = [x1, x2, x3]

    def load(i, *pairs):
        for src, dst in pairs:
            pltpu.make_async_copy(src, dst, ld_sem.at[i]).start()

    def loaded(i, dst):
        pltpu.make_async_copy(dst, dst, ld_sem.at[i]).wait()

    HID, GA, FREQ, WQ, WKV, WGU, WD, WO, GF, KEY, VAL, EMB = 0, 1, 2, 3, 4, 5, 9, 10, 11, 12, 16, 20
    kb = (kb0, kb1, kb2, kb3, kb4)
    load(HID, (hidden_hbm, hid))
    load(GA, (ga_hbm, ga))
    barrier = pltpu.get_barrier_semaphore()
    for dy in range(4):
        for dx in range(4):
            if dy or dx:
                pl.semaphore_signal(barrier, inc=1,
                                    device_id={"yax": (yi + dy) % 4, "xax": (xi + dx) % 4}, device_id_type=MESH)
    load(FREQ, (freq_hbm, freq))
    load(WQ, (wq_hbm, wq))
    load(WKV, (wk_hbm, wkv.at[0]), (wv_hbm, wkv.at[1]))
    load(KEY, (k_hbm.at[0], kb[1]))
    for i, xx in enumerate((x1, x3, x2, xi)):
        cols = pl.ds(pl.multiple_of(xx * ffc, ffc), ffc)
        load(WGU + i, (wg_hbm.at[:, cols], wgu.at[xx, 0]), (wu_hbm.at[:, cols], wgu.at[xx, 1]))
    for j in range(1, 4):
        load(KEY + j, (k_hbm.at[j], kb[j + 1]))
    for j in range(4):
        load(VAL + j, (v_hbm.at[j], vbuf.at[j]))
    load(WD, (wd_hbm, wd))
    load(WO, (wo_hbm, wo))
    load(GF, (gf_hbm, gf))

    ST, QP, KVP, Q, GU, GUX, M, O1, O2, B, S2, FN, LSE, L1, LX, L2 = range(16)

    def send(src, dst, i, yy, xx, rsem=None):
        pltpu.make_async_remote_copy(src_ref=src, dst_ref=dst, send_sem=snd_sem.at[i],
                                     recv_sem=rcv_sem.at[i] if rsem is None else rsem,
                                     device_id={"yax": yy, "xax": xx}, device_id_type=MESH).start()

    def recv(dst, i):
        pltpu.make_async_copy(dst, dst, rcv_sem.at[i]).wait()

    def recv_chunk(dst, sem):
        pltpu.make_async_copy(dst, dst, sem).wait()

    def sent(src, i):
        pltpu.make_async_copy(src, src, snd_sem.at[i]).wait()

    three = pl.ds(0, 3)
    most = pl.ds(0, 15)

    def transpose_keys(j):
        loaded(KEY + j, kb[j + 1])

        def one(t, carry):
            at = pl.ds(pl.multiple_of(t * 256, 256), 256)
            kb[j][at] = kb[j + 1][at].T
            return carry

        lax.fori_loop(0, seq // 256, one, 0, unroll=8)

    loaded(HID, hid)
    loaded(GA, ga)
    h = hid[...].astype(F32)
    mean_l = jnp.sum(h, axis=1, keepdims=True) * (1.0 / wid)
    dev = h - mean_l
    m2_l = jnp.sum(dev * dev, axis=1, keepdims=True)
    lane = lax.broadcasted_iota(jnp.int32, (rows, 128), 1)
    stat = jnp.where(lane == 0, mean_l, m2_l)
    stat_t = jnp.concatenate([stat, stat], axis=0).T[:8]
    st_send[...] = stat_t
    pl.semaphore_wait(barrier, 15)
    for xx in xpeers:
        send(st_send, st_recv.at[xi], ST, yi, xx)
    perm = one_hot_rows(96, 64, lambda r: jnp.where(
        r % 24 < 16, ((r % 24) // 4) * 16 + (r // 24) * 4 + r % 4,
        jnp.where(r % 24 < 20, yi * 16 + (r // 24) * 4 + r % 4, -1)))
    loaded(FREQ, freq)
    prow = lax.broadcasted_iota(jnp.int32, (24, 128), 0)
    posn = jnp.zeros((24, 128), jnp.int32)
    for r in range(20):
        at = (r // 4) * 16 + xi * 4 + r % 4 if r < 16 else me * 4 + r - 16
        posn = jnp.where(prow == r, lens[at], posn)
    angle = posn.astype(F32) * freq[...]
    table[0] = jnp.cos(angle)
    table[1] = jnp.sin(angle)
    transpose_keys(0)
    recv(st_recv.at[three], ST)
    parts = [stat_t] + [st_recv[xx] for xx in xpeers]
    means = [p[0:1] for p in parts]
    mu = (means[0] + means[1] + means[2] + means[3]) * 0.25
    m2 = sum([p[1:2] for p in parts]) + wid * sum([(m - mu) * (m - mu) for m in means])
    rstd = lax.rsqrt(m2 * (1.0 / (4 * wid)) + EPS)
    sub = lax.broadcasted_iota(jnp.int32, (128, 128), 0)
    cols_t = jnp.where(sub == 0, mu, rstd).T
    mu_c = cols_t[:rows, 0:1]
    rstd_c = cols_t[:rows, 1:2]
    normed = ((h - mu_c) * rstd_c * ga[...]).astype(BF16)
    n_perm = dot(perm, normed).astype(BF16)

    loaded(WQ, wq)
    loaded(WKV, wkv)
    q_part = dot(n_perm, wq[...])
    kv_part = jnp.concatenate([dot(n_perm, wkv[0]), dot(n_perm, wkv[1])], axis=1)
    prow = lax.broadcasted_iota(jnp.int32, (96, 2 * hd), 0)
    qkv[...] = jnp.where(prow % 24 < 16, q_part, kv_part).reshape(4, 24, 2 * hd)
    q_rows, kv_rows = pl.ds(0, 16), pl.ds(16, 8)
    for xx in (x2, x3, x1):
        send(qkv.at[xx, q_rows], qkv_recv.at[xi, q_rows], QP, yi, xx)
    for xx in (x2, x3, x1):
        send(qkv.at[xx, kv_rows], qkv_recv.at[xi, kv_rows], KVP, yi, xx)

    for i, xx in enumerate((x1, x3, x2, xi)):
        loaded(WGU + i, wgu.at[xx])
        gup[xx, 0] = dot(normed, wgu[xx, 0])
        gup[xx, 1] = dot(normed, wgu[xx, 1])
        if i < 2:
            send(gup.at[xx], gu_recv.at[i], GU, yi, x1)

    transpose_keys(1)
    transpose_keys(2)
    half = hd // 2
    recv(qkv_recv.at[three, q_rows], QP)

    def total(at):
        return ((qkv[xi, at] + qkv_recv[x1, at]) + (qkv_recv[x2, at] + qkv_recv[x3, at])).astype(BF16).astype(F32)

    def rotary(lo, hi, at):
        cos_a, sin_a = table[0, at], table[1, at]
        return (lo * cos_a - hi * sin_a).astype(BF16), (hi * cos_a + lo * sin_a).astype(BF16)

    tot = total(q_rows)
    lo0, hi0, lo1, hi1 = [tot[:, i * half:(i + 1) * half] for i in range(4)]
    r0, r1 = rotary(lo0, hi0, q_rows)
    r2, r3 = rotary(lo1, hi1, q_rows)
    stacked = jnp.concatenate([r0, r1, r2, r3], axis=0)
    s1 = one_hot_rows(64, 64, lambda r: ((r // 4) % 4) * 16 + (r // 16) * 4 + r % 4)
    q_send[...] = dot(s1, stacked).astype(BF16).reshape(4, 16, 128)
    for yy in ypeers:
        send(q_send.at[yy], q_recv.at[yi], Q, yy, xi)
    q_recv[yi] = q_send[yi]
    recv(qkv_recv.at[three, kv_rows], KVP)
    tot = total(kv_rows)
    r0, r1 = rotary(tot[:, :half], tot[:, half:hd], kv_rows)
    kns[:, :half] = r0.astype(F32)
    kns[:, half:] = r1.astype(F32)
    vns[...] = tot[:, hd:]
    kv_out[0] = kns[...]
    kv_out[1] = vns[...]

    recv(gu_recv, GU)
    gux[...] = gup[x2] + gu_recv[1]
    send(gux, gux_recv, GUX, yi, x2)
    transpose_keys(3)
    recv(q_recv.at[three], Q)
    s2 = one_hot_rows(64, 64, lambda r: ((r // 2) % 4) * 16 + (r % 2) * 8 + (r // 32) * 4 + (r // 8) % 4)
    q_all = dot(s2, q_recv[...].reshape(64, 128))
    qs[...] = jnp.concatenate([q_all[:32], q_all[32:]], axis=1).reshape(4, 8, hd)

    for j in range(4):
        loaded(VAL + j, vbuf.at[j])
    scale = hd ** -0.5
    pos = lax.broadcasted_iota(jnp.int32, (8, seq), 1)

    def scores(j):
        qj = qs[j].astype(BF16)
        for t in range(seq // 256):
            at = pl.ds(t * 256, 256)
            sbuf[j % 2, :, at] = dot(qj, kb[j][at])

    def mix(j):
        s_new = jnp.sum(qs[j] * kns[j:j + 1, :], axis=1, keepdims=True) * scale
        s = jnp.where(pos < lens[me * 4 + j], sbuf[j % 2] * scale, -jnp.inf)
        top = jnp.maximum(jnp.max(s, axis=1, keepdims=True), s_new)
        w = jnp.exp(s - top)
        w_new = jnp.exp(s_new - top)
        inv = 1.0 / (jnp.sum(w, axis=1, keepdims=True) + w_new)
        prob = (w * inv).astype(BF16)
        p_new = (w_new * inv).astype(BF16).astype(F32)
        hs = seq // 2
        acc = dot(prob[:, :hs], vbuf[j, :hs]) + dot(prob[:, hs:], vbuf[j, hs:])
        os_[j] = acc + p_new * vns[j:j + 1, :]

    s3 = one_hot_rows(32, 32, lambda r: ((r // 2) % 2) * 16 + (r % 2) * 8 + (r // 8) * 2 + (r // 4) % 2)

    def send_outputs(pair, i):
        o_bf = os_[2 * pair:2 * pair + 2].reshape(16, hd).astype(BF16)
        o_rows = dot(s3, jnp.concatenate([o_bf[:, :half], o_bf[:, half:]], axis=0))
        o_send[pair] = o_rows.reshape(4, 8, 128).astype(BF16)
        for yy in ypeers:
            for xx in (x3, x2, x1, xi):
                send(o_send.at[pair, yy], o_recv.at[pair, me], i, yy, xx)
        for xx in xpeers:
            send(o_send.at[pair, yi], o_recv.at[pair, me], i, yi, xx)
        o_recv[pair, me] = o_send[pair, yi]

    scores(0)
    scores(1)
    mix(0)
    scores(2)
    mix(1)
    scores(3)
    mix(2)
    recv(gux_recv, GUX)
    gu = gup[xi] + gu_recv[0] + gux_recv[...]
    gate = gu[0].astype(BF16).astype(F32)
    up_val = gu[1].astype(BF16).astype(F32)
    m_all[xi] = (gate * jax.nn.sigmoid(gate) * up_val).astype(BF16)
    for xx in (x2, x3, x1):
        send(m_all.at[xi], m_all.at[xi], M, yi, xx)
    send_outputs(0, O1)
    mix(3)
    send_outputs(1, O2)
    for j in range(4):
        voc = pl.ds(j * vb, vb)
        load(EMB, (emb_hbm.at[voc, pl.ds(0, hd)], vbuf.at[j, pl.ds(0, vb)]),
             (emb_hbm.at[voc, pl.ds(hd, hd)], vbuf.at[j, pl.ds(seq // 2, vb)]))
    loaded(WD, wd)
    loaded(WO, wo)
    loaded(GF, gf)
    recv(m_all.at[three], M)
    mdown[...] = sum([dot(m_all[i], wd[pl.ds(i * ffc, ffc)]) for i in range(4)])
    s4 = one_hot_rows(256, 256, lambda r: ((r // 2) % 2) * 128 + ((r % 64) // 4) * 8 + (r // 64) * 2 + r % 2)
    recv(o_recv.at[0, most], O1)
    recv(o_recv.at[1, most], O2)
    o_rows = jnp.concatenate([o_recv[pair, i].astype(F32) for pair in range(2) for i in range(16)], axis=0)
    a_all = dot(s4, o_rows.astype(BF16)).astype(BF16)
    attn = jnp.concatenate([a_all[i * 64:(i + 1) * 64] for i in range(4)], axis=1)
    bpart[...] = (dot(attn, wo[...]) + mdown[...]).reshape(4, 16, wid)
    for yy in (ypeers[1], ypeers[0], ypeers[2]):
        send(bpart.at[yy], b_recv.at[yi], B, yy, xi)
    res = hid[pl.ds(pl.multiple_of(yi * 16, 16), 16), :].astype(F32)
    recv(b_recv.at[three], B)
    res = res + ((bpart[yi] + b_recv[ypeers[0]]) + (b_recv[ypeers[1]] + b_recv[ypeers[2]]))

    mean_l = jnp.sum(res, axis=1, keepdims=True) * (1.0 / wid)
    dev = res - mean_l
    m2_l = jnp.sum(dev * dev, axis=1, keepdims=True)
    lane = lax.broadcasted_iota(jnp.int32, (16, 128), 1)
    s2_send[...] = jnp.where(lane < 64, mean_l, m2_l)
    for xx in xpeers:
        send(s2_send, s2_recv.at[xi], S2, yi, xx)
    recv(s2_recv.at[three], S2)
    parts = [s2_recv[xx] for xx in xpeers]
    means = [mean_l] + [p[:, 0:1] for p in parts]
    mu = (means[0] + means[1] + means[2] + means[3]) * 0.25
    m2 = m2_l + sum([p[:, 64:65] for p in parts]) + wid * sum([(m - mu) * (m - mu) for m in means])
    rstd = lax.rsqrt(m2 * (1.0 / (4 * wid)) + EPS)
    f_own = ((res - mu) * rstd * gf[...]).astype(BF16)
    fbuf[yi] = f_own
    for yy in ypeers:
        send(fbuf.at[yi], fbuf.at[yi], FN, yy, xi)
    loaded(EMB, vbuf.at[:, pl.ds(0, 2 * vb)])

    def logit_part(f, xx, c0, cn):
        return dot_t(f[:, :hd], vbuf[xx, pl.ds(c0, cn)]) + dot_t(f[:, hd:], vbuf[xx, pl.ds(seq // 2 + c0, cn)])

    def cross(i, at):
        recv_chunk(lrecv1.at[at], l1_sem.at[i])
        hold[at] = hold[at] + lrecv1[at]
        send(hold.at[at], xrecv.at[at], LX, yi, x2, lx_sem.at[i])

    def cross_blocks(f, slots, chunks, first):
        n = f.shape[0] // 16
        prev = None
        for i, (c0, cn) in enumerate(chunks):
            at = (slots, slice(None), pl.ds(c0, cn))
            lsend1[at] = logit_part(f, x3, c0, cn).reshape(n, 16, cn)
            send(lsend1.at[at], lrecv1.at[at], L1, yi, x1, l1_sem.at[first + i])
            hold[at] = logit_part(f, x2, c0, cn).reshape(n, 16, cn)
            if prev is not None:
                cross(*prev)
            prev = (first + i, at)
        cross(*prev)

    slot_a = pl.ds(0, 1)
    slot_b = pl.ds(1, 3)
    na = len(chunks_a)
    cross_blocks(f_own, slot_a, chunks_a, 0)
    recv(fbuf.at[three], FN)
    f_rest = jnp.concatenate([fbuf[yy] for yy in ypeers], axis=0)
    cross_blocks(f_rest, slot_b, chunks_b, na)
    f_all = jnp.concatenate([f_own, f_rest], axis=0)
    for i, (c0, cn) in enumerate(chunks_c):
        at = (slice(None), slice(None), pl.ds(c0, cn))
        lsend2[at] = logit_part(f_all, x1, c0, cn).reshape(4, 16, cn)
        send(lsend2.at[at], lrecv2.at[at], L2, yi, x1, l2_sem.at[i])
        own[at] = logit_part(f_all, xi, c0, cn).reshape(4, 16, cn)
    recv_chunk(lrecv2, l2_sem.at[0]) if len(chunks_c) == 1 else [
        recv_chunk(lrecv2.at[:, :, pl.ds(c0, cn)], l2_sem.at[i]) for i, (c0, cn) in enumerate(chunks_c)]
    tops, totals = {}, {}
    for d in range(4):
        tops[d] = jnp.full((16, 1), -jnp.inf, F32)
        totals[d] = jnp.zeros((16, 1), F32)
    for chunks, slots, ds, first in ((chunks_a, slot_a, (0,), 0), (chunks_b, slot_b, (1, 2, 3), na)):
        for i, (c0, cn) in enumerate(chunks):
            recv_chunk(xrecv.at[slots, :, pl.ds(c0, cn)], lx_sem.at[first + i])
            cs = pl.ds(c0, cn)
            for d in ds:
                row = pl.ds(pl.multiple_of(((yi + d) % 4) * 16, 16), 16)
                z = own[d, :, cs] + lrecv2[d, :, cs] + xrecv[d, :, cs]
                if c0 + cn > vb:
                    z_out[row, c0:vb] = z[:, :vb - c0]
                    z = jnp.where(lax.broadcasted_iota(jnp.int32, (16, cn), 1) < vb - c0, z, -jnp.inf)
                else:
                    z_out[row, cs] = z
                m_new = jnp.maximum(tops[d], jnp.max(z, axis=1, keepdims=True))
                totals[d] = totals[d] * jnp.exp(tops[d] - m_new) + jnp.sum(jnp.exp(z - m_new), axis=1, keepdims=True)
                tops[d] = m_new
    lane = lax.broadcasted_iota(jnp.int32, (16, 128), 1)
    for d in range(4):
        lcol[(yi + d) % 4] = jnp.where(lane == 0, tops[d], totals[d])

    stat = lcol[...].reshape(rows, 128)
    mine = jnp.concatenate([stat, stat], axis=0).T[0:2]
    l_send[...] = mine
    for yy in ypeers:
        for xx in (x3, x2, x1, xi):
            send(l_send, l_recv.at[me], LSE, yy, xx)
    for xx in xpeers:
        send(l_send, l_recv.at[me], LSE, yi, xx)
    l_recv[me] = mine
    sent(st_recv.at[three], ST)
    sent(qkv.at[three, q_rows], QP)
    sent(qkv.at[three, kv_rows], KVP)
    sent(q_send.at[three], Q)
    sent(gu_recv, GU)
    sent(gux, GUX)
    sent(m_all.at[three], M)
    sent(o_recv.at[0, most], O1)
    sent(o_recv.at[1, most], O2)
    sent(bpart.at[three], B)
    sent(s2_recv.at[three], S2)
    sent(fbuf.at[three], FN)
    sent(lsend1, L1)
    sent(hold, LX)
    sent(lsend2, L2)
    recv(l_recv.at[most], LSE)
    tops = [l_recv[i, 0:1, :] for i in range(16)]
    top = functools.reduce(jnp.maximum, tops)
    total = sum([l_recv[i, 1:2, :] * jnp.exp(tops[i] - top) for i in range(16)])
    log_norm = top + jnp.log(total)
    lr_out[...] = log_norm[:, :rows]
    ln_out[...] = jnp.broadcast_to(log_norm, (128, 128)).T[:rows, 0:1]
    sent(l_recv.at[most], LSE)


def finish_kernel(own_rows, kv, z, ln, lr, k_out, v_out, lp_out, ln_out, k_s, v_s, lp_s, sem):
    k_s[...] = kv[0].astype(BF16)[:own_rows]
    v_s[...] = kv[1].astype(BF16)[:own_rows]
    copies = [pltpu.make_async_copy(k_s, k_out, sem.at[0]), pltpu.make_async_copy(v_s, v_out, sem.at[1]),
              pltpu.make_async_copy(lr, ln_out, sem.at[2])]
    for cp in copies:
        cp.start()
    for i in range(z.shape[0] // 8):
        at = pl.ds(i * 8, 8)
        lp_s[at] = z[at] - ln[at]
        copies.append(pltpu.make_async_copy(lp_s.at[at], lp_out.at[at], sem.at[3 + i]))
        copies[-1].start()
    for cp in copies:
        cp.wait()


def solution(mesh):
    row_spec = P(("dp", "yax", "xax"))

    def local_step(hidden, cache_len, k_cache, v_cache, g_attn, w_query, w_key, w_value,
                   w_gate, w_up, w_out, w_down, g_final, embedding):
        rows, wid = hidden.shape
        own_rows, seq, hd = k_cache.shape
        ffc = w_gate.shape[1] // 4
        vb = embedding.shape[0] // 4
        inv_freq = np.power(ROPE_BASE, -2.0 * np.arange(hd // 2) / hd).astype(np.float32).reshape(1, hd // 2)
        vbp = -(-vb // 128) * 128
        def cut(step):
            return [(c, min(step, vbp - c)) for c in range(0, vbp, step)]

        chunks_a, chunks_b, chunks_c = cut(512), cut(512), cut(1024)
        nx, nc = len(chunks_a) + len(chunks_b), len(chunks_c)
        sizes = (rows, wid, seq, hd, ffc, vb, chunks_a, chunks_b, chunks_c)
        any_spec = pl.BlockSpec(memory_space=pltpu.HBM)
        vmem = pl.BlockSpec(memory_space=pltpu.VMEM)
        v = pltpu.VMEM
        dma = pltpu.SemaphoreType.DMA
        scratch = [
            v((rows, wid), BF16), v((1, hd // 2), F32), v((2, 24, hd // 2), F32), v((1, wid), F32), v((1, wid), F32),
            *[v((seq, hd), BF16)] * 5, v((4, seq, hd), BF16),
            v((wid, 2 * hd), BF16), v((2, wid, hd), BF16), v((4, 2, wid, ffc), BF16),
            v((2 * hd, wid), BF16), v((4 * ffc, wid), BF16),
            v((8, 128), F32), v((4, 8, 128), F32), v((4, 24, 2 * hd), F32), v((4, 24, 2 * hd), F32),
            v((4, 16, 128), BF16), v((4, 16, 128), BF16), v((4, 8, hd), F32), v((8, hd), F32), v((8, hd), F32),
            v((4, 8, hd), F32), v((2, 8, seq), F32), v((2, 4, 8, 128), BF16), v((2, 16, 8, 128), BF16),
            v((4, 2, rows, ffc), F32), v((2, 2, rows, ffc), F32), v((2, rows, ffc), F32), v((2, rows, ffc), F32),
            v((4, rows, ffc), BF16), v((rows, wid), F32), v((4, 16, wid), F32), v((4, 16, wid), F32),
            v((16, 128), F32), v((4, 16, 128), F32), v((4, 16, wid), BF16),
            v((4, 16, vbp), F32), v((4, 16, vbp), F32), v((4, 16, vbp), F32), v((4, 16, vbp), F32),
            v((4, 16, vbp), F32), v((4, 16, vbp), F32), v((4, 16, vbp), F32), v((4, 16, 128), F32),
            v((2, 128), F32), v((16, 2, 128), F32),
            dma((21,)), dma((16,)), dma((13,)), dma((nx,)), dma((nx,)), dma((nc,)),
        ]
        kv, z, ln, lr = pl.pallas_call(
            functools.partial(step_kernel, sizes),
            name="decode_step",
            out_shape=(v((2, 8, hd), F32), v((rows, vb), F32), v((rows, 1), F32), v((1, rows), F32)),
            in_specs=[pl.BlockSpec(memory_space=pltpu.SMEM)] + [any_spec] * 14,
            out_specs=(vmem, vmem, vmem, vmem),
            scratch_shapes=scratch,
            compiler_params=pltpu.CompilerParams(collective_id=0, has_side_effects=True,
                                                 vmem_limit_bytes=67043328 - 900 * 1024),
        )(cache_len, hidden, jnp.asarray(inv_freq), k_cache, v_cache, g_attn.reshape(1, wid), w_query, w_key, w_value,
          w_gate, w_up, w_out, w_down, g_final.reshape(1, wid), embedding)
        k_new, v_new, log_probs, log_norm = pl.pallas_call(
            functools.partial(finish_kernel, own_rows),
            name="finish_step",
            out_shape=(jax.ShapeDtypeStruct((own_rows, hd), BF16), jax.ShapeDtypeStruct((own_rows, hd), BF16),
                       jax.ShapeDtypeStruct((rows, vb), F32), jax.ShapeDtypeStruct((1, rows), F32)),
            in_specs=[vmem] * 4,
            out_specs=(any_spec,) * 4,
            scratch_shapes=[v((own_rows, hd), BF16), v((own_rows, hd), BF16), v((rows, vb), F32), dma((11,))],
            compiler_params=pltpu.CompilerParams(vmem_limit_bytes=4 * 1024 * 1024),
        )(kv, z, ln, lr)
        return k_new, v_new, log_probs, log_norm[0]

    in_specs = (P("dp", "xax"), P("dp"), row_spec, row_spec, P("xax"), P("xax", "yax"),
                P("xax", None), P("xax", None), P("xax", "yax"), P("xax", "yax"),
                P("yax", "xax"), P("yax", "xax"), P("xax"), P("yax", "xax"))
    out_specs = (row_spec, row_spec, P("dp", ("yax", "xax")), P("dp"))
    return jax.shard_map(local_step, mesh=mesh, in_specs=in_specs, out_specs=out_specs, check_vma=False)
```

```python
import functools

import jax
import jax.numpy as jnp
import numpy as np
from jax import lax
from jax.experimental import pallas as pl
from jax.experimental.pallas import tpu as pltpu
from jax.sharding import PartitionSpec as P

EPS = 1e-6
ROPE_BASE = 10000.0
F32 = jnp.float32
BF16 = jnp.bfloat16
MESH = pl.DeviceIdType.MESH


def dot(a, b):
    return jnp.dot(a, b, preferred_element_type=F32)


def dot_t(a, b):
    return lax.dot_general(a, b, (((1,), (1,)), ((), ())), preferred_element_type=F32)


def one_hot_rows(rows, cols, source):
    r = lax.broadcasted_iota(jnp.int32, (rows, cols), 0)
    c = lax.broadcasted_iota(jnp.int32, (rows, cols), 1)
    return jnp.where(c == source(r), 1.0, 0.0).astype(BF16)


def step_kernel(sizes,
                lens, hidden_hbm, freq_hbm, k_hbm, v_hbm, ga_hbm, wq_hbm, wk_hbm, wv_hbm, wg_hbm, wu_hbm,
                wo_hbm, wd_hbm, gf_hbm, emb_hbm,
                kv_out, z_out, ln_out, lr_out,
                hid, freq, table, ga, gf, kb0, kb1, kb2, kb3, kb4, vbuf, wq, wkv, wgu, wo, wd,
                st_send, st_recv, qkv, qkv_recv, q_send, q_recv, qs, kns, vns, os_, sbuf, o_send, o_recv,
                gup, gu_recv, gux, gux_recv, m_all, mdown, bpart, b_recv, s2_send, s2_recv, fbuf,
                lsend1, lrecv1, hold, xrecv, drecv, lsend2, lrecv2, own, lcol, l_send, l_recv,
                ld_sem, snd_sem, rcv_sem, l1_sem, lx_sem, l2_sem, d_sem, x_ok, y_ok):
    rows, wid, seq, hd, ffc, vb, chunks_a, chunks_b, chunks_c = sizes
    yi = lax.axis_index("yax")
    xi = lax.axis_index("xax")
    x1 = xi + 1 - 2 * (xi % 2)
    x2 = (xi + 2) % 4
    x3 = (x1 + 2) % 4
    me = yi * 4 + xi
    ypeers = [(yi + d) % 4 for d in (1, 2, 3)]
    xpeers = [x1, x2, x3]

    def load(i, *pairs):
        for src, dst in pairs:
            pltpu.make_async_copy(src, dst, ld_sem.at[i]).start()

    def loaded(i, dst):
        pltpu.make_async_copy(dst, dst, ld_sem.at[i]).wait()

    HID, GA, FREQ, WQ, WKV, WGU, WD, WO, GF, KEY, VAL, EMB = 0, 1, 2, 3, 4, 5, 9, 10, 11, 12, 16, 20
    kb = (kb0, kb1, kb2, kb3, kb4)
    load(HID, (hidden_hbm, hid))
    load(GA, (ga_hbm, ga))
    barrier = pltpu.get_barrier_semaphore()
    odd = xi % 2 == 1
    even = xi % 2 == 0

    def signal(sem, yy, xx):
        pl.semaphore_signal(sem, inc=1, device_id={"yax": yy, "xax": xx}, device_id_type=MESH)

    @pl.when(odd)
    def _():
        signal(barrier, yi, x2)

    @pl.when(even)
    def _():
        signal(barrier, yi, x1)
        signal(barrier, yi, x3)

    load(FREQ, (freq_hbm, freq))
    load(WQ, (wq_hbm, wq))
    load(WKV, (wk_hbm, wkv.at[0]), (wv_hbm, wkv.at[1]))
    load(KEY, (k_hbm.at[0], kb[1]))
    for i, xx in enumerate((x1, x3, x2, xi)):
        cols = pl.ds(pl.multiple_of(xx * ffc, ffc), ffc)
        load(WGU + i, (wg_hbm.at[:, cols], wgu.at[xx, 0]), (wu_hbm.at[:, cols], wgu.at[xx, 1]))
    for j in range(1, 4):
        load(KEY + j, (k_hbm.at[j], kb[j + 1]))
    for j in range(4):
        load(VAL + j, (v_hbm.at[j], vbuf.at[j]))
    load(WD, (wd_hbm, wd))
    load(WO, (wo_hbm, wo))
    load(GF, (gf_hbm, gf))

    ST, QP, KVP, Q, GU, GUX, M, O1, O2, B, S2, FN, LSE, L1, LX, L2 = range(16)

    def send(src, dst, i, yy, xx, rsem=None):
        pltpu.make_async_remote_copy(src_ref=src, dst_ref=dst, send_sem=snd_sem.at[i],
                                     recv_sem=rcv_sem.at[i] if rsem is None else rsem,
                                     device_id={"yax": yy, "xax": xx}, device_id_type=MESH).start()

    def recv(dst, i):
        pltpu.make_async_copy(dst, dst, rcv_sem.at[i]).wait()

    def recv_chunk(dst, sem):
        pltpu.make_async_copy(dst, dst, sem).wait()

    def sent(src, i):
        pltpu.make_async_copy(src, src, snd_sem.at[i]).wait()

    three = pl.ds(0, 3)
    most = pl.ds(0, 15)

    tq = seq // 1024

    def transpose_keys(j, start, stop):
        if start == 0:
            loaded(KEY + j, kb[j + 1])

        def one(t, carry):
            at = pl.ds(pl.multiple_of(t * 256, 256), 256)
            kb[j][at] = kb[j + 1][at].T
            return carry

        lax.fori_loop(start * tq, stop * tq, one, 0, unroll=tq)

    loaded(HID, hid)
    loaded(GA, ga)
    h = hid[...].astype(F32)
    mean_l = jnp.sum(h, axis=1, keepdims=True) * (1.0 / wid)
    dev = h - mean_l
    m2_l = jnp.sum(dev * dev, axis=1, keepdims=True)
    lane = lax.broadcasted_iota(jnp.int32, (rows, 128), 1)
    stat = jnp.where(lane == 0, mean_l, m2_l)
    stat_t = jnp.concatenate([stat, stat], axis=0).T[:8]
    st_send[...] = stat_t

    @pl.when(odd)
    def _():
        pl.semaphore_wait(barrier, 3)
        signal(x_ok, yi, x1)

    @pl.when(even)
    def _():
        pl.semaphore_wait(x_ok, 1)
        for yy in ypeers:
            signal(barrier, yy, xi)

    for xx in xpeers:
        send(st_send, st_recv.at[xi], ST, yi, xx)
    perm = one_hot_rows(96, 64, lambda r: jnp.where(
        r % 24 < 16, ((r % 24) // 4) * 16 + (r // 24) * 4 + r % 4,
        jnp.where(r % 24 < 20, yi * 16 + (r // 24) * 4 + r % 4, -1)))
    loaded(FREQ, freq)
    prow = lax.broadcasted_iota(jnp.int32, (24, 128), 0)
    posn = jnp.zeros((24, 128), jnp.int32)
    for r in range(20):
        at = (r // 4) * 16 + xi * 4 + r % 4 if r < 16 else me * 4 + r - 16
        posn = jnp.where(prow == r, lens[at], posn)
    angle = posn.astype(F32) * freq[...]
    table[0] = jnp.cos(angle)
    table[1] = jnp.sin(angle)
    transpose_keys(0, 0, 4)
    recv(st_recv.at[three], ST)
    parts = [stat_t] + [st_recv[xx] for xx in xpeers]
    means = [p[0:1] for p in parts]
    mu = (means[0] + means[1] + means[2] + means[3]) * 0.25
    m2 = sum([p[1:2] for p in parts]) + wid * sum([(m - mu) * (m - mu) for m in means])
    rstd = lax.rsqrt(m2 * (1.0 / (4 * wid)) + EPS)
    sub = lax.broadcasted_iota(jnp.int32, (128, 128), 0)
    cols_t = jnp.where(sub == 0, mu, rstd).T
    mu_c = cols_t[:rows, 0:1]
    rstd_c = cols_t[:rows, 1:2]
    normed = ((h - mu_c) * rstd_c * ga[...]).astype(BF16)
    n_perm = dot(perm, normed).astype(BF16)

    loaded(WQ, wq)
    loaded(WKV, wkv)
    q_part = dot(n_perm, wq[...])
    kv_part = jnp.concatenate([dot(n_perm, wkv[0]), dot(n_perm, wkv[1])], axis=1)
    prow = lax.broadcasted_iota(jnp.int32, (96, 2 * hd), 0)
    qkv[...] = jnp.where(prow % 24 < 16, q_part, kv_part).reshape(4, 24, 2 * hd)
    q_rows, kv_rows = pl.ds(0, 16), pl.ds(16, 8)
    for xx in (x2, x3, x1):
        send(qkv.at[xx, q_rows], qkv_recv.at[xi, q_rows], QP, yi, xx)
    for xx in (x2, x3, x1):
        send(qkv.at[xx, kv_rows], qkv_recv.at[xi, kv_rows], KVP, yi, xx)

    for i, xx in enumerate((x1, x3, x2, xi)):
        loaded(WGU + i, wgu.at[xx])
        gup[xx, 0] = dot(normed, wgu[xx, 0])
        gup[xx, 1] = dot(normed, wgu[xx, 1])
        if i < 2:
            send(gup.at[xx], gu_recv.at[i], GU, yi, x1)

    transpose_keys(1, 0, 4)
    transpose_keys(2, 0, 2)
    half = hd // 2
    recv(qkv_recv.at[three, q_rows], QP)

    def total(at):
        return ((qkv[xi, at] + qkv_recv[x1, at]) + (qkv_recv[x2, at] + qkv_recv[x3, at])).astype(BF16).astype(F32)

    def rotary(lo, hi, at):
        cos_a, sin_a = table[0, at], table[1, at]
        return (lo * cos_a - hi * sin_a).astype(BF16), (hi * cos_a + lo * sin_a).astype(BF16)

    tot = total(q_rows)
    lo0, hi0, lo1, hi1 = [tot[:, i * half:(i + 1) * half] for i in range(4)]
    r0, r1 = rotary(lo0, hi0, q_rows)
    r2, r3 = rotary(lo1, hi1, q_rows)
    stacked = jnp.concatenate([r0, r1, r2, r3], axis=0)
    s1 = one_hot_rows(64, 64, lambda r: ((r // 4) % 4) * 16 + (r // 16) * 4 + r % 4)
    q_send[...] = dot(s1, stacked).astype(BF16).reshape(4, 16, 128)

    @pl.when(even)
    def _():
        pl.semaphore_wait(barrier, 3)
        signal(y_ok, yi, x1)

    @pl.when(odd)
    def _():
        pl.semaphore_wait(y_ok, 1)

    for yy in ypeers:
        send(q_send.at[yy], q_recv.at[yi], Q, yy, xi)
    q_recv[yi] = q_send[yi]
    recv(qkv_recv.at[three, kv_rows], KVP)
    tot = total(kv_rows)
    r0, r1 = rotary(tot[:, :half], tot[:, half:hd], kv_rows)
    kns[:, :half] = r0.astype(F32)
    kns[:, half:] = r1.astype(F32)
    vns[...] = tot[:, hd:]
    kv_out[0] = kns[...]
    kv_out[1] = vns[...]

    recv(gu_recv, GU)
    gux[...] = gup[x2] + gu_recv[1]
    send(gux, gux_recv, GUX, yi, x2)
    transpose_keys(2, 2, 4)
    transpose_keys(3, 0, 4)
    recv(q_recv.at[three], Q)
    s2 = one_hot_rows(64, 64, lambda r: ((r // 2) % 4) * 16 + (r % 2) * 8 + (r // 32) * 4 + (r // 8) % 4)
    q_all = dot(s2, q_recv[...].reshape(64, 128))
    qs[...] = jnp.concatenate([q_all[:32], q_all[32:]], axis=1).reshape(4, 8, hd)

    for j in range(4):
        loaded(VAL + j, vbuf.at[j])
    scale = hd ** -0.5
    pos = lax.broadcasted_iota(jnp.int32, (8, seq), 1)

    def scores(j):
        qj = qs[j].astype(BF16)
        for t in range(seq // 256):
            at = pl.ds(t * 256, 256)
            sbuf[j % 2, :, at] = dot(qj, kb[j][at])

    def mix(j):
        s_new = jnp.sum(qs[j] * kns[j:j + 1, :], axis=1, keepdims=True) * scale
        s = jnp.where(pos < lens[me * 4 + j], sbuf[j % 2] * scale, -jnp.inf)
        top = jnp.maximum(jnp.max(s, axis=1, keepdims=True), s_new)
        w = jnp.exp(s - top)
        w_new = jnp.exp(s_new - top)
        inv = 1.0 / (jnp.sum(w, axis=1, keepdims=True) + w_new)
        prob = (w * inv).astype(BF16)
        p_new = (w_new * inv).astype(BF16).astype(F32)
        hs = seq // 2
        acc = dot(prob[:, :hs], vbuf[j, :hs]) + dot(prob[:, hs:], vbuf[j, hs:])
        os_[j] = acc + p_new * vns[j:j + 1, :]

    s3 = one_hot_rows(32, 32, lambda r: ((r // 2) % 2) * 16 + (r % 2) * 8 + (r // 8) * 2 + (r // 4) % 2)

    def send_outputs(pair, i):
        o_bf = os_[2 * pair:2 * pair + 2].reshape(16, hd).astype(BF16)
        o_rows = dot(s3, jnp.concatenate([o_bf[:, :half], o_bf[:, half:]], axis=0))
        o_send[pair] = o_rows.reshape(4, 8, 128).astype(BF16)
        for yy in ypeers:
            for xx in (x3, x2, x1, xi):
                send(o_send.at[pair, yy], o_recv.at[pair, me], i, yy, xx)
        for xx in xpeers:
            send(o_send.at[pair, yi], o_recv.at[pair, me], i, yi, xx)
        o_recv[pair, me] = o_send[pair, yi]

    scores(0)
    scores(1)
    mix(0)
    scores(2)
    mix(1)
    scores(3)
    mix(2)
    recv(gux_recv, GUX)
    gu = gup[xi] + gu_recv[0] + gux_recv[...]
    gate = gu[0].astype(BF16).astype(F32)
    up_val = gu[1].astype(BF16).astype(F32)
    m_all[xi] = (gate * jax.nn.sigmoid(gate) * up_val).astype(BF16)
    for xx in (x2, x3, x1):
        send(m_all.at[xi], m_all.at[xi], M, yi, xx)
    send_outputs(0, O1)
    mix(3)
    send_outputs(1, O2)
    for j in range(4):
        voc = pl.ds(j * vb, vb)
        load(EMB, (emb_hbm.at[voc, pl.ds(0, hd)], vbuf.at[j, pl.ds(0, vb)]),
             (emb_hbm.at[voc, pl.ds(hd, hd)], vbuf.at[j, pl.ds(seq // 2, vb)]))
    loaded(WD, wd)
    loaded(WO, wo)
    loaded(GF, gf)
    recv(m_all.at[three], M)
    mdown[...] = sum([dot(m_all[i], wd[pl.ds(i * ffc, ffc)]) for i in range(4)])
    s4 = one_hot_rows(256, 256, lambda r: ((r // 2) % 2) * 128 + ((r % 64) // 4) * 8 + (r // 64) * 2 + r % 2)
    recv(o_recv.at[0, most], O1)
    recv(o_recv.at[1, most], O2)
    o_rows = jnp.concatenate([o_recv[pair, i].astype(F32) for pair in range(2) for i in range(16)], axis=0)
    a_all = dot(s4, o_rows.astype(BF16)).astype(BF16)
    attn = jnp.concatenate([a_all[i * 64:(i + 1) * 64] for i in range(4)], axis=1)
    bpart[...] = (dot(attn, wo[...]) + mdown[...]).reshape(4, 16, wid)
    for yy in (ypeers[1], ypeers[0], ypeers[2]):
        send(bpart.at[yy], b_recv.at[yi], B, yy, xi)
    res = hid[pl.ds(pl.multiple_of(yi * 16, 16), 16), :].astype(F32)
    recv(b_recv.at[three], B)
    res = res + ((bpart[yi] + b_recv[ypeers[0]]) + (b_recv[ypeers[1]] + b_recv[ypeers[2]]))

    mean_l = jnp.sum(res, axis=1, keepdims=True) * (1.0 / wid)
    dev = res - mean_l
    m2_l = jnp.sum(dev * dev, axis=1, keepdims=True)
    lane = lax.broadcasted_iota(jnp.int32, (16, 128), 1)
    s2_send[...] = jnp.where(lane < 64, mean_l, m2_l)
    for xx in xpeers:
        send(s2_send, s2_recv.at[xi], S2, yi, xx)
    recv(s2_recv.at[three], S2)
    parts = [s2_recv[xx] for xx in xpeers]
    means = [mean_l] + [p[:, 0:1] for p in parts]
    mu = (means[0] + means[1] + means[2] + means[3]) * 0.25
    m2 = m2_l + sum([p[:, 64:65] for p in parts]) + wid * sum([(m - mu) * (m - mu) for m in means])
    rstd = lax.rsqrt(m2 * (1.0 / (4 * wid)) + EPS)
    f_own = ((res - mu) * rstd * gf[...]).astype(BF16)
    fbuf[yi] = f_own
    for yy in ypeers:
        send(fbuf.at[yi], fbuf.at[yi], FN, yy, xi)
    loaded(EMB, vbuf.at[:, pl.ds(0, 2 * vb)])

    def logit_part(f, xx, c0, cn):
        return dot_t(f[:, :hd], vbuf[xx, pl.ds(c0, cn)]) + dot_t(f[:, hd:], vbuf[xx, pl.ds(seq // 2 + c0, cn)])

    def cross(i, at):
        recv_chunk(lrecv1.at[at], l1_sem.at[i])
        hold[at] = hold[at] + lrecv1[at]
        send(hold.at[at], xrecv.at[at], LX, yi, x2, lx_sem.at[i])

    def cross_blocks(f, slots, chunks, first):
        n = f.shape[0] // 16
        prev = None
        for i, (c0, cn) in enumerate(chunks):
            at = (slots, slice(None), pl.ds(c0, cn))
            if first + i == 0:
                hold[at] = logit_part(f, x2, c0, cn).reshape(n, 16, cn)
                send(hold.at[at], xrecv.at[at], LX, yi, x2, lx_sem.at[0])
                lsend1[at] = logit_part(f, x3, c0, cn).reshape(n, 16, cn)
                send(lsend1.at[at], drecv, L1, yi, x3, d_sem)
                continue
            lsend1[at] = logit_part(f, x3, c0, cn).reshape(n, 16, cn)
            send(lsend1.at[at], lrecv1.at[at], L1, yi, x1, l1_sem.at[first + i])
            hold[at] = logit_part(f, x2, c0, cn).reshape(n, 16, cn)
            if prev is not None:
                cross(*prev)
            prev = (first + i, at)
        cross(*prev)

    slot_a = pl.ds(0, 1)
    slot_b = pl.ds(1, 3)
    na = len(chunks_a)
    cross_blocks(f_own, slot_a, chunks_a, 0)
    recv(fbuf.at[three], FN)
    f_rest = jnp.concatenate([fbuf[yy] for yy in ypeers], axis=0)
    cross_blocks(f_rest, slot_b, chunks_b, na)
    f_all = jnp.concatenate([f_own, f_rest], axis=0)
    for i, (c0, cn) in enumerate(chunks_c):
        at = (slice(None), slice(None), pl.ds(c0, cn))
        lsend2[at] = logit_part(f_all, x1, c0, cn).reshape(4, 16, cn)
        send(lsend2.at[at], lrecv2.at[at], L2, yi, x1, l2_sem.at[i])
        own[at] = logit_part(f_all, xi, c0, cn).reshape(4, 16, cn)
    recv_chunk(lrecv2, l2_sem.at[0]) if len(chunks_c) == 1 else [
        recv_chunk(lrecv2.at[:, :, pl.ds(c0, cn)], l2_sem.at[i]) for i, (c0, cn) in enumerate(chunks_c)]
    tops, totals = {}, {}
    for d in range(4):
        tops[d] = jnp.full((16, 1), -jnp.inf, F32)
        totals[d] = jnp.zeros((16, 1), F32)
    for chunks, slots, ds, first in ((chunks_a, slot_a, (0,), 0), (chunks_b, slot_b, (1, 2, 3), na)):
        for i, (c0, cn) in enumerate(chunks):
            recv_chunk(xrecv.at[slots, :, pl.ds(c0, cn)], lx_sem.at[first + i])
            if first + i == 0:
                recv_chunk(drecv, d_sem)
            cs = pl.ds(c0, cn)
            for d in ds:
                row = pl.ds(pl.multiple_of(((yi + d) % 4) * 16, 16), 16)
                z = own[d, :, cs] + lrecv2[d, :, cs] + xrecv[d, :, cs]
                if first + i == 0:
                    z = z + drecv[0]
                if c0 + cn > vb:
                    z_out[row, c0:vb] = z[:, :vb - c0]
                    z = jnp.where(lax.broadcasted_iota(jnp.int32, (16, cn), 1) < vb - c0, z, -jnp.inf)
                else:
                    z_out[row, cs] = z
                m_new = jnp.maximum(tops[d], jnp.max(z, axis=1, keepdims=True))
                totals[d] = totals[d] * jnp.exp(tops[d] - m_new) + jnp.sum(jnp.exp(z - m_new), axis=1, keepdims=True)
                tops[d] = m_new
    lane = lax.broadcasted_iota(jnp.int32, (16, 128), 1)
    for d in range(4):
        lcol[(yi + d) % 4] = jnp.where(lane == 0, tops[d], totals[d])

    stat = lcol[...].reshape(rows, 128)
    mine = jnp.concatenate([stat, stat], axis=0).T[0:2]
    l_send[...] = mine
    for yy in ypeers:
        for xx in (x3, x2, x1, xi):
            send(l_send, l_recv.at[me], LSE, yy, xx)
    for xx in xpeers:
        send(l_send, l_recv.at[me], LSE, yi, xx)
    l_recv[me] = mine
    sent(st_recv.at[three], ST)
    sent(qkv.at[three, q_rows], QP)
    sent(qkv.at[three, kv_rows], KVP)
    sent(q_send.at[three], Q)
    sent(gu_recv, GU)
    sent(gux, GUX)
    sent(m_all.at[three], M)
    sent(o_recv.at[0, most], O1)
    sent(o_recv.at[1, most], O2)
    sent(bpart.at[three], B)
    sent(s2_recv.at[three], S2)
    sent(fbuf.at[three], FN)
    sent(lsend1, L1)
    sent(hold, LX)
    sent(lsend2, L2)
    recv(l_recv.at[most], LSE)
    tops = [l_recv[i, 0:1, :] for i in range(16)]
    top = functools.reduce(jnp.maximum, tops)
    total = sum([l_recv[i, 1:2, :] * jnp.exp(tops[i] - top) for i in range(16)])
    log_norm = top + jnp.log(total)
    lr_out[...] = log_norm[:, :rows]
    ln_out[...] = jnp.broadcast_to(log_norm, (128, 128)).T[:rows, 0:1]
    sent(l_recv.at[most], LSE)


def finish_kernel(own_rows, kv, z, ln, lr, k_out, v_out, lp_out, ln_out, k_s, v_s, lp_s, sem):
    k_s[...] = kv[0].astype(BF16)[:own_rows]
    v_s[...] = kv[1].astype(BF16)[:own_rows]
    copies = [pltpu.make_async_copy(k_s, k_out, sem.at[0]), pltpu.make_async_copy(v_s, v_out, sem.at[1]),
              pltpu.make_async_copy(lr, ln_out, sem.at[2])]
    for cp in copies:
        cp.start()
    for i in range(z.shape[0] // 8):
        at = pl.ds(i * 8, 8)
        lp_s[at] = z[at] - ln[at]
        copies.append(pltpu.make_async_copy(lp_s.at[at], lp_out.at[at], sem.at[3 + i]))
        copies[-1].start()
    for cp in copies:
        cp.wait()


def solution(mesh):
    row_spec = P(("dp", "yax", "xax"))

    def local_step(hidden, cache_len, k_cache, v_cache, g_attn, w_query, w_key, w_value,
                   w_gate, w_up, w_out, w_down, g_final, embedding):
        rows, wid = hidden.shape
        own_rows, seq, hd = k_cache.shape
        ffc = w_gate.shape[1] // 4
        vb = embedding.shape[0] // 4
        inv_freq = np.power(ROPE_BASE, -2.0 * np.arange(hd // 2) / hd).astype(np.float32).reshape(1, hd // 2)
        vbp = -(-vb // 128) * 128
        def cut(step):
            return [(c, min(step, vbp - c)) for c in range(0, vbp, step)]

        chunks_a, chunks_b, chunks_c = cut(512), cut(512), cut(1024)
        nx, nc = len(chunks_a) + len(chunks_b), len(chunks_c)
        sizes = (rows, wid, seq, hd, ffc, vb, chunks_a, chunks_b, chunks_c)
        any_spec = pl.BlockSpec(memory_space=pltpu.HBM)
        vmem = pl.BlockSpec(memory_space=pltpu.VMEM)
        v = pltpu.VMEM
        dma = pltpu.SemaphoreType.DMA
        scratch = [
            v((rows, wid), BF16), v((1, hd // 2), F32), v((2, 24, hd // 2), F32), v((1, wid), F32), v((1, wid), F32),
            *[v((seq, hd), BF16)] * 5, v((4, seq, hd), BF16),
            v((wid, 2 * hd), BF16), v((2, wid, hd), BF16), v((4, 2, wid, ffc), BF16),
            v((2 * hd, wid), BF16), v((4 * ffc, wid), BF16),
            v((8, 128), F32), v((4, 8, 128), F32), v((4, 24, 2 * hd), F32), v((4, 24, 2 * hd), F32),
            v((4, 16, 128), BF16), v((4, 16, 128), BF16), v((4, 8, hd), F32), v((8, hd), F32), v((8, hd), F32),
            v((4, 8, hd), F32), v((2, 8, seq), F32), v((2, 4, 8, 128), BF16), v((2, 16, 8, 128), BF16),
            v((4, 2, rows, ffc), F32), v((2, 2, rows, ffc), F32), v((2, rows, ffc), F32), v((2, rows, ffc), F32),
            v((4, rows, ffc), BF16), v((rows, wid), F32), v((4, 16, wid), F32), v((4, 16, wid), F32),
            v((16, 128), F32), v((4, 16, 128), F32), v((4, 16, wid), BF16),
            v((4, 16, vbp), F32), v((4, 16, vbp), F32), v((4, 16, vbp), F32), v((4, 16, vbp), F32),
            v((1, 16, chunks_a[0][1]), F32), v((4, 16, vbp), F32), v((4, 16, vbp), F32), v((4, 16, vbp), F32), v((4, 16, 128), F32),
            v((2, 128), F32), v((16, 2, 128), F32),
            dma((21,)), dma((16,)), dma((13,)), dma((nx,)), dma((nx,)), dma((nc,)), dma(()), pltpu.SemaphoreType.REGULAR, pltpu.SemaphoreType.REGULAR,
        ]
        kv, z, ln, lr = pl.pallas_call(
            functools.partial(step_kernel, sizes),
            name="decode_step",
            out_shape=(v((2, 8, hd), F32), v((rows, vb), F32), v((rows, 1), F32), v((1, rows), F32)),
            in_specs=[pl.BlockSpec(memory_space=pltpu.SMEM)] + [any_spec] * 14,
            out_specs=(vmem, vmem, vmem, vmem),
            scratch_shapes=scratch,
            compiler_params=pltpu.CompilerParams(collective_id=0, has_side_effects=True,
                                                 vmem_limit_bytes=67043328 - 900 * 1024),
        )(cache_len, hidden, jnp.asarray(inv_freq), k_cache, v_cache, g_attn.reshape(1, wid), w_query, w_key, w_value,
          w_gate, w_up, w_out, w_down, g_final.reshape(1, wid), embedding)
        k_new, v_new, log_probs, log_norm = pl.pallas_call(
            functools.partial(finish_kernel, own_rows),
            name="finish_step",
            out_shape=(jax.ShapeDtypeStruct((own_rows, hd), BF16), jax.ShapeDtypeStruct((own_rows, hd), BF16),
                       jax.ShapeDtypeStruct((rows, vb), F32), jax.ShapeDtypeStruct((1, rows), F32)),
            in_specs=[vmem] * 4,
            out_specs=(any_spec,) * 4,
            scratch_shapes=[v((own_rows, hd), BF16), v((own_rows, hd), BF16), v((rows, vb), F32), dma((11,))],
            compiler_params=pltpu.CompilerParams(vmem_limit_bytes=4 * 1024 * 1024),
        )(kv, z, ln, lr)
        return k_new, v_new, log_probs, log_norm[0]

    in_specs = (P("dp", "xax"), P("dp"), row_spec, row_spec, P("xax"), P("xax", "yax"),
                P("xax", None), P("xax", None), P("xax", "yax"), P("xax", "yax"),
                P("yax", "xax"), P("yax", "xax"), P("xax"), P("yax", "xax"))
    out_specs = (row_spec, row_spec, P("dp", ("yax", "xax")), P("dp"))
    return jax.shard_map(local_step, mesh=mesh, in_specs=in_specs, out_specs=out_specs, check_vma=False)
```

```python
import functools

import jax
import jax.numpy as jnp
import numpy as np
from jax import lax
from jax.experimental import pallas as pl
from jax.experimental.pallas import tpu as pltpu
from jax.sharding import PartitionSpec as P

EPS = 1e-6
ROPE_BASE = 10000.0
F32 = jnp.float32
BF16 = jnp.bfloat16
MESH = pl.DeviceIdType.MESH


def dot(a, b):
    return jnp.dot(a, b, preferred_element_type=F32)


def dot_t(a, b):
    return lax.dot_general(a, b, (((1,), (1,)), ((), ())), preferred_element_type=F32)


def one_hot_rows(rows, cols, source):
    r = lax.broadcasted_iota(jnp.int32, (rows, cols), 0)
    c = lax.broadcasted_iota(jnp.int32, (rows, cols), 1)
    return jnp.where(c == source(r), 1.0, 0.0).astype(BF16)


def step_kernel(sizes,
                lens, hidden_hbm, freq_hbm, k_hbm, v_hbm, ga_hbm, wq_hbm, wk_hbm, wv_hbm, wg_hbm, wu_hbm,
                wo_hbm, wd_hbm, gf_hbm, emb_hbm,
                kv_out, z_out, ln_out, lr_out,
                hid, freq, table, ga, gf, kb0, kb1, kb2, kb3, kb4, vbuf, wq, wkv, wgu, wo, wd,
                st_send, st_recv, qkv, qkv_recv, q_send, q_recv, qs, kns, vns, os_, sbuf, o_send, o_recv,
                gup, gu_recv, gux, gux_recv, m_all, mdown, bpart, b_recv, s2_send, s2_recv, fbuf,
                lsend1, lrecv1, hold, xrecv, drecv, lsend2, lrecv2, own, lcol, l_send, l_recv,
                ld_sem, snd_sem, rcv_sem, l1_sem, lx_sem, l2_sem, d_sem, x_ok, y_ok):
    rows, wid, seq, hd, ffc, vb, chunks_a, chunks_b, chunks_c = sizes
    yi = lax.axis_index("yax")
    xi = lax.axis_index("xax")
    x1 = xi + 1 - 2 * (xi % 2)
    x2 = (xi + 2) % 4
    x3 = (x1 + 2) % 4
    me = yi * 4 + xi
    ypeers = [3 * (1 - yi // 2), 2 - yi // 2, yi + 1 - 2 * (yi % 2)]
    xpeers = [x1, x2, x3]

    def load(i, *pairs):
        for src, dst in pairs:
            pltpu.make_async_copy(src, dst, ld_sem.at[i]).start()

    def loaded(i, dst):
        pltpu.make_async_copy(dst, dst, ld_sem.at[i]).wait()

    HID, GA, FREQ, WQ, WKV, WGU, WD, WO, GF, KEY, VAL, EMB = 0, 1, 2, 3, 4, 5, 9, 10, 11, 12, 16, 20
    kb = (kb0, kb1, kb2, kb3, kb4)
    load(HID, (hidden_hbm, hid))
    load(GA, (ga_hbm, ga))
    barrier = pltpu.get_barrier_semaphore()
    odd = xi % 2 == 1
    even = xi % 2 == 0

    def signal(sem, yy, xx):
        pl.semaphore_signal(sem, inc=1, device_id={"yax": yy, "xax": xx}, device_id_type=MESH)

    @pl.when(odd)
    def _():
        signal(barrier, yi, x2)

    @pl.when(even)
    def _():
        signal(barrier, yi, x1)
        signal(barrier, yi, x3)

    load(FREQ, (freq_hbm, freq))
    load(WQ, (wq_hbm, wq))
    load(WKV, (wk_hbm, wkv.at[0]), (wv_hbm, wkv.at[1]))
    load(KEY, (k_hbm.at[0], kb[1]))
    for i, xx in enumerate((x1, x3, x2, xi)):
        cols = pl.ds(pl.multiple_of(xx * ffc, ffc), ffc)
        load(WGU + i, (wg_hbm.at[:, cols], wgu.at[xx, 0]), (wu_hbm.at[:, cols], wgu.at[xx, 1]))
    for j in range(1, 4):
        load(KEY + j, (k_hbm.at[j], kb[j + 1]))
    for j in range(4):
        load(VAL + j, (v_hbm.at[j], vbuf.at[j]))
    load(WD, (wd_hbm, wd))
    load(WO, (wo_hbm, wo))
    load(GF, (gf_hbm, gf))

    ST, QP, KVP, Q, GU, GUX, M, O1, O2, B, S2, FN, LSE, L1, LX, L2 = range(16)

    def send(src, dst, i, yy, xx, rsem=None):
        pltpu.make_async_remote_copy(src_ref=src, dst_ref=dst, send_sem=snd_sem.at[i],
                                     recv_sem=rcv_sem.at[i] if rsem is None else rsem,
                                     device_id={"yax": yy, "xax": xx}, device_id_type=MESH).start()

    def recv(dst, i):
        pltpu.make_async_copy(dst, dst, rcv_sem.at[i]).wait()

    def recv_chunk(dst, sem):
        pltpu.make_async_copy(dst, dst, sem).wait()

    def sent(src, i):
        pltpu.make_async_copy(src, src, snd_sem.at[i]).wait()

    three = pl.ds(0, 3)
    most = pl.ds(0, 15)

    tq = seq // 1024

    def transpose_keys(j, start, stop):
        if start == 0:
            loaded(KEY + j, kb[j + 1])

        def one(t, carry):
            at = pl.ds(pl.multiple_of(t * 256, 256), 256)
            kb[j][at] = kb[j + 1][at].T
            return carry

        lax.fori_loop(start * tq, stop * tq, one, 0, unroll=tq)

    loaded(HID, hid)
    loaded(GA, ga)
    h = hid[...].astype(F32)
    mean_l = jnp.sum(h, axis=1, keepdims=True) * (1.0 / wid)
    dev = h - mean_l
    m2_l = jnp.sum(dev * dev, axis=1, keepdims=True)
    lane = lax.broadcasted_iota(jnp.int32, (rows, 128), 1)
    stat = jnp.where(lane == 0, mean_l, m2_l)
    stat_t = jnp.concatenate([stat, stat], axis=0).T[:8]
    st_send[...] = stat_t

    @pl.when(odd)
    def _():
        pl.semaphore_wait(barrier, 3)
        signal(x_ok, yi, x1)

    @pl.when(even)
    def _():
        pl.semaphore_wait(x_ok, 1)
        for yy in ypeers:
            signal(barrier, yy, xi)

    for xx in xpeers:
        send(st_send, st_recv.at[xi], ST, yi, xx)
    perm = one_hot_rows(96, 64, lambda r: jnp.where(
        r % 24 < 16, ((r % 24) // 4) * 16 + (r // 24) * 4 + r % 4,
        jnp.where(r % 24 < 20, yi * 16 + (r // 24) * 4 + r % 4, -1)))
    loaded(FREQ, freq)
    prow = lax.broadcasted_iota(jnp.int32, (24, 128), 0)
    posn = jnp.zeros((24, 128), jnp.int32)
    for r in range(20):
        at = (r // 4) * 16 + xi * 4 + r % 4 if r < 16 else me * 4 + r - 16
        posn = jnp.where(prow == r, lens[at], posn)
    angle = posn.astype(F32) * freq[...]
    table[0] = jnp.cos(angle)
    table[1] = jnp.sin(angle)
    transpose_keys(0, 0, 2)
    recv(st_recv.at[three], ST)
    parts = [stat_t] + [st_recv[xx] for xx in xpeers]
    means = [p[0:1] for p in parts]
    mu = (means[0] + means[1] + means[2] + means[3]) * 0.25
    m2 = sum([p[1:2] for p in parts]) + wid * sum([(m - mu) * (m - mu) for m in means])
    rstd = lax.rsqrt(m2 * (1.0 / (4 * wid)) + EPS)
    sub = lax.broadcasted_iota(jnp.int32, (128, 128), 0)
    cols_t = jnp.where(sub == 0, mu, rstd).T
    mu_c = cols_t[:rows, 0:1]
    rstd_c = cols_t[:rows, 1:2]
    normed = ((h - mu_c) * rstd_c * ga[...]).astype(BF16)
    n_perm = dot(perm, normed).astype(BF16)

    loaded(WQ, wq)
    loaded(WKV, wkv)
    q_part = dot(n_perm, wq[...])
    kv_part = jnp.concatenate([dot(n_perm, wkv[0]), dot(n_perm, wkv[1])], axis=1)
    prow = lax.broadcasted_iota(jnp.int32, (96, 2 * hd), 0)
    qkv[...] = jnp.where(prow % 24 < 16, q_part, kv_part).reshape(4, 24, 2 * hd)
    q_rows, kv_rows = pl.ds(0, 16), pl.ds(16, 8)
    for xx in (x2, x3, x1):
        send(qkv.at[xx, q_rows], qkv_recv.at[xi, q_rows], QP, yi, xx)
    for xx in (x2, x3, x1):
        send(qkv.at[xx, kv_rows], qkv_recv.at[xi, kv_rows], KVP, yi, xx)

    for i, xx in enumerate((x1, x3, x2, xi)):
        loaded(WGU + i, wgu.at[xx])
        gup[xx, 0] = dot(normed, wgu[xx, 0])
        gup[xx, 1] = dot(normed, wgu[xx, 1])
        if i < 2:
            send(gup.at[xx], gu_recv.at[i], GU, yi, x1)

    transpose_keys(0, 2, 4)
    recv(gu_recv, GU)
    gux[...] = gup[x2] + gu_recv[1]
    send(gux, gux_recv, GUX, yi, x2)
    transpose_keys(1, 0, 4)
    transpose_keys(2, 0, 1)
    half = hd // 2
    recv(qkv_recv.at[three, q_rows], QP)

    def total(at):
        return ((qkv[xi, at] + qkv_recv[x1, at]) + (qkv_recv[x2, at] + qkv_recv[x3, at])).astype(BF16).astype(F32)

    def rotary(lo, hi, at):
        cos_a, sin_a = table[0, at], table[1, at]
        return (lo * cos_a - hi * sin_a).astype(BF16), (hi * cos_a + lo * sin_a).astype(BF16)

    tot = total(q_rows)
    lo0, hi0, lo1, hi1 = [tot[:, i * half:(i + 1) * half] for i in range(4)]
    r0, r1 = rotary(lo0, hi0, q_rows)
    r2, r3 = rotary(lo1, hi1, q_rows)
    stacked = jnp.concatenate([r0, r1, r2, r3], axis=0)
    s1 = one_hot_rows(64, 64, lambda r: ((r // 4) % 4) * 16 + (r // 16) * 4 + r % 4)
    q_send[...] = dot(s1, stacked).astype(BF16).reshape(4, 16, 128)

    @pl.when(even)
    def _():
        pl.semaphore_wait(barrier, 3)
        signal(y_ok, yi, x1)

    @pl.when(odd)
    def _():
        pl.semaphore_wait(y_ok, 1)

    for yy in ypeers:
        send(q_send.at[yy], q_recv.at[yi], Q, yy, xi)
    q_recv[yi] = q_send[yi]
    recv(qkv_recv.at[three, kv_rows], KVP)
    tot = total(kv_rows)
    r0, r1 = rotary(tot[:, :half], tot[:, half:hd], kv_rows)
    kns[:, :half] = r0.astype(F32)
    kns[:, half:] = r1.astype(F32)
    vns[...] = tot[:, hd:]
    kv_out[0] = kns[...]
    kv_out[1] = vns[...]

    transpose_keys(2, 1, 4)
    transpose_keys(3, 0, 4)
    recv(q_recv.at[three], Q)
    s2 = one_hot_rows(64, 64, lambda r: ((r // 2) % 4) * 16 + (r % 2) * 8 + (r // 32) * 4 + (r // 8) % 4)
    q_all = dot(s2, q_recv[...].reshape(64, 128))
    qs[...] = jnp.concatenate([q_all[:32], q_all[32:]], axis=1).reshape(4, 8, hd)

    scale = hd ** -0.5
    pos = lax.broadcasted_iota(jnp.int32, (8, seq), 1)

    def scores(j):
        qj = qs[j].astype(BF16)
        for t in range(seq // 256):
            at = pl.ds(t * 256, 256)
            sbuf[j % 2, :, at] = dot(qj, kb[j][at])

    def weights(j):
        s_new = jnp.sum(qs[j] * kns[j:j + 1, :], axis=1, keepdims=True) * scale
        s = jnp.where(pos < lens[me * 4 + j], sbuf[j % 2] * scale, -jnp.inf)
        top = jnp.maximum(jnp.max(s, axis=1, keepdims=True), s_new)
        w = jnp.exp(s - top)
        w_new = jnp.exp(s_new - top)
        inv = 1.0 / (jnp.sum(w, axis=1, keepdims=True) + w_new)
        return (w * inv).astype(BF16), (w_new * inv).astype(BF16).astype(F32)

    def mix(j, prob, p_new):
        hs = seq // 2
        acc = dot(prob[:, :hs], vbuf[j, :hs]) + dot(prob[:, hs:], vbuf[j, hs:])
        os_[j] = acc + p_new * vns[j:j + 1, :]

    s3 = one_hot_rows(32, 32, lambda r: ((r // 2) % 2) * 16 + (r % 2) * 8 + (r // 8) * 2 + (r // 4) % 2)

    def send_outputs(pair, i):
        o_bf = os_[2 * pair:2 * pair + 2].reshape(16, hd).astype(BF16)
        o_rows = dot(s3, jnp.concatenate([o_bf[:, :half], o_bf[:, half:]], axis=0))
        o_send[pair] = o_rows.reshape(4, 8, 128).astype(BF16)
        for yy in ypeers:
            for xx in (x3, x2, x1, xi):
                send(o_send.at[pair, yy], o_recv.at[pair, me], i, yy, xx)
        for xx in xpeers:
            send(o_send.at[pair, yi], o_recv.at[pair, me], i, yi, xx)
        o_recv[pair, me] = o_send[pair, yi]

    scores(0)
    scores(1)
    w0 = weights(0)
    loaded(VAL, vbuf.at[0])
    loaded(VAL + 1, vbuf.at[1])
    mix(0, *w0)
    scores(2)
    mix(1, *weights(1))
    recv(gux_recv, GUX)
    gu = gup[xi] + gu_recv[0] + gux_recv[...]
    gate = gu[0].astype(BF16).astype(F32)
    up_val = gu[1].astype(BF16).astype(F32)
    m_all[xi] = (gate * jax.nn.sigmoid(gate) * up_val).astype(BF16)
    for xx in (x2, x3, x1):
        send(m_all.at[xi], m_all.at[xi], M, yi, xx)
    loaded(VAL + 2, vbuf.at[2])
    scores(3)
    mix(2, *weights(2))
    w3 = weights(3)
    loaded(VAL + 3, vbuf.at[3])
    send_outputs(0, O1)
    mix(3, *w3)
    send_outputs(1, O2)
    for j in range(4):
        voc = pl.ds(j * vb, vb)
        load(EMB, (emb_hbm.at[voc, pl.ds(0, hd)], vbuf.at[j, pl.ds(0, vb)]),
             (emb_hbm.at[voc, pl.ds(hd, hd)], vbuf.at[j, pl.ds(seq // 2, vb)]))
    loaded(WD, wd)
    loaded(WO, wo)
    loaded(GF, gf)
    recv(m_all.at[three], M)
    mdown[...] = sum([dot(m_all[i], wd[pl.ds(i * ffc, ffc)]) for i in range(4)])
    s4 = one_hot_rows(256, 256, lambda r: ((r // 2) % 2) * 128 + ((r % 64) // 4) * 8 + (r // 64) * 2 + r % 2)
    recv(o_recv.at[0, most], O1)
    recv(o_recv.at[1, most], O2)
    o_rows = jnp.concatenate([o_recv[pair, i].astype(F32) for pair in range(2) for i in range(16)], axis=0)
    a_all = dot(s4, o_rows.astype(BF16)).astype(BF16)
    attn = jnp.concatenate([a_all[i * 64:(i + 1) * 64] for i in range(4)], axis=1)
    bpart[...] = (dot(attn, wo[...]) + mdown[...]).reshape(4, 16, wid)
    for yy in ypeers:
        send(bpart.at[yy], b_recv.at[yi], B, yy, xi)
    res = hid[pl.ds(pl.multiple_of(yi * 16, 16), 16), :].astype(F32)
    recv(b_recv.at[three], B)
    res = res + ((bpart[yi] + b_recv[ypeers[0]]) + (b_recv[ypeers[1]] + b_recv[ypeers[2]]))

    mean_l = jnp.sum(res, axis=1, keepdims=True) * (1.0 / wid)
    dev = res - mean_l
    m2_l = jnp.sum(dev * dev, axis=1, keepdims=True)
    lane = lax.broadcasted_iota(jnp.int32, (16, 128), 1)
    s2_send[...] = jnp.where(lane < 64, mean_l, m2_l)
    for xx in xpeers:
        send(s2_send, s2_recv.at[xi], S2, yi, xx)
    recv(s2_recv.at[three], S2)
    parts = [s2_recv[xx] for xx in xpeers]
    means = [mean_l] + [p[:, 0:1] for p in parts]
    mu = (means[0] + means[1] + means[2] + means[3]) * 0.25
    m2 = m2_l + sum([p[:, 64:65] for p in parts]) + wid * sum([(m - mu) * (m - mu) for m in means])
    rstd = lax.rsqrt(m2 * (1.0 / (4 * wid)) + EPS)
    f_own = ((res - mu) * rstd * gf[...]).astype(BF16)
    fbuf[yi] = f_own
    for yy in ypeers:
        send(fbuf.at[yi], fbuf.at[yi], FN, yy, xi)
    loaded(EMB, vbuf.at[:, pl.ds(0, 2 * vb)])

    def logit_part(f, xx, c0, cn):
        return dot_t(f[:, :hd], vbuf[xx, pl.ds(c0, cn)]) + dot_t(f[:, hd:], vbuf[xx, pl.ds(seq // 2 + c0, cn)])

    def cross(i, at):
        recv_chunk(lrecv1.at[at], l1_sem.at[i])
        hold[at] = hold[at] + lrecv1[at]
        send(hold.at[at], xrecv.at[at], LX, yi, x2, lx_sem.at[i])

    def cross_blocks(f, slots, chunks, first):
        n = f.shape[0] // 16
        prev = None
        for i, (c0, cn) in enumerate(chunks):
            at = (slots, slice(None), pl.ds(c0, cn))
            if first + i == 0:
                hold[at] = logit_part(f, x2, c0, cn).reshape(n, 16, cn)
                send(hold.at[at], xrecv.at[at], LX, yi, x2, lx_sem.at[0])
                lsend1[at] = logit_part(f, x3, c0, cn).reshape(n, 16, cn)
                send(lsend1.at[at], drecv, L1, yi, x3, d_sem)
                continue
            lsend1[at] = logit_part(f, x3, c0, cn).reshape(n, 16, cn)
            send(lsend1.at[at], lrecv1.at[at], L1, yi, x1, l1_sem.at[first + i])
            hold[at] = logit_part(f, x2, c0, cn).reshape(n, 16, cn)
            if prev is not None:
                cross(*prev)
            prev = (first + i, at)
        cross(*prev)

    slot_a = pl.ds(0, 1)
    slot_b = pl.ds(1, 3)
    na = len(chunks_a)
    cross_blocks(f_own, slot_a, chunks_a, 0)
    recv(fbuf.at[three], FN)
    f_rest = jnp.concatenate([fbuf[yy] for yy in ypeers], axis=0)
    cross_blocks(f_rest, slot_b, chunks_b, na)
    f_all = jnp.concatenate([f_own, f_rest], axis=0)
    for i, (c0, cn) in enumerate(chunks_c):
        at = (slice(None), slice(None), pl.ds(c0, cn))
        lsend2[at] = logit_part(f_all, x1, c0, cn).reshape(4, 16, cn)
        send(lsend2.at[at], lrecv2.at[at], L2, yi, x1, l2_sem.at[i])
        own[at] = logit_part(f_all, xi, c0, cn).reshape(4, 16, cn)
    recv_chunk(lrecv2, l2_sem.at[0]) if len(chunks_c) == 1 else [
        recv_chunk(lrecv2.at[:, :, pl.ds(c0, cn)], l2_sem.at[i]) for i, (c0, cn) in enumerate(chunks_c)]
    tops, totals = {}, {}
    order = [yi] + ypeers
    for d in range(4):
        tops[d] = jnp.full((16, 1), -jnp.inf, F32)
        totals[d] = jnp.zeros((16, 1), F32)
    for chunks, slots, ds, first in ((chunks_a, slot_a, (0,), 0), (chunks_b, slot_b, (1, 2, 3), na)):
        for i, (c0, cn) in enumerate(chunks):
            recv_chunk(xrecv.at[slots, :, pl.ds(c0, cn)], lx_sem.at[first + i])
            if first + i == 0:
                recv_chunk(drecv, d_sem)
            cs = pl.ds(c0, cn)
            for d in ds:
                row = pl.ds(pl.multiple_of(order[d] * 16, 16), 16)
                z = own[d, :, cs] + lrecv2[d, :, cs] + xrecv[d, :, cs]
                if first + i == 0:
                    z = z + drecv[0]
                if c0 + cn > vb:
                    z_out[row, c0:vb] = z[:, :vb - c0]
                    z = jnp.where(lax.broadcasted_iota(jnp.int32, (16, cn), 1) < vb - c0, z, -jnp.inf)
                else:
                    z_out[row, cs] = z
                m_new = jnp.maximum(tops[d], jnp.max(z, axis=1, keepdims=True))
                totals[d] = totals[d] * jnp.exp(tops[d] - m_new) + jnp.sum(jnp.exp(z - m_new), axis=1, keepdims=True)
                tops[d] = m_new
    lane = lax.broadcasted_iota(jnp.int32, (16, 128), 1)
    for d in range(4):
        lcol[order[d]] = jnp.where(lane == 0, tops[d], totals[d])

    stat = lcol[...].reshape(rows, 128)
    mine = jnp.concatenate([stat, stat], axis=0).T[0:2]
    l_send[...] = mine
    for yy in ypeers:
        for xx in (x3, x2, x1, xi):
            send(l_send, l_recv.at[me], LSE, yy, xx)
    for xx in xpeers:
        send(l_send, l_recv.at[me], LSE, yi, xx)
    l_recv[me] = mine
    sent(st_recv.at[three], ST)
    sent(qkv.at[three, q_rows], QP)
    sent(qkv.at[three, kv_rows], KVP)
    sent(q_send.at[three], Q)
    sent(gu_recv, GU)
    sent(gux, GUX)
    sent(m_all.at[three], M)
    sent(o_recv.at[0, most], O1)
    sent(o_recv.at[1, most], O2)
    sent(bpart.at[three], B)
    sent(s2_recv.at[three], S2)
    sent(fbuf.at[three], FN)
    sent(lsend1, L1)
    sent(hold, LX)
    sent(lsend2, L2)
    recv(l_recv.at[most], LSE)
    tops = [l_recv[i, 0:1, :] for i in range(16)]
    top = functools.reduce(jnp.maximum, tops)
    total = sum([l_recv[i, 1:2, :] * jnp.exp(tops[i] - top) for i in range(16)])
    log_norm = top + jnp.log(total)
    lr_out[...] = log_norm[:, :rows]
    ln_out[...] = jnp.broadcast_to(log_norm, (128, 128)).T[:rows, 0:1]
    sent(l_recv.at[most], LSE)


def finish_kernel(own_rows, kv, z, ln, lr, k_out, v_out, lp_out, ln_out, k_s, v_s, lp_s, sem):
    k_s[...] = kv[0].astype(BF16)[:own_rows]
    v_s[...] = kv[1].astype(BF16)[:own_rows]
    copies = [pltpu.make_async_copy(k_s, k_out, sem.at[0]), pltpu.make_async_copy(v_s, v_out, sem.at[1]),
              pltpu.make_async_copy(lr, ln_out, sem.at[2])]
    for cp in copies:
        cp.start()
    for i in range(z.shape[0] // 8):
        at = pl.ds(i * 8, 8)
        lp_s[at] = z[at] - ln[at]
        copies.append(pltpu.make_async_copy(lp_s.at[at], lp_out.at[at], sem.at[3 + i]))
        copies[-1].start()
    for cp in copies:
        cp.wait()


def solution(mesh):
    row_spec = P(("dp", "yax", "xax"))

    def local_step(hidden, cache_len, k_cache, v_cache, g_attn, w_query, w_key, w_value,
                   w_gate, w_up, w_out, w_down, g_final, embedding):
        rows, wid = hidden.shape
        own_rows, seq, hd = k_cache.shape
        ffc = w_gate.shape[1] // 4
        vb = embedding.shape[0] // 4
        inv_freq = np.power(ROPE_BASE, -2.0 * np.arange(hd // 2) / hd).astype(np.float32).reshape(1, hd // 2)
        vbp = -(-vb // 128) * 128
        def cut(step, start=0):
            return [(c, min(step, vbp - c)) for c in range(start, vbp, step)]

        chunks_a = [(0, 512)] + cut(768, 512)
        chunks_b, chunks_c = cut(768), cut(1792)
        nx, nc = len(chunks_a) + len(chunks_b), len(chunks_c)
        sizes = (rows, wid, seq, hd, ffc, vb, chunks_a, chunks_b, chunks_c)
        any_spec = pl.BlockSpec(memory_space=pltpu.HBM)
        vmem = pl.BlockSpec(memory_space=pltpu.VMEM)
        v = pltpu.VMEM
        dma = pltpu.SemaphoreType.DMA
        scratch = [
            v((rows, wid), BF16), v((1, hd // 2), F32), v((2, 24, hd // 2), F32), v((1, wid), F32), v((1, wid), F32),
            *[v((seq, hd), BF16)] * 5, v((4, seq, hd), BF16),
            v((wid, 2 * hd), BF16), v((2, wid, hd), BF16), v((4, 2, wid, ffc), BF16),
            v((2 * hd, wid), BF16), v((4 * ffc, wid), BF16),
            v((8, 128), F32), v((4, 8, 128), F32), v((4, 24, 2 * hd), F32), v((4, 24, 2 * hd), F32),
            v((4, 16, 128), BF16), v((4, 16, 128), BF16), v((4, 8, hd), F32), v((8, hd), F32), v((8, hd), F32),
            v((4, 8, hd), F32), v((2, 8, seq), F32), v((2, 4, 8, 128), BF16), v((2, 16, 8, 128), BF16),
            v((4, 2, rows, ffc), F32), v((2, 2, rows, ffc), F32), v((2, rows, ffc), F32), v((2, rows, ffc), F32),
            v((4, rows, ffc), BF16), v((rows, wid), F32), v((4, 16, wid), F32), v((4, 16, wid), F32),
            v((16, 128), F32), v((4, 16, 128), F32), v((4, 16, wid), BF16),
            v((4, 16, vbp), F32), v((4, 16, vbp), F32), v((4, 16, vbp), F32), v((4, 16, vbp), F32),
            v((1, 16, chunks_a[0][1]), F32), v((4, 16, vbp), F32), v((4, 16, vbp), F32), v((4, 16, vbp), F32), v((4, 16, 128), F32),
            v((2, 128), F32), v((16, 2, 128), F32),
            dma((21,)), dma((16,)), dma((13,)), dma((nx,)), dma((nx,)), dma((nc,)), dma(()), pltpu.SemaphoreType.REGULAR, pltpu.SemaphoreType.REGULAR,
        ]
        kv, z, ln, lr = pl.pallas_call(
            functools.partial(step_kernel, sizes),
            name="decode_step",
            out_shape=(v((2, 8, hd), F32), v((rows, vb), F32), v((rows, 1), F32), v((1, rows), F32)),
            in_specs=[pl.BlockSpec(memory_space=pltpu.SMEM)] + [any_spec] * 14,
            out_specs=(vmem, vmem, vmem, vmem),
            scratch_shapes=scratch,
            compiler_params=pltpu.CompilerParams(collective_id=0, has_side_effects=True,
                                                 vmem_limit_bytes=67043328 - 900 * 1024),
        )(cache_len, hidden, jnp.asarray(inv_freq), k_cache, v_cache, g_attn.reshape(1, wid), w_query, w_key, w_value,
          w_gate, w_up, w_out, w_down, g_final.reshape(1, wid), embedding)
        k_new, v_new, log_probs, log_norm = pl.pallas_call(
            functools.partial(finish_kernel, own_rows),
            name="finish_step",
            out_shape=(jax.ShapeDtypeStruct((own_rows, hd), BF16), jax.ShapeDtypeStruct((own_rows, hd), BF16),
                       jax.ShapeDtypeStruct((rows, vb), F32), jax.ShapeDtypeStruct((1, rows), F32)),
            in_specs=[vmem] * 4,
            out_specs=(any_spec,) * 4,
            scratch_shapes=[v((own_rows, hd), BF16), v((own_rows, hd), BF16), v((rows, vb), F32), dma((11,))],
            compiler_params=pltpu.CompilerParams(vmem_limit_bytes=4 * 1024 * 1024),
        )(kv, z, ln, lr)
        return k_new, v_new, log_probs, log_norm[0]

    in_specs = (P("dp", "xax"), P("dp"), row_spec, row_spec, P("xax"), P("xax", "yax"),
                P("xax", None), P("xax", None), P("xax", "yax"), P("xax", "yax"),
                P("yax", "xax"), P("yax", "xax"), P("xax"), P("yax", "xax"))
    out_specs = (row_spec, row_spec, P("dp", ("yax", "xax")), P("dp"))
    return jax.shard_map(local_step, mesh=mesh, in_specs=in_specs, out_specs=out_specs, check_vma=False)
```

```python
import functools

import jax
import jax.numpy as jnp
import numpy as np
from jax import lax
from jax.experimental import pallas as pl
from jax.experimental.pallas import tpu as pltpu
from jax.sharding import PartitionSpec as P

EPS = 1e-6
ROPE_BASE = 10000.0
F32 = jnp.float32
BF16 = jnp.bfloat16
MESH = pl.DeviceIdType.MESH


def dot(a, b):
    return jnp.dot(a, b, preferred_element_type=F32)


def dot_t(a, b):
    return lax.dot_general(a, b, (((1,), (1,)), ((), ())), preferred_element_type=F32)


def one_hot_rows(rows, cols, source):
    r = lax.broadcasted_iota(jnp.int32, (rows, cols), 0)
    c = lax.broadcasted_iota(jnp.int32, (rows, cols), 1)
    return jnp.where(c == source(r), 1.0, 0.0).astype(BF16)


def step_kernel(sizes,
                lens, hidden_hbm, freq_hbm, k_hbm, v_hbm, ga_hbm, wq_hbm, wk_hbm, wv_hbm, wg_hbm, wu_hbm,
                wo_hbm, wd_hbm, gf_hbm, emb_hbm,
                kv_out, z_out, ln_out, lr_out,
                hid, freq, table, ga, gf, kb0, kb1, kb2, kb3, kb4, vbuf, wq, wkv, wgu, wo, wd,
                st_send, st_recv, qkv, qkv_recv, q_send, q_recv, qs, kns, vns, os_, sbuf, o_send, o_recv,
                gup, gu_recv, gux, gux_recv, m_all, mdown, resid, bpart, b_recv, s2_send, s2_recv, fbuf,
                lsend1, lrecv1, hold, xrecv, drecv, lsend2, lrecv2, own, lcol, l_send, l_recv,
                ld_sem, snd_sem, rcv_sem, l1_sem, lx_sem, l2_sem, d_sem, x_ok, y_ok):
    rows, wid, seq, hd, ffc, vb, chunks_a, chunks_b, chunks_c = sizes
    yi = lax.axis_index("yax")
    xi = lax.axis_index("xax")
    x1 = xi + 1 - 2 * (xi % 2)
    x2 = (xi + 2) % 4
    x3 = (x1 + 2) % 4
    me = yi * 4 + xi
    ypeers = [3 * (1 - yi // 2), 2 - yi // 2, yi + 1 - 2 * (yi % 2)]
    xpeers = [x1, x2, x3]

    def load(i, *pairs):
        for src, dst in pairs:
            pltpu.make_async_copy(src, dst, ld_sem.at[i]).start()

    def loaded(i, dst):
        pltpu.make_async_copy(dst, dst, ld_sem.at[i]).wait()

    HID, GA, FREQ, WQ, WKV, WGU, WD, WO, GF, KEY, VAL, EMB = 0, 1, 2, 3, 4, 5, 9, 10, 11, 12, 16, 20
    kb = (kb0, kb1, kb2, kb3, kb4)
    load(HID, (hidden_hbm, hid))
    load(GA, (ga_hbm, ga))
    barrier = pltpu.get_barrier_semaphore()
    odd = xi % 2 == 1
    even = xi % 2 == 0

    def signal(sem, yy, xx):
        pl.semaphore_signal(sem, inc=1, device_id={"yax": yy, "xax": xx}, device_id_type=MESH)

    @pl.when(odd)
    def _():
        signal(barrier, yi, x2)

    @pl.when(even)
    def _():
        signal(barrier, yi, x1)
        signal(barrier, yi, x3)

    load(FREQ, (freq_hbm, freq))
    load(WQ, (wq_hbm, wq))
    load(WKV, (wk_hbm, wkv.at[0]), (wv_hbm, wkv.at[1]))
    load(KEY, (k_hbm.at[0], kb[1]))
    for i, xx in enumerate((x1, x3, x2, xi)):
        cols = pl.ds(pl.multiple_of(xx * ffc, ffc), ffc)
        load(WGU + i, (wg_hbm.at[:, cols], wgu.at[xx, 0]), (wu_hbm.at[:, cols], wgu.at[xx, 1]))
    for j in range(1, 4):
        load(KEY + j, (k_hbm.at[j], kb[j + 1]))
    for j in range(4):
        load(VAL + j, (v_hbm.at[j], vbuf.at[j]))
    load(WD, (wd_hbm, wd))
    load(WO, (wo_hbm, wo))
    load(GF, (gf_hbm, gf))

    ST, QP, KVP, Q, GU, GUX, M, O1, O2, B1, B2, S2, FN, LSE, L1, LX, L2 = range(17)

    def send(src, dst, i, yy, xx, rsem=None):
        pltpu.make_async_remote_copy(src_ref=src, dst_ref=dst, send_sem=snd_sem.at[i],
                                     recv_sem=rcv_sem.at[i] if rsem is None else rsem,
                                     device_id={"yax": yy, "xax": xx}, device_id_type=MESH).start()

    def recv(dst, i):
        pltpu.make_async_copy(dst, dst, rcv_sem.at[i]).wait()

    def recv_chunk(dst, sem):
        pltpu.make_async_copy(dst, dst, sem).wait()

    def sent(src, i):
        pltpu.make_async_copy(src, src, snd_sem.at[i]).wait()

    three = pl.ds(0, 3)
    most = pl.ds(0, 15)

    tq = seq // 1024

    def transpose_keys(j, start, stop):
        if start == 0:
            loaded(KEY + j, kb[j + 1])

        def one(t, carry):
            at = pl.ds(pl.multiple_of(t * 256, 256), 256)
            kb[j][at] = kb[j + 1][at].T
            return carry

        lax.fori_loop(start * tq, stop * tq, one, 0, unroll=tq)

    loaded(HID, hid)
    loaded(GA, ga)
    h = hid[...].astype(F32)
    mean_l = jnp.sum(h, axis=1, keepdims=True) * (1.0 / wid)
    dev = h - mean_l
    m2_l = jnp.sum(dev * dev, axis=1, keepdims=True)
    lane = lax.broadcasted_iota(jnp.int32, (rows, 128), 1)
    stat = jnp.where(lane == 0, mean_l, m2_l)
    stat_t = jnp.concatenate([stat, stat], axis=0).T[:8]
    st_send[...] = stat_t

    @pl.when(odd)
    def _():
        pl.semaphore_wait(barrier, 3)
        signal(x_ok, yi, x1)

    @pl.when(even)
    def _():
        pl.semaphore_wait(x_ok, 1)
        for yy in ypeers:
            signal(barrier, yy, xi)

    for xx in xpeers:
        send(st_send, st_recv.at[xi], ST, yi, xx)
    perm = one_hot_rows(160, 64, lambda r: jnp.where(
        r >= 96, ((r % 32) // 2) * 4 + ((r - 96) // 32) * 2 + r % 2,
        jnp.where(r % 24 < 16, ((r % 24) // 4) * 16 + (r // 24) * 4 + r % 4,
                  jnp.where(r % 24 < 20, yi * 16 + (r // 24) * 4 + r % 4, -1))))
    loaded(FREQ, freq)
    prow = lax.broadcasted_iota(jnp.int32, (24, 128), 0)
    posn = jnp.zeros((24, 128), jnp.int32)
    for r in range(20):
        at = (r // 4) * 16 + xi * 4 + r % 4 if r < 16 else me * 4 + r - 16
        posn = jnp.where(prow == r, lens[at], posn)
    angle = posn.astype(F32) * freq[...]
    table[0] = jnp.cos(angle)
    table[1] = jnp.sin(angle)
    transpose_keys(0, 0, 2)
    recv(st_recv.at[three], ST)
    parts = [stat_t] + [st_recv[xx] for xx in xpeers]
    means = [p[0:1] for p in parts]
    mu = (means[0] + means[1] + means[2] + means[3]) * 0.25
    m2 = sum([p[1:2] for p in parts]) + wid * sum([(m - mu) * (m - mu) for m in means])
    rstd = lax.rsqrt(m2 * (1.0 / (4 * wid)) + EPS)
    sub = lax.broadcasted_iota(jnp.int32, (128, 128), 0)
    cols_t = jnp.where(sub == 0, mu, rstd).T
    mu_c = cols_t[:rows, 0:1]
    rstd_c = cols_t[:rows, 1:2]
    normed = ((h - mu_c) * rstd_c * ga[...]).astype(BF16)
    n_perm = dot(perm, normed).astype(BF16)

    loaded(WQ, wq)
    loaded(WKV, wkv)
    n_qkv, n_pair = n_perm[:96], n_perm[96:]
    q_part = dot(n_qkv, wq[...])
    kv_part = jnp.concatenate([dot(n_qkv, wkv[0]), dot(n_qkv, wkv[1])], axis=1)
    prow = lax.broadcasted_iota(jnp.int32, (96, 2 * hd), 0)
    qkv[...] = jnp.where(prow % 24 < 16, q_part, kv_part).reshape(4, 24, 2 * hd)
    q_rows, kv_rows = pl.ds(0, 16), pl.ds(16, 8)
    for xx in (x2, x3, x1):
        send(qkv.at[xx, q_rows], qkv_recv.at[xi, q_rows], QP, yi, xx)
    for xx in (x2, x3, x1):
        send(qkv.at[xx, kv_rows], qkv_recv.at[xi, kv_rows], KVP, yi, xx)

    for i, xx in enumerate((x1, x3, x2, xi)):
        loaded(WGU + i, wgu.at[xx])
        gup[xx, 0] = dot(n_pair, wgu[xx, 0])
        gup[xx, 1] = dot(n_pair, wgu[xx, 1])
        if i < 2:
            send(gup.at[xx], gu_recv.at[i], GU, yi, x1)

    transpose_keys(0, 2, 4)
    recv(gu_recv, GU)
    gux[...] = gup[x2] + gu_recv[1]
    send(gux, gux_recv, GUX, yi, x2)
    transpose_keys(1, 0, 4)
    transpose_keys(2, 0, 1)
    half = hd // 2
    recv(qkv_recv.at[three, q_rows], QP)

    def total(at):
        return ((qkv[xi, at] + qkv_recv[x1, at]) + (qkv_recv[x2, at] + qkv_recv[x3, at])).astype(BF16).astype(F32)

    def rotary(lo, hi, at):
        cos_a, sin_a = table[0, at], table[1, at]
        return (lo * cos_a - hi * sin_a).astype(BF16), (hi * cos_a + lo * sin_a).astype(BF16)

    tot = total(q_rows)
    lo0, hi0, lo1, hi1 = [tot[:, i * half:(i + 1) * half] for i in range(4)]
    r0, r1 = rotary(lo0, hi0, q_rows)
    r2, r3 = rotary(lo1, hi1, q_rows)
    stacked = jnp.concatenate([r0, r1, r2, r3], axis=0)
    s1 = one_hot_rows(64, 64, lambda r: ((r // 4) % 4) * 16 + (r // 16) * 4 + r % 4)
    q_send[...] = dot(s1, stacked).astype(BF16).reshape(4, 16, 128)

    @pl.when(even)
    def _():
        pl.semaphore_wait(barrier, 3)
        signal(y_ok, yi, x1)

    @pl.when(odd)
    def _():
        pl.semaphore_wait(y_ok, 1)

    for yy in ypeers:
        send(q_send.at[yy], q_recv.at[yi], Q, yy, xi)
    q_recv[yi] = q_send[yi]
    recv(qkv_recv.at[three, kv_rows], KVP)
    tot = total(kv_rows)
    r0, r1 = rotary(tot[:, :half], tot[:, half:hd], kv_rows)
    kns[:, :half] = r0.astype(F32)
    kns[:, half:] = r1.astype(F32)
    vns[...] = tot[:, hd:]
    kv_out[0] = kns[...]
    kv_out[1] = vns[...]

    transpose_keys(2, 1, 4)
    transpose_keys(3, 0, 4)
    recv(q_recv.at[three], Q)
    s2 = one_hot_rows(64, 64, lambda r: ((r // 2) % 4) * 16 + (r % 2) * 8 + (r // 32) * 4 + (r // 8) % 4)
    q_all = dot(s2, q_recv[...].reshape(64, 128))
    qs[...] = jnp.concatenate([q_all[:32], q_all[32:]], axis=1).reshape(4, 8, hd)

    scale = hd ** -0.5
    pos = lax.broadcasted_iota(jnp.int32, (8, seq), 1)

    def scores(j):
        qj = qs[j].astype(BF16)
        for t in range(seq // 256):
            at = pl.ds(t * 256, 256)
            sbuf[j % 2, :, at] = dot(qj, kb[j][at])

    def weights(j):
        s_new = jnp.sum(qs[j] * kns[j:j + 1, :], axis=1, keepdims=True) * scale
        s = jnp.where(pos < lens[me * 4 + j], sbuf[j % 2] * scale, -jnp.inf)
        top = jnp.maximum(jnp.max(s, axis=1, keepdims=True), s_new)
        w = jnp.exp(s - top)
        w_new = jnp.exp(s_new - top)
        inv = 1.0 / (jnp.sum(w, axis=1, keepdims=True) + w_new)
        return (w * inv).astype(BF16), (w_new * inv).astype(BF16).astype(F32)

    def mix(j, prob, p_new):
        hs = seq // 2
        acc = dot(prob[:, :hs], vbuf[j, :hs]) + dot(prob[:, hs:], vbuf[j, hs:])
        os_[j] = acc + p_new * vns[j:j + 1, :]

    s3 = one_hot_rows(32, 32, lambda r: ((r // 2) % 2) * 16 + (r % 2) * 8 + (r // 8) * 2 + (r // 4) % 2)

    def send_outputs(pair, i):
        o_bf = os_[2 * pair:2 * pair + 2].reshape(16, hd).astype(BF16)
        o_rows = dot(s3, jnp.concatenate([o_bf[:, :half], o_bf[:, half:]], axis=0))
        o_send[pair] = o_rows.reshape(4, 8, 128).astype(BF16)
        for yy in ypeers:
            for xx in (x3, x2, x1, xi):
                send(o_send.at[pair, yy], o_recv.at[pair, me], i, yy, xx)
        for xx in xpeers:
            send(o_send.at[pair, yi], o_recv.at[pair, me], i, yi, xx)
        o_recv[pair, me] = o_send[pair, yi]

    scores(0)
    scores(1)
    w0 = weights(0)
    loaded(VAL, vbuf.at[0])
    loaded(VAL + 1, vbuf.at[1])
    mix(0, *w0)
    scores(2)
    mix(1, *weights(1))
    send_outputs(0, O1)
    recv(gux_recv, GUX)
    gu = gup[xi] + gu_recv[0] + gux_recv[...]
    gate = gu[0].astype(BF16).astype(F32)
    up_val = gu[1].astype(BF16).astype(F32)
    m_all[xi] = (gate * jax.nn.sigmoid(gate) * up_val).astype(BF16)
    for xx in (x2, x3, x1):
        send(m_all.at[xi], m_all.at[xi], M, yi, xx)
    loaded(VAL + 2, vbuf.at[2])
    scores(3)
    mix(2, *weights(2))
    w3 = weights(3)
    loaded(VAL + 3, vbuf.at[3])
    mix(3, *w3)
    send_outputs(1, O2)
    for j in range(4):
        voc = pl.ds(j * vb, vb)
        load(EMB, (emb_hbm.at[voc, pl.ds(0, hd)], vbuf.at[j, pl.ds(0, vb)]),
             (emb_hbm.at[voc, pl.ds(hd, hd)], vbuf.at[j, pl.ds(seq // 2, vb)]))
    s5 = one_hot_rows(16, 16, lambda r: ((r % 8) // 2) * 4 + (r // 8) * 2 + r % 2)
    resid[...] = dot(s5, hid[pl.ds(pl.multiple_of(yi * 16, 16), 16), :])
    loaded(WD, wd)
    loaded(WO, wo)
    loaded(GF, gf)
    recv(m_all.at[three], M)
    mdown[...] = sum([dot(m_all[i], wd[pl.ds(i * ffc, ffc)]) for i in range(4)])
    s4 = one_hot_rows(128, 128, lambda r: ((r % 32) // 2) * 8 + (r // 32) * 2 + r % 2)

    def products(pair, i):
        o_rows = jnp.concatenate([o_recv[pair, k].astype(F32) for k in range(16)], axis=0)
        a_all = dot(s4, o_rows.astype(BF16)).astype(BF16)
        attn = jnp.concatenate([a_all[k * 32:(k + 1) * 32] for k in range(4)], axis=1)
        bpart[pair] = (dot(attn, wo[...]) + mdown[pl.ds(pair * 32, 32)]).reshape(4, 8, wid)
        for yy in ypeers:
            send(bpart.at[pair, yy], b_recv.at[pair, yi], i, yy, xi)

    recv(o_recv.at[0, most], O1)
    products(0, B1)
    recv(o_recv.at[1, most], O2)
    products(1, B2)
    recv(b_recv.at[0, three], B1)
    recv(b_recv.at[1, three], B2)
    res = resid[...] + jnp.concatenate([
        (bpart[p, yi] + b_recv[p, ypeers[0]]) + (b_recv[p, ypeers[1]] + b_recv[p, ypeers[2]]) for p in range(2)], axis=0)

    mean_l = jnp.sum(res, axis=1, keepdims=True) * (1.0 / wid)
    dev = res - mean_l
    m2_l = jnp.sum(dev * dev, axis=1, keepdims=True)
    lane = lax.broadcasted_iota(jnp.int32, (16, 128), 1)
    s2_send[...] = jnp.where(lane < 64, mean_l, m2_l)
    for xx in xpeers:
        send(s2_send, s2_recv.at[xi], S2, yi, xx)
    recv(s2_recv.at[three], S2)
    parts = [s2_recv[xx] for xx in xpeers]
    means = [mean_l] + [p[:, 0:1] for p in parts]
    mu = (means[0] + means[1] + means[2] + means[3]) * 0.25
    m2 = m2_l + sum([p[:, 64:65] for p in parts]) + wid * sum([(m - mu) * (m - mu) for m in means])
    rstd = lax.rsqrt(m2 * (1.0 / (4 * wid)) + EPS)
    s6 = one_hot_rows(16, 16, lambda r: ((r // 2) % 2) * 8 + (r // 4) * 2 + r % 2)
    f_own = dot(s6, ((res - mu) * rstd * gf[...]).astype(BF16)).astype(BF16)
    fbuf[yi] = f_own
    for yy in ypeers:
        send(fbuf.at[yi], fbuf.at[yi], FN, yy, xi)
    loaded(EMB, vbuf.at[:, pl.ds(0, 2 * vb)])

    def logit_part(f, xx, c0, cn):
        return dot_t(f[:, :hd], vbuf[xx, pl.ds(c0, cn)]) + dot_t(f[:, hd:], vbuf[xx, pl.ds(seq // 2 + c0, cn)])

    def cross(i, at):
        recv_chunk(lrecv1.at[at], l1_sem.at[i])
        hold[at] = hold[at] + lrecv1[at]
        send(hold.at[at], xrecv.at[at], LX, yi, x2, lx_sem.at[i])

    def cross_blocks(f, slots, chunks, first):
        n = f.shape[0] // 16
        prev = None
        for i, (c0, cn) in enumerate(chunks):
            at = (slots, slice(None), pl.ds(c0, cn))
            if first + i == 0:
                hold[at] = logit_part(f, x2, c0, cn).reshape(n, 16, cn)
                send(hold.at[at], xrecv.at[at], LX, yi, x2, lx_sem.at[0])
                lsend1[at] = logit_part(f, x3, c0, cn).reshape(n, 16, cn)
                send(lsend1.at[at], drecv, L1, yi, x3, d_sem)
                continue
            lsend1[at] = logit_part(f, x3, c0, cn).reshape(n, 16, cn)
            send(lsend1.at[at], lrecv1.at[at], L1, yi, x1, l1_sem.at[first + i])
            hold[at] = logit_part(f, x2, c0, cn).reshape(n, 16, cn)
            if prev is not None:
                cross(*prev)
            prev = (first + i, at)
        cross(*prev)

    slot_a = pl.ds(0, 1)
    slot_b = pl.ds(1, 3)
    na = len(chunks_a)
    cross_blocks(f_own, slot_a, chunks_a, 0)
    recv(fbuf.at[three], FN)
    f_rest = jnp.concatenate([fbuf[yy] for yy in ypeers], axis=0)
    cross_blocks(f_rest, slot_b, chunks_b, na)
    f_all = jnp.concatenate([f_own, f_rest], axis=0)
    for i, (c0, cn) in enumerate(chunks_c):
        at = (slice(None), slice(None), pl.ds(c0, cn))
        lsend2[at] = logit_part(f_all, x1, c0, cn).reshape(4, 16, cn)
        send(lsend2.at[at], lrecv2.at[at], L2, yi, x1, l2_sem.at[i])
        own[at] = logit_part(f_all, xi, c0, cn).reshape(4, 16, cn)
    recv_chunk(lrecv2, l2_sem.at[0]) if len(chunks_c) == 1 else [
        recv_chunk(lrecv2.at[:, :, pl.ds(c0, cn)], l2_sem.at[i]) for i, (c0, cn) in enumerate(chunks_c)]
    tops, totals = {}, {}
    order = [yi] + ypeers
    for d in range(4):
        tops[d] = jnp.full((16, 1), -jnp.inf, F32)
        totals[d] = jnp.zeros((16, 1), F32)
    for chunks, slots, ds, first in ((chunks_a, slot_a, (0,), 0), (chunks_b, slot_b, (1, 2, 3), na)):
        for i, (c0, cn) in enumerate(chunks):
            recv_chunk(xrecv.at[slots, :, pl.ds(c0, cn)], lx_sem.at[first + i])
            if first + i == 0:
                recv_chunk(drecv, d_sem)
            cs = pl.ds(c0, cn)
            for d in ds:
                row = pl.ds(pl.multiple_of(order[d] * 16, 16), 16)
                z = own[d, :, cs] + lrecv2[d, :, cs] + xrecv[d, :, cs]
                if first + i == 0:
                    z = z + drecv[0]
                if c0 + cn > vb:
                    z_out[row, c0:vb] = z[:, :vb - c0]
                    z = jnp.where(lax.broadcasted_iota(jnp.int32, (16, cn), 1) < vb - c0, z, -jnp.inf)
                else:
                    z_out[row, cs] = z
                m_new = jnp.maximum(tops[d], jnp.max(z, axis=1, keepdims=True))
                totals[d] = totals[d] * jnp.exp(tops[d] - m_new) + jnp.sum(jnp.exp(z - m_new), axis=1, keepdims=True)
                tops[d] = m_new
    lane = lax.broadcasted_iota(jnp.int32, (16, 128), 1)
    for d in range(4):
        lcol[order[d]] = jnp.where(lane == 0, tops[d], totals[d])

    stat = lcol[...].reshape(rows, 128)
    mine = jnp.concatenate([stat, stat], axis=0).T[0:2]
    l_send[...] = mine
    for yy in ypeers:
        for xx in (x3, x2, x1, xi):
            send(l_send, l_recv.at[me], LSE, yy, xx)
    for xx in xpeers:
        send(l_send, l_recv.at[me], LSE, yi, xx)
    l_recv[me] = mine
    sent(st_recv.at[three], ST)
    sent(qkv.at[three, q_rows], QP)
    sent(qkv.at[three, kv_rows], KVP)
    sent(q_send.at[three], Q)
    sent(gu_recv, GU)
    sent(gux, GUX)
    sent(m_all.at[three], M)
    sent(o_recv.at[0, most], O1)
    sent(o_recv.at[1, most], O2)
    sent(bpart.at[0, three], B1)
    sent(bpart.at[1, three], B2)
    sent(s2_recv.at[three], S2)
    sent(fbuf.at[three], FN)
    sent(lsend1, L1)
    sent(hold, LX)
    sent(lsend2, L2)
    recv(l_recv.at[most], LSE)
    tops = [l_recv[i, 0:1, :] for i in range(16)]
    top = functools.reduce(jnp.maximum, tops)
    total = sum([l_recv[i, 1:2, :] * jnp.exp(tops[i] - top) for i in range(16)])
    log_norm = top + jnp.log(total)
    lr_out[...] = log_norm[:, :rows]
    ln_out[...] = jnp.broadcast_to(log_norm, (128, 128)).T[:rows, 0:1]
    sent(l_recv.at[most], LSE)


def finish_kernel(own_rows, kv, z, ln, lr, k_out, v_out, lp_out, ln_out, k_s, v_s, lp_s, sem):
    k_s[...] = kv[0].astype(BF16)[:own_rows]
    v_s[...] = kv[1].astype(BF16)[:own_rows]
    copies = [pltpu.make_async_copy(k_s, k_out, sem.at[0]), pltpu.make_async_copy(v_s, v_out, sem.at[1]),
              pltpu.make_async_copy(lr, ln_out, sem.at[2])]
    for cp in copies:
        cp.start()
    for i in range(z.shape[0] // 8):
        at = pl.ds(i * 8, 8)
        lp_s[at] = z[at] - ln[at]
        copies.append(pltpu.make_async_copy(lp_s.at[at], lp_out.at[at], sem.at[3 + i]))
        copies[-1].start()
    for cp in copies:
        cp.wait()


def solution(mesh):
    row_spec = P(("dp", "yax", "xax"))

    def local_step(hidden, cache_len, k_cache, v_cache, g_attn, w_query, w_key, w_value,
                   w_gate, w_up, w_out, w_down, g_final, embedding):
        rows, wid = hidden.shape
        own_rows, seq, hd = k_cache.shape
        ffc = w_gate.shape[1] // 4
        vb = embedding.shape[0] // 4
        inv_freq = np.power(ROPE_BASE, -2.0 * np.arange(hd // 2) / hd).astype(np.float32).reshape(1, hd // 2)
        vbp = -(-vb // 128) * 128
        def cut(step, start=0):
            return [(c, min(step, vbp - c)) for c in range(start, vbp, step)]

        chunks_a = [(0, 512)] + cut(768, 512)
        chunks_b, chunks_c = cut(768), cut(1792)
        nx, nc = len(chunks_a) + len(chunks_b), len(chunks_c)
        sizes = (rows, wid, seq, hd, ffc, vb, chunks_a, chunks_b, chunks_c)
        any_spec = pl.BlockSpec(memory_space=pltpu.HBM)
        vmem = pl.BlockSpec(memory_space=pltpu.VMEM)
        v = pltpu.VMEM
        dma = pltpu.SemaphoreType.DMA
        scratch = [
            v((rows, wid), BF16), v((1, hd // 2), F32), v((2, 24, hd // 2), F32), v((1, wid), F32), v((1, wid), F32),
            *[v((seq, hd), BF16)] * 5, v((4, seq, hd), BF16),
            v((wid, 2 * hd), BF16), v((2, wid, hd), BF16), v((4, 2, wid, ffc), BF16),
            v((2 * hd, wid), BF16), v((4 * ffc, wid), BF16),
            v((8, 128), F32), v((4, 8, 128), F32), v((4, 24, 2 * hd), F32), v((4, 24, 2 * hd), F32),
            v((4, 16, 128), BF16), v((4, 16, 128), BF16), v((4, 8, hd), F32), v((8, hd), F32), v((8, hd), F32),
            v((4, 8, hd), F32), v((2, 8, seq), F32), v((2, 4, 8, 128), BF16), v((2, 16, 8, 128), BF16),
            v((4, 2, rows, ffc), F32), v((2, 2, rows, ffc), F32), v((2, rows, ffc), F32), v((2, rows, ffc), F32),
            v((4, rows, ffc), BF16), v((rows, wid), F32), v((16, wid), F32), v((2, 4, 8, wid), F32), v((2, 4, 8, wid), F32),
            v((16, 128), F32), v((4, 16, 128), F32), v((4, 16, wid), BF16),
            v((4, 16, vbp), F32), v((4, 16, vbp), F32), v((4, 16, vbp), F32), v((4, 16, vbp), F32),
            v((1, 16, chunks_a[0][1]), F32), v((4, 16, vbp), F32), v((4, 16, vbp), F32), v((4, 16, vbp), F32), v((4, 16, 128), F32),
            v((2, 128), F32), v((16, 2, 128), F32),
            dma((21,)), dma((17,)), dma((14,)), dma((nx,)), dma((nx,)), dma((nc,)), dma(()), pltpu.SemaphoreType.REGULAR, pltpu.SemaphoreType.REGULAR,
        ]
        kv, z, ln, lr = pl.pallas_call(
            functools.partial(step_kernel, sizes),
            name="decode_step",
            out_shape=(v((2, 8, hd), F32), v((rows, vb), F32), v((rows, 1), F32), v((1, rows), F32)),
            in_specs=[pl.BlockSpec(memory_space=pltpu.SMEM)] + [any_spec] * 14,
            out_specs=(vmem, vmem, vmem, vmem),
            scratch_shapes=scratch,
            compiler_params=pltpu.CompilerParams(collective_id=0, has_side_effects=True,
                                                 vmem_limit_bytes=67043328 - 900 * 1024),
        )(cache_len, hidden, jnp.asarray(inv_freq), k_cache, v_cache, g_attn.reshape(1, wid), w_query, w_key, w_value,
          w_gate, w_up, w_out, w_down, g_final.reshape(1, wid), embedding)
        k_new, v_new, log_probs, log_norm = pl.pallas_call(
            functools.partial(finish_kernel, own_rows),
            name="finish_step",
            out_shape=(jax.ShapeDtypeStruct((own_rows, hd), BF16), jax.ShapeDtypeStruct((own_rows, hd), BF16),
                       jax.ShapeDtypeStruct((rows, vb), F32), jax.ShapeDtypeStruct((1, rows), F32)),
            in_specs=[vmem] * 4,
            out_specs=(any_spec,) * 4,
            scratch_shapes=[v((own_rows, hd), BF16), v((own_rows, hd), BF16), v((rows, vb), F32), dma((11,))],
            compiler_params=pltpu.CompilerParams(vmem_limit_bytes=4 * 1024 * 1024),
        )(kv, z, ln, lr)
        return k_new, v_new, log_probs, log_norm[0]

    in_specs = (P("dp", "xax"), P("dp"), row_spec, row_spec, P("xax"), P("xax", "yax"),
                P("xax", None), P("xax", None), P("xax", "yax"), P("xax", "yax"),
                P("yax", "xax"), P("yax", "xax"), P("xax"), P("yax", "xax"))
    out_specs = (row_spec, row_spec, P("dp", ("yax", "xax")), P("dp"))
    return jax.shard_map(local_step, mesh=mesh, in_specs=in_specs, out_specs=out_specs, check_vma=False)
```

```python
import functools

import jax
import jax.numpy as jnp
import numpy as np
from jax import lax
from jax.experimental import pallas as pl
from jax.experimental.pallas import tpu as pltpu
from jax.sharding import PartitionSpec as P

EPS = 1e-6
ROPE_BASE = 10000.0
F32 = jnp.float32
BF16 = jnp.bfloat16
MESH = pl.DeviceIdType.MESH


def dot(a, b):
    return jnp.dot(a, b, preferred_element_type=F32)


def dot_t(a, b):
    return lax.dot_general(a, b, (((1,), (1,)), ((), ())), preferred_element_type=F32)


def one_hot_rows(rows, cols, source):
    r = lax.broadcasted_iota(jnp.int32, (rows, cols), 0)
    c = lax.broadcasted_iota(jnp.int32, (rows, cols), 1)
    return jnp.where(c == source(r), 1.0, 0.0).astype(BF16)


def step_kernel(sizes,
                lens, hidden_hbm, freq_hbm, k_hbm, v_hbm, ga_hbm, wq_hbm, wk_hbm, wv_hbm, wg_hbm, wu_hbm,
                wo_hbm, wd_hbm, gf_hbm, emb_hbm,
                kv_out, z_out, ln_out, lr_out,
                hid, small, table, kb0, kb1, kb2, kb3, kb4, vbuf, wqkv, wgu, wdo,
                st_send, st_recv, qkv, qkv_recv, q_send, q_recv, qs, kns, vns, os_, sbuf, o_send, o_recv,
                gup, gu_recv, gux, gux_recv, m_all, mdown, resid, bpart, b_recv, s2_send, s2_recv, fbuf,
                lbuf, lrecv1, xrecv, drecv, lrecv2, own, lcol, l_send, l_recv,
                ld_sem, snd_sem, rcv_sem, l1_sem, lx_sem, l2_sem, d_sem, x_ok, y_ok):
    rows, wid, seq, hd, ffc, vb, chunks_a, chunks_b, chunks_c = sizes
    yi = lax.axis_index("yax")
    xi = lax.axis_index("xax")
    x1 = xi + 1 - 2 * (xi % 2)
    x2 = (xi + 2) % 4
    x3 = (x1 + 2) % 4
    me = yi * 4 + xi
    ypeers = [3 * (1 - yi // 2), 2 - yi // 2, yi + 1 - 2 * (yi % 2)]
    xpeers = [x1, x2, x3]

    def load(i, *pairs):
        for src, dst in pairs:
            pltpu.make_async_copy(src, dst, ld_sem.at[i]).start()

    def loaded(i, dst):
        pltpu.make_async_copy(dst, dst, ld_sem.at[i]).wait()

    HID, SMALL, WQKV, WGU, WDO, KEY0, KEY1, KEY2, VAL0, VAL2, VAL3, EMB = range(12)
    ga, freq, gf = small.at[:, :wid], small.at[:, wid:wid + hd // 2], small.at[:, wid + hd // 2:]
    kb = (kb0, kb1, kb2, kb3, kb4)
    wd, wo = wdo.at[:4 * ffc], wdo.at[4 * ffc:]
    load(HID, (hidden_hbm, hid))
    load(SMALL, (ga_hbm, ga), (freq_hbm, freq), (gf_hbm, gf))
    barrier = pltpu.get_barrier_semaphore()
    odd = xi % 2 == 1
    even = xi % 2 == 0

    def signal(sem, yy, xx):
        pl.semaphore_signal(sem, inc=1, device_id={"yax": yy, "xax": xx}, device_id_type=MESH)

    @pl.when(odd)
    def _():
        signal(barrier, yi, x2)

    @pl.when(even)
    def _():
        signal(barrier, yi, x1)
        signal(barrier, yi, x3)

    load(WQKV, (wq_hbm, wqkv.at[0]), (wk_hbm, wqkv.at[1, :, :hd]), (wv_hbm, wqkv.at[1, :, hd:]))
    load(KEY0, (k_hbm.at[0], kb[1]))
    for i, xx in enumerate((x1, x3, x2, xi)):
        cols = pl.ds(pl.multiple_of(xx * ffc, ffc), ffc)
        load(WGU, (wg_hbm.at[:, cols], wgu.at[xx, 0]), (wu_hbm.at[:, cols], wgu.at[xx, 1]))
    load(KEY1, (k_hbm.at[1], kb[2]))
    load(KEY2, (k_hbm.at[2], kb[3]), (k_hbm.at[3], kb[4]))
    load(VAL0, (v_hbm.at[0], vbuf.at[0]), (v_hbm.at[1], vbuf.at[1]))
    load(VAL2, (v_hbm.at[2], vbuf.at[2]))
    load(VAL3, (v_hbm.at[3], vbuf.at[3]))
    load(WDO, (wd_hbm, wd), (wo_hbm, wo))

    ST, QP, KVP, Q, GU, GUX, M, O1, O2, B1, B2, S2, FN, LSE, L1, LX, L2 = range(17)

    snd = {ST: 0, S2: 0, QP: 1, KVP: 1, FN: 1, Q: 2, O1: 2, O2: 2, GU: 3, B1: 3, B2: 3, GUX: 4, LSE: 4, M: 5,
           L1: 5, LX: 5, L2: 5}

    def send(src, dst, i, yy, xx, rsem=None):
        pltpu.make_async_remote_copy(src_ref=src, dst_ref=dst, send_sem=snd_sem.at[snd[i]],
                                     recv_sem=rcv_sem.at[i] if rsem is None else rsem,
                                     device_id={"yax": yy, "xax": xx}, device_id_type=MESH).start()

    def recv(dst, i):
        pltpu.make_async_copy(dst, dst, rcv_sem.at[i]).wait()

    def recv_chunk(dst, sem):
        pltpu.make_async_copy(dst, dst, sem).wait()

    def sent(src, i):
        pltpu.make_async_copy(src, src, snd_sem.at[snd[i]]).wait()

    three = pl.ds(0, 3)
    most = pl.ds(0, 15)

    tq = seq // 1024

    def transpose_keys(j, start, stop):
        if start == 0 and j < 2:
            loaded((KEY0, KEY1)[j], kb[j + 1])
        elif start == 0 and j == 2:
            loaded(KEY2, vbuf.at[pl.ds(0, 2)])

        def one(t, carry):
            at = pl.ds(pl.multiple_of(t * 256, 256), 256)
            kb[j][at] = kb[j + 1][at].T
            return carry

        lax.fori_loop(start * tq, stop * tq, one, 0, unroll=tq)

    loaded(HID, hid)
    loaded(SMALL, small)
    h = hid[...].astype(F32)
    mean_l = jnp.sum(h, axis=1, keepdims=True) * (1.0 / wid)
    dev = h - mean_l
    m2_l = jnp.sum(dev * dev, axis=1, keepdims=True)
    lane = lax.broadcasted_iota(jnp.int32, (rows, 128), 1)
    stat = jnp.where(lane == 0, mean_l, m2_l)
    stat_t = jnp.concatenate([stat, stat], axis=0).T[:8]
    st_send[...] = stat_t

    @pl.when(odd)
    def _():
        pl.semaphore_wait(barrier, 3)
        signal(x_ok, yi, x1)

    @pl.when(even)
    def _():
        pl.semaphore_wait(x_ok, 1)
        for yy in ypeers:
            signal(barrier, yy, xi)

    for xx in xpeers:
        send(st_send, st_recv.at[xi], ST, yi, xx)
    perm = one_hot_rows(160, 64, lambda r: jnp.where(
        r >= 96, ((r % 32) // 2) * 4 + ((r - 96) // 32) * 2 + r % 2,
        jnp.where(r % 24 < 16, ((r % 24) // 4) * 16 + (r // 24) * 4 + r % 4,
                  jnp.where(r % 24 < 20, yi * 16 + (r // 24) * 4 + r % 4, -1))))
    prow = lax.broadcasted_iota(jnp.int32, (24, 128), 0)
    posn = jnp.zeros((24, 128), jnp.int32)
    for r in range(20):
        at = (r // 4) * 16 + xi * 4 + r % 4 if r < 16 else me * 4 + r - 16
        posn = jnp.where(prow == r, lens[at], posn)
    angle = posn.astype(F32) * freq[...]
    table[0] = jnp.cos(angle)
    table[1] = jnp.sin(angle)
    transpose_keys(0, 0, 2)
    recv(st_recv.at[three], ST)
    parts = [stat_t] + [st_recv[xx] for xx in xpeers]
    means = [p[0:1] for p in parts]
    mu = (means[0] + means[1] + means[2] + means[3]) * 0.25
    m2 = sum([p[1:2] for p in parts]) + wid * sum([(m - mu) * (m - mu) for m in means])
    rstd = lax.rsqrt(m2 * (1.0 / (4 * wid)) + EPS)
    sub = lax.broadcasted_iota(jnp.int32, (128, 128), 0)
    cols_t = jnp.where(sub == 0, mu, rstd).T
    mu_c = cols_t[:rows, 0:1]
    rstd_c = cols_t[:rows, 1:2]
    normed = ((h - mu_c) * rstd_c * ga[...]).astype(BF16)
    n_perm = dot(perm, normed).astype(BF16)

    loaded(WQKV, wqkv)
    n_qkv, n_pair = n_perm[:96], n_perm[96:]
    q_part = dot(n_qkv, wqkv[0])
    kv_part = dot(n_qkv, wqkv[1])
    prow = lax.broadcasted_iota(jnp.int32, (96, 2 * hd), 0)
    qkv[...] = jnp.where(prow % 24 < 16, q_part, kv_part).reshape(4, 24, 2 * hd)
    q_rows, kv_rows = pl.ds(0, 16), pl.ds(16, 8)
    for xx in (x2, x3, x1):
        send(qkv.at[xx, q_rows], qkv_recv.at[xi, q_rows], QP, yi, xx)
    for xx in (x2, x3, x1):
        send(qkv.at[xx, kv_rows], qkv_recv.at[xi, kv_rows], KVP, yi, xx)

    for i, xx in enumerate((x1, x3, x2, xi)):
        if i == 0:
            loaded(WGU, wgu)
        gup[xx, 0] = dot(n_pair, wgu[xx, 0])
        gup[xx, 1] = dot(n_pair, wgu[xx, 1])
        if i < 2:
            send(gup.at[xx], gu_recv.at[i], GU, yi, x1)

    transpose_keys(0, 2, 4)
    recv(gu_recv, GU)
    gux[...] = gup[x2] + gu_recv[1]
    send(gux, gux_recv, GUX, yi, x2)
    transpose_keys(1, 0, 4)
    transpose_keys(2, 0, 1)
    half = hd // 2
    recv(qkv_recv.at[three, q_rows], QP)

    def total(at):
        return ((qkv[xi, at] + qkv_recv[x1, at]) + (qkv_recv[x2, at] + qkv_recv[x3, at])).astype(BF16).astype(F32)

    def rotary(lo, hi, at):
        cos_a, sin_a = table[0, at], table[1, at]
        return (lo * cos_a - hi * sin_a).astype(BF16), (hi * cos_a + lo * sin_a).astype(BF16)

    tot = total(q_rows)
    lo0, hi0, lo1, hi1 = [tot[:, i * half:(i + 1) * half] for i in range(4)]
    r0, r1 = rotary(lo0, hi0, q_rows)
    r2, r3 = rotary(lo1, hi1, q_rows)
    stacked = jnp.concatenate([r0, r1, r2, r3], axis=0)
    s1 = one_hot_rows(64, 64, lambda r: ((r // 4) % 4) * 16 + (r // 16) * 4 + r % 4)
    q_send[...] = dot(s1, stacked).astype(BF16).reshape(4, 16, 128)

    @pl.when(even)
    def _():
        pl.semaphore_wait(barrier, 3)
        signal(y_ok, yi, x1)

    @pl.when(odd)
    def _():
        pl.semaphore_wait(y_ok, 1)

    for yy in ypeers:
        send(q_send.at[yy], q_recv.at[yi], Q, yy, xi)
    q_recv[yi] = q_send[yi]
    recv(qkv_recv.at[three, kv_rows], KVP)
    tot = total(kv_rows)
    r0, r1 = rotary(tot[:, :half], tot[:, half:hd], kv_rows)
    kns[:, :half] = r0.astype(F32)
    kns[:, half:] = r1.astype(F32)
    vns[...] = tot[:, hd:]
    kv_out[0] = kns[...]
    kv_out[1] = vns[...]

    transpose_keys(2, 1, 4)
    transpose_keys(3, 0, 4)
    recv(q_recv.at[three], Q)
    s2 = one_hot_rows(64, 64, lambda r: ((r // 2) % 4) * 16 + (r % 2) * 8 + (r // 32) * 4 + (r // 8) % 4)
    q_all = dot(s2, q_recv[...].reshape(64, 128))
    qs[...] = jnp.concatenate([q_all[:32], q_all[32:]], axis=1).reshape(4, 8, hd)

    scale = hd ** -0.5
    pos = lax.broadcasted_iota(jnp.int32, (8, seq), 1)

    def scores(j):
        qj = qs[j].astype(BF16)
        for t in range(seq // 256):
            at = pl.ds(t * 256, 256)
            sbuf[j % 2, :, at] = dot(qj, kb[j][at])

    def weights(j):
        s_new = jnp.sum(qs[j] * kns[j:j + 1, :], axis=1, keepdims=True) * scale
        s = jnp.where(pos < lens[me * 4 + j], sbuf[j % 2] * scale, -jnp.inf)
        top = jnp.maximum(jnp.max(s, axis=1, keepdims=True), s_new)
        w = jnp.exp(s - top)
        w_new = jnp.exp(s_new - top)
        inv = 1.0 / (jnp.sum(w, axis=1, keepdims=True) + w_new)
        return (w * inv).astype(BF16), (w_new * inv).astype(BF16).astype(F32)

    def mix(j, prob, p_new):
        hs = seq // 2
        acc = dot(prob[:, :hs], vbuf[j, :hs]) + dot(prob[:, hs:], vbuf[j, hs:])
        os_[j] = acc + p_new * vns[j:j + 1, :]

    s3 = one_hot_rows(32, 32, lambda r: ((r // 2) % 2) * 16 + (r % 2) * 8 + (r // 8) * 2 + (r // 4) % 2)

    sent(q_send.at[three], Q)
    sent(gu_recv, GU)
    sent(qkv.at[three], QP)

    def send_outputs(pair, i):
        o_bf = os_[2 * pair:2 * pair + 2].reshape(16, hd).astype(BF16)
        o_rows = dot(s3, jnp.concatenate([o_bf[:, :half], o_bf[:, half:]], axis=0))
        o_send[pair] = o_rows.reshape(4, 8, 128).astype(BF16)
        for yy in ypeers:
            for xx in (x3, x2, x1, xi):
                send(o_send.at[pair, yy], o_recv.at[pair, me], i, yy, xx)
        for xx in xpeers:
            send(o_send.at[pair, yi], o_recv.at[pair, me], i, yi, xx)
        o_recv[pair, me] = o_send[pair, yi]

    scores(0)
    scores(1)
    w0 = weights(0)
    loaded(VAL0, vbuf.at[pl.ds(0, 2)])
    mix(0, *w0)
    scores(2)
    mix(1, *weights(1))
    send_outputs(0, O1)
    recv(gux_recv, GUX)
    gu = gup[xi] + gu_recv[0] + gux_recv[...]
    gate = gu[0].astype(BF16).astype(F32)
    up_val = gu[1].astype(BF16).astype(F32)
    m_all[xi] = (gate * jax.nn.sigmoid(gate) * up_val).astype(BF16)
    for xx in (x2, x3, x1):
        send(m_all.at[xi], m_all.at[xi], M, yi, xx)
    loaded(VAL2, vbuf.at[2])
    scores(3)
    mix(2, *weights(2))
    w3 = weights(3)
    loaded(VAL3, vbuf.at[3])
    mix(3, *w3)
    send_outputs(1, O2)
    for j in range(4):
        voc = pl.ds(j * vb, vb)
        load(EMB, (emb_hbm.at[voc, pl.ds(0, hd)], vbuf.at[j, pl.ds(0, vb)]),
             (emb_hbm.at[voc, pl.ds(hd, hd)], vbuf.at[j, pl.ds(seq // 2, vb)]))
    s5 = one_hot_rows(16, 16, lambda r: ((r % 8) // 2) * 4 + (r // 8) * 2 + r % 2)
    resid[...] = dot(s5, hid[pl.ds(pl.multiple_of(yi * 16, 16), 16), :])
    loaded(WDO, wdo)
    recv(m_all.at[three], M)
    mdown[...] = sum([dot(m_all[i], wd[pl.ds(i * ffc, ffc)]) for i in range(4)])
    s4 = one_hot_rows(128, 128, lambda r: ((r % 32) // 2) * 8 + (r // 32) * 2 + r % 2)

    def products(pair, i):
        o_rows = jnp.concatenate([o_recv[pair, k].astype(F32) for k in range(16)], axis=0)
        a_all = dot(s4, o_rows.astype(BF16)).astype(BF16)
        attn = jnp.concatenate([a_all[k * 32:(k + 1) * 32] for k in range(4)], axis=1)
        bpart[pair] = (dot(attn, wo[...]) + mdown[pl.ds(pair * 32, 32)]).reshape(4, 8, wid)
        for yy in ypeers:
            send(bpart.at[pair, yy], b_recv.at[pair, yi], i, yy, xi)

    recv(o_recv.at[0, most], O1)
    products(0, B1)
    recv(o_recv.at[1, most], O2)
    products(1, B2)
    recv(b_recv.at[0, three], B1)
    recv(b_recv.at[1, three], B2)
    res = resid[...] + jnp.concatenate([
        (bpart[p, yi] + b_recv[p, ypeers[0]]) + (b_recv[p, ypeers[1]] + b_recv[p, ypeers[2]]) for p in range(2)], axis=0)

    mean_l = jnp.sum(res, axis=1, keepdims=True) * (1.0 / wid)
    dev = res - mean_l
    m2_l = jnp.sum(dev * dev, axis=1, keepdims=True)
    lane = lax.broadcasted_iota(jnp.int32, (16, 128), 1)
    s2_send[...] = jnp.where(lane < 64, mean_l, m2_l)
    sent(st_recv.at[three], ST)
    sent(gux, GUX)
    sent(m_all.at[three], M)
    for xx in xpeers:
        send(s2_send, s2_recv.at[xi], S2, yi, xx)
    recv(s2_recv.at[three], S2)
    parts = [s2_recv[xx] for xx in xpeers]
    means = [mean_l] + [p[:, 0:1] for p in parts]
    mu = (means[0] + means[1] + means[2] + means[3]) * 0.25
    m2 = m2_l + sum([p[:, 64:65] for p in parts]) + wid * sum([(m - mu) * (m - mu) for m in means])
    rstd = lax.rsqrt(m2 * (1.0 / (4 * wid)) + EPS)
    s6 = one_hot_rows(16, 16, lambda r: ((r // 2) % 2) * 8 + (r // 4) * 2 + r % 2)
    f_own = dot(s6, ((res - mu) * rstd * gf[...]).astype(BF16)).astype(BF16)
    fbuf[yi] = f_own
    for yy in ypeers:
        send(fbuf.at[yi], fbuf.at[yi], FN, yy, xi)
    loaded(EMB, vbuf.at[:, pl.ds(0, 2 * vb)])

    lsend1, hold, lsend2 = lbuf.at[0], lbuf.at[1], lbuf.at[2]

    def logit_part(f, xx, c0, cn):
        return dot_t(f[:, :hd], vbuf[xx, pl.ds(c0, cn)]) + dot_t(f[:, hd:], vbuf[xx, pl.ds(seq // 2 + c0, cn)])

    def cross(i, at):
        recv_chunk(lrecv1.at[at], l1_sem.at[i - 1])
        hold[at] = hold[at] + lrecv1[at]
        send(hold.at[at], xrecv.at[at], LX, yi, x2, lx_sem.at[i])

    def cross_blocks(f, slots, chunks, first):
        n = f.shape[0] // 16
        prev = None
        for i, (c0, cn) in enumerate(chunks):
            at = (slots, slice(None), pl.ds(c0, cn))
            if first + i == 0:
                hold[at] = logit_part(f, x2, c0, cn).reshape(n, 16, cn)
                send(hold.at[at], xrecv.at[at], LX, yi, x2, lx_sem.at[0])
                lsend1[at] = logit_part(f, x3, c0, cn).reshape(n, 16, cn)
                send(lsend1.at[at], drecv, L1, yi, x3, d_sem)
                continue
            lsend1[at] = logit_part(f, x3, c0, cn).reshape(n, 16, cn)
            send(lsend1.at[at], lrecv1.at[at], L1, yi, x1, l1_sem.at[first + i - 1])
            hold[at] = logit_part(f, x2, c0, cn).reshape(n, 16, cn)
            if prev is not None:
                cross(*prev)
            prev = (first + i, at)
        cross(*prev)

    slot_a = pl.ds(0, 1)
    slot_b = pl.ds(1, 3)
    na = len(chunks_a)
    cross_blocks(f_own, slot_a, chunks_a, 0)
    recv(fbuf.at[three], FN)
    f_rest = jnp.concatenate([fbuf[yy] for yy in ypeers], axis=0)
    cross_blocks(f_rest, slot_b, chunks_b, na)
    f_all = jnp.concatenate([f_own, f_rest], axis=0)
    for i, (c0, cn) in enumerate(chunks_c):
        at = (slice(None), slice(None), pl.ds(c0, cn))
        lsend2[at] = logit_part(f_all, x1, c0, cn).reshape(4, 16, cn)
        send(lsend2.at[at], lrecv2.at[at], L2, yi, x1, l2_sem.at[i])
        own[at] = logit_part(f_all, xi, c0, cn).reshape(4, 16, cn)
    recv_chunk(lrecv2, l2_sem.at[0]) if len(chunks_c) == 1 else [
        recv_chunk(lrecv2.at[:, :, pl.ds(c0, cn)], l2_sem.at[i]) for i, (c0, cn) in enumerate(chunks_c)]
    tops, totals = {}, {}
    order = [yi] + ypeers
    for d in range(4):
        tops[d] = jnp.full((16, 1), -jnp.inf, F32)
        totals[d] = jnp.zeros((16, 1), F32)
    for chunks, slots, ds, first in ((chunks_a, slot_a, (0,), 0), (chunks_b, slot_b, (1, 2, 3), na)):
        for i, (c0, cn) in enumerate(chunks):
            recv_chunk(xrecv.at[slots, :, pl.ds(c0, cn)], lx_sem.at[first + i])
            if first + i == 0:
                recv_chunk(drecv, d_sem)
            cs = pl.ds(c0, cn)
            for d in ds:
                row = pl.ds(pl.multiple_of(order[d] * 16, 16), 16)
                z = own[d, :, cs] + lrecv2[d, :, cs] + xrecv[d, :, cs]
                if first + i == 0:
                    z = z + drecv[0]
                if c0 + cn > vb:
                    z_out[row, c0:vb] = z[:, :vb - c0]
                    z = jnp.where(lax.broadcasted_iota(jnp.int32, (16, cn), 1) < vb - c0, z, -jnp.inf)
                else:
                    z_out[row, cs] = z
                m_new = jnp.maximum(tops[d], jnp.max(z, axis=1, keepdims=True))
                totals[d] = totals[d] * jnp.exp(tops[d] - m_new) + jnp.sum(jnp.exp(z - m_new), axis=1, keepdims=True)
                tops[d] = m_new
    lane = lax.broadcasted_iota(jnp.int32, (16, 128), 1)
    for d in range(4):
        lcol[order[d]] = jnp.where(lane == 0, tops[d], totals[d])

    stat = lcol[...].reshape(rows, 128)
    mine = jnp.concatenate([stat, stat], axis=0).T[0:2]
    l_send[...] = mine
    for yy in ypeers:
        for xx in (x3, x2, x1, xi):
            send(l_send, l_recv.at[me], LSE, yy, xx)
    for xx in xpeers:
        send(l_send, l_recv.at[me], LSE, yi, xx)
    l_recv[me] = mine
    sent(s2_recv.at[three], S2)
    sent(fbuf.at[three], FN)
    sent(o_recv.at[:, most], O1)
    sent(bpart.at[:, three], B1)
    sent(lbuf, L1)
    recv(l_recv.at[most], LSE)
    tops = [l_recv[i, 0:1, :] for i in range(16)]
    top = functools.reduce(jnp.maximum, tops)
    total = sum([l_recv[i, 1:2, :] * jnp.exp(tops[i] - top) for i in range(16)])
    log_norm = top + jnp.log(total)
    lr_out[...] = log_norm[:, :rows]
    ln_out[...] = jnp.broadcast_to(log_norm, (128, 128)).T[:rows, 0:1]
    sent(l_recv.at[most], LSE)


def finish_kernel(own_rows, kv, z, ln, lr, k_out, v_out, lp_out, ln_out, k_s, v_s, lp_s, sem):
    k_s[...] = kv[0].astype(BF16)[:own_rows]
    v_s[...] = kv[1].astype(BF16)[:own_rows]
    copies = [pltpu.make_async_copy(k_s, k_out, sem.at[0]), pltpu.make_async_copy(v_s, v_out, sem.at[1]),
              pltpu.make_async_copy(lr, ln_out, sem.at[2])]
    for cp in copies:
        cp.start()
    for i in range(z.shape[0] // 8):
        at = pl.ds(i * 8, 8)
        lp_s[at] = z[at] - ln[at]
        copies.append(pltpu.make_async_copy(lp_s.at[at], lp_out.at[at], sem.at[3 + i]))
        copies[-1].start()
    for cp in copies:
        cp.wait()


def solution(mesh):
    row_spec = P(("dp", "yax", "xax"))

    def local_step(hidden, cache_len, k_cache, v_cache, g_attn, w_query, w_key, w_value,
                   w_gate, w_up, w_out, w_down, g_final, embedding):
        rows, wid = hidden.shape
        own_rows, seq, hd = k_cache.shape
        ffc = w_gate.shape[1] // 4
        vb = embedding.shape[0] // 4
        inv_freq = np.power(ROPE_BASE, -2.0 * np.arange(hd // 2) / hd).astype(np.float32).reshape(1, hd // 2)
        vbp = -(-vb // 128) * 128
        def cut(step, start=0):
            return [(c, min(step, vbp - c)) for c in range(start, vbp, step)]

        chunks_a = [(0, 512)] + cut(768, 512)
        chunks_b, chunks_c = cut(768), [(0, vbp)]
        nx, nc = len(chunks_a) + len(chunks_b), len(chunks_c)
        sizes = (rows, wid, seq, hd, ffc, vb, chunks_a, chunks_b, chunks_c)
        any_spec = pl.BlockSpec(memory_space=pltpu.HBM)
        vmem = pl.BlockSpec(memory_space=pltpu.VMEM)
        v = pltpu.VMEM
        dma = pltpu.SemaphoreType.DMA
        scratch = [
            v((rows, wid), BF16), v((1, 2 * wid + hd // 2), F32), v((2, 24, hd // 2), F32),
            *[v((seq, hd), BF16)] * 5, v((4, seq, hd), BF16),
            v((2, wid, 2 * hd), BF16), v((4, 2, wid, ffc), BF16),
            v((4 * ffc + 2 * hd, wid), BF16),
            v((8, 128), F32), v((4, 8, 128), F32), v((4, 24, 2 * hd), F32), v((4, 24, 2 * hd), F32),
            v((4, 16, 128), BF16), v((4, 16, 128), BF16), v((4, 8, hd), F32), v((8, hd), F32), v((8, hd), F32),
            v((4, 8, hd), F32), v((2, 8, seq), F32), v((2, 4, 8, 128), BF16), v((2, 16, 8, 128), BF16),
            v((4, 2, rows, ffc), F32), v((2, 2, rows, ffc), F32), v((2, rows, ffc), F32), v((2, rows, ffc), F32),
            v((4, rows, ffc), BF16), v((rows, wid), F32), v((16, wid), F32), v((2, 4, 8, wid), F32), v((2, 4, 8, wid), F32),
            v((16, 128), F32), v((4, 16, 128), F32), v((4, 16, wid), BF16),
            v((3, 4, 16, vbp), F32), v((4, 16, vbp), F32), v((4, 16, vbp), F32), v((1, 16, chunks_a[0][1]), F32),
            v((4, 16, vbp), F32), v((4, 16, vbp), F32), v((4, 16, 128), F32),
            v((2, 128), F32), v((16, 2, 128), F32),
            dma((12,)), dma((6,)), dma((14,)), dma((nx - 1,)), dma((nx,)), dma((nc,)), dma(()), pltpu.SemaphoreType.REGULAR, pltpu.SemaphoreType.REGULAR,
        ]
        kv, z, ln, lr = pl.pallas_call(
            functools.partial(step_kernel, sizes),
            name="decode_step",
            out_shape=(v((2, 8, hd), F32), v((rows, vb), F32), v((rows, 1), F32), v((1, rows), F32)),
            in_specs=[pl.BlockSpec(memory_space=pltpu.SMEM)] + [any_spec] * 14,
            out_specs=(vmem, vmem, vmem, vmem),
            scratch_shapes=scratch,
            compiler_params=pltpu.CompilerParams(collective_id=0, has_side_effects=True,
                                                 vmem_limit_bytes=67043328 - 900 * 1024),
        )(cache_len, hidden, jnp.asarray(inv_freq), k_cache, v_cache, g_attn.reshape(1, wid), w_query, w_key, w_value,
          w_gate, w_up, w_out, w_down, g_final.reshape(1, wid), embedding)
        k_new, v_new, log_probs, log_norm = pl.pallas_call(
            functools.partial(finish_kernel, own_rows),
            name="finish_step",
            out_shape=(jax.ShapeDtypeStruct((own_rows, hd), BF16), jax.ShapeDtypeStruct((own_rows, hd), BF16),
                       jax.ShapeDtypeStruct((rows, vb), F32), jax.ShapeDtypeStruct((1, rows), F32)),
            in_specs=[vmem] * 4,
            out_specs=(any_spec,) * 4,
            scratch_shapes=[v((own_rows, hd), BF16), v((own_rows, hd), BF16), v((rows, vb), F32), dma((11,))],
            compiler_params=pltpu.CompilerParams(vmem_limit_bytes=4 * 1024 * 1024),
        )(kv, z, ln, lr)
        return k_new, v_new, log_probs, log_norm[0]

    in_specs = (P("dp", "xax"), P("dp"), row_spec, row_spec, P("xax"), P("xax", "yax"),
                P("xax", None), P("xax", None), P("xax", "yax"), P("xax", "yax"),
                P("yax", "xax"), P("yax", "xax"), P("xax"), P("yax", "xax"))
    out_specs = (row_spec, row_spec, P("dp", ("yax", "xax")), P("dp"))
    return jax.shard_map(local_step, mesh=mesh, in_specs=in_specs, out_specs=out_specs, check_vma=False)
```

```python
import functools

import jax
import jax.numpy as jnp
import numpy as np
from jax import lax
from jax.experimental import pallas as pl
from jax.experimental.pallas import tpu as pltpu
from jax.sharding import PartitionSpec as P

EPS = 1e-6
ROPE_BASE = 10000.0
F32 = jnp.float32
BF16 = jnp.bfloat16
MESH = pl.DeviceIdType.MESH


def dot(a, b):
    return jnp.dot(a, b, preferred_element_type=F32)


def dot_t(a, b):
    return lax.dot_general(a, b, (((1,), (1,)), ((), ())), preferred_element_type=F32)


def one_hot_rows(rows, cols, source):
    r = lax.broadcasted_iota(jnp.int32, (rows, cols), 0)
    c = lax.broadcasted_iota(jnp.int32, (rows, cols), 1)
    return jnp.where(c == source(r), 1.0, 0.0).astype(BF16)


def step_kernel(sizes,
                lens, hidden_hbm, freq_hbm, k_hbm, v_hbm, ga_hbm, wq_hbm, wk_hbm, wv_hbm, wg_hbm, wu_hbm,
                wo_hbm, wd_hbm, gf_hbm, emb_hbm,
                kv_out, z_out, ln_out, lr_out,
                hid, small, table, kb0, kb1, kb2, kb3, kb4, vbuf, wqkv, wgu, wdo,
                st_send, st_recv, qkv, qkv_recv, q_send, q_recv, qs, kns, vns, os_, sbuf, o_send, o_recv,
                gup, gu_recv, gux, gux_recv, m_all, mdown, resid, bpart, b_recv, s2_send, s2_recv, fbuf,
                lbuf, lrecv1, xrecv, drecv, lrecv2, own, lcol, l_send, l_recv,
                ld_sem, snd_sem, rcv_sem, l1_sem, lx_sem, l2_sem, d_sem, x_ok, y_ok):
    rows, wid, seq, hd, ffc, vb, chunks_a, chunks_b, chunks_c = sizes
    yi = lax.axis_index("yax")
    xi = lax.axis_index("xax")
    x1 = xi + 1 - 2 * (xi % 2)
    x2 = (xi + 2) % 4
    x3 = (x1 + 2) % 4
    me = yi * 4 + xi
    ypeers = [3 * (1 - yi // 2), 2 - yi // 2, yi + 1 - 2 * (yi % 2)]
    xpeers = [x1, x2, x3]

    def load(i, *pairs):
        for src, dst in pairs:
            pltpu.make_async_copy(src, dst, ld_sem.at[i]).start()

    def loaded(i, dst):
        pltpu.make_async_copy(dst, dst, ld_sem.at[i]).wait()

    HID, SMALL, WQKV, WGU, WDO, KEY0, KEY1, KEY2, VAL0, VAL2, VAL3, EMB = range(12)
    ga, freq, gf = small.at[:, :wid], small.at[:, wid:wid + hd // 2], small.at[:, wid + hd // 2:]
    kb = (kb0, kb1, kb2, kb3, kb4)
    wd, wo = wdo.at[:4 * ffc], wdo.at[4 * ffc:]
    load(HID, (hidden_hbm, hid))
    load(SMALL, (ga_hbm, ga), (freq_hbm, freq), (gf_hbm, gf))
    barrier = pltpu.get_barrier_semaphore()
    odd = xi % 2 == 1
    even = xi % 2 == 0

    def signal(sem, yy, xx):
        pl.semaphore_signal(sem, inc=1, device_id={"yax": yy, "xax": xx}, device_id_type=MESH)

    @pl.when(odd)
    def _():
        signal(barrier, yi, x2)

    @pl.when(even)
    def _():
        signal(barrier, yi, x1)
        signal(barrier, yi, x3)

    load(WQKV, (wq_hbm, wqkv.at[0]), (wk_hbm, wqkv.at[1, :, :hd]), (wv_hbm, wqkv.at[1, :, hd:]))
    load(KEY0, (k_hbm.at[0], kb[1]))
    for i, xx in enumerate((x1, x3, x2, xi)):
        cols = pl.ds(pl.multiple_of(xx * ffc, ffc), ffc)
        load(WGU, (wg_hbm.at[:, cols], wgu.at[xx, 0]), (wu_hbm.at[:, cols], wgu.at[xx, 1]))
    load(KEY1, (k_hbm.at[1], kb[2]))
    load(KEY2, (k_hbm.at[2], kb[3]), (k_hbm.at[3], kb[4]))
    load(VAL0, (v_hbm.at[0], vbuf.at[0]), (v_hbm.at[1], vbuf.at[1]))
    load(VAL2, (v_hbm.at[2], vbuf.at[2]))
    load(VAL3, (v_hbm.at[3], vbuf.at[3]))
    load(WDO, (wd_hbm, wd), (wo_hbm, wo))

    ST, QP, KVP, Q, GU, GUX, M, O1, O2, B1, B2, S2, FN, LSE, L1, LX, L2 = range(17)

    snd = {ST: 0, S2: 0, QP: 1, KVP: 1, FN: 1, Q: 2, O1: 2, O2: 2, GU: 3, B1: 3, B2: 3, GUX: 4, LSE: 4, M: 5,
           L1: 5, LX: 5, L2: 5}

    def send(src, dst, i, yy, xx, rsem=None):
        pltpu.make_async_remote_copy(src_ref=src, dst_ref=dst, send_sem=snd_sem.at[snd[i]],
                                     recv_sem=rcv_sem.at[i] if rsem is None else rsem,
                                     device_id={"yax": yy, "xax": xx}, device_id_type=MESH).start()

    def recv(dst, i):
        pltpu.make_async_copy(dst, dst, rcv_sem.at[i]).wait()

    def recv_chunk(dst, sem):
        pltpu.make_async_copy(dst, dst, sem).wait()

    def sent(src, i):
        pltpu.make_async_copy(src, src, snd_sem.at[snd[i]]).wait()

    three = pl.ds(0, 3)
    most = pl.ds(0, 15)

    tq = seq // 1024

    def transpose_keys(j, start, stop):
        if start == 0 and j < 2:
            loaded((KEY0, KEY1)[j], kb[j + 1])
        elif start == 0 and j == 2:
            loaded(KEY2, vbuf.at[pl.ds(0, 2)])

        def one(t, carry):
            at = pl.ds(pl.multiple_of(t * 256, 256), 256)
            kb[j][at] = kb[j + 1][at].T
            return carry

        lax.fori_loop(start * tq, stop * tq, one, 0, unroll=tq)

    loaded(HID, hid)
    loaded(SMALL, small)
    h = hid[...].astype(F32)
    mean_l = jnp.sum(h, axis=1, keepdims=True) * (1.0 / wid)
    dev = h - mean_l
    m2_l = jnp.sum(dev * dev, axis=1, keepdims=True)
    lane = lax.broadcasted_iota(jnp.int32, (rows, 128), 1)
    stat = jnp.where(lane == 0, mean_l, m2_l)
    stat_t = jnp.concatenate([stat, stat], axis=0).T[:8]
    st_send[...] = stat_t

    @pl.when(odd)
    def _():
        pl.semaphore_wait(barrier, 3)
        signal(x_ok, yi, x1)

    @pl.when(even)
    def _():
        pl.semaphore_wait(x_ok, 1)
        for yy in ypeers:
            signal(barrier, yy, xi)

    for xx in xpeers:
        send(st_send, st_recv.at[xi], ST, yi, xx)
    perm = one_hot_rows(160, 64, lambda r: jnp.where(
        r >= 96, ((r % 32) // 2) * 4 + ((r - 96) // 32) * 2 + r % 2,
        jnp.where(r % 24 < 16, ((r % 24) // 4) * 16 + (r // 24) * 4 + r % 4,
                  jnp.where(r % 24 < 20, yi * 16 + (r // 24) * 4 + r % 4, -1))))
    prow = lax.broadcasted_iota(jnp.int32, (24, 128), 0)
    posn = jnp.zeros((24, 128), jnp.int32)
    for r in range(20):
        at = (r // 4) * 16 + xi * 4 + r % 4 if r < 16 else me * 4 + r - 16
        posn = jnp.where(prow == r, lens[at], posn)
    angle = posn.astype(F32) * freq[...]
    table[0] = jnp.cos(angle)
    table[1] = jnp.sin(angle)
    transpose_keys(0, 0, 2)
    recv(st_recv.at[three], ST)
    parts = [stat_t] + [st_recv[xx] for xx in xpeers]
    means = [p[0:1] for p in parts]
    mu = (means[0] + means[1] + means[2] + means[3]) * 0.25
    m2 = sum([p[1:2] for p in parts]) + wid * sum([(m - mu) * (m - mu) for m in means])
    rstd = lax.rsqrt(m2 * (1.0 / (4 * wid)) + EPS)
    sub = lax.broadcasted_iota(jnp.int32, (128, 128), 0)
    cols_t = jnp.where(sub == 0, mu, rstd).T
    mu_c = cols_t[:rows, 0:1]
    rstd_c = cols_t[:rows, 1:2]
    normed = ((h - mu_c) * rstd_c * ga[...]).astype(BF16)
    n_perm = dot(perm, normed).astype(BF16)

    loaded(WQKV, wqkv)
    n_qkv, n_pair = n_perm[:96], n_perm[96:]
    q_part = dot(n_qkv, wqkv[0])
    kv_part = dot(n_qkv, wqkv[1])
    prow = lax.broadcasted_iota(jnp.int32, (96, 2 * hd), 0)
    qkv[...] = jnp.where(prow % 24 < 16, q_part, kv_part).reshape(4, 24, 2 * hd)
    q_rows, kv_rows = pl.ds(0, 16), pl.ds(16, 8)
    for xx in (x2, x3, x1):
        send(qkv.at[xx, q_rows], qkv_recv.at[xi, q_rows], QP, yi, xx)
    for xx in (x2, x3, x1):
        send(qkv.at[xx, kv_rows], qkv_recv.at[xi, kv_rows], KVP, yi, xx)

    for i, xx in enumerate((x1, x3, x2, xi)):
        if i == 0:
            loaded(WGU, wgu)
        gup[xx, 0] = dot(n_pair, wgu[xx, 0])
        gup[xx, 1] = dot(n_pair, wgu[xx, 1])
        if i < 2:
            send(gup.at[xx], gu_recv.at[i], GU, yi, x1)

    transpose_keys(0, 2, 4)
    recv(gu_recv, GU)
    gux[...] = gup[x2] + gu_recv[1]
    send(gux, gux_recv, GUX, yi, x2)
    transpose_keys(1, 0, 4)
    transpose_keys(2, 0, 1)
    half = hd // 2
    recv(qkv_recv.at[three, q_rows], QP)

    def total(at):
        return ((qkv[xi, at] + qkv_recv[x1, at]) + (qkv_recv[x2, at] + qkv_recv[x3, at])).astype(BF16).astype(F32)

    def rotary(lo, hi, at):
        cos_a, sin_a = table[0, at], table[1, at]
        return (lo * cos_a - hi * sin_a).astype(BF16), (hi * cos_a + lo * sin_a).astype(BF16)

    tot = total(q_rows)
    lo0, hi0, lo1, hi1 = [tot[:, i * half:(i + 1) * half] for i in range(4)]
    r0, r1 = rotary(lo0, hi0, q_rows)
    r2, r3 = rotary(lo1, hi1, q_rows)
    stacked = jnp.concatenate([r0, r1, r2, r3], axis=0)
    s1 = one_hot_rows(64, 64, lambda r: ((r // 4) % 4) * 16 + (r // 16) * 4 + r % 4)
    q_send[...] = dot(s1, stacked).astype(BF16).reshape(4, 16, 128)

    @pl.when(even)
    def _():
        pl.semaphore_wait(barrier, 3)
        signal(y_ok, yi, x1)

    @pl.when(odd)
    def _():
        pl.semaphore_wait(y_ok, 1)

    for yy in ypeers:
        send(q_send.at[yy], q_recv.at[yi], Q, yy, xi)
    q_recv[yi] = q_send[yi]
    recv(qkv_recv.at[three, kv_rows], KVP)
    tot = total(kv_rows)
    r0, r1 = rotary(tot[:, :half], tot[:, half:hd], kv_rows)
    kns[:, :half] = r0.astype(F32)
    kns[:, half:] = r1.astype(F32)
    vns[...] = tot[:, hd:]
    kv_out[0] = kns[...]
    kv_out[1] = vns[...]

    transpose_keys(2, 1, 4)
    transpose_keys(3, 0, 4)
    recv(q_recv.at[three], Q)
    s2 = one_hot_rows(64, 64, lambda r: ((r // 2) % 4) * 16 + (r % 2) * 8 + (r // 32) * 4 + (r // 8) % 4)
    q_all = dot(s2, q_recv[...].reshape(64, 128))
    qs[...] = jnp.concatenate([q_all[:32], q_all[32:]], axis=1).reshape(4, 8, hd)

    scale = hd ** -0.5
    pos = lax.broadcasted_iota(jnp.int32, (8, seq), 1)

    def scores(j):
        qj = qs[j].astype(BF16)
        for t in range(seq // 256):
            at = pl.ds(t * 256, 256)
            sbuf[j % 2, :, at] = dot(qj, kb[j][at])

    def weights(j):
        s_new = jnp.sum(qs[j] * kns[j:j + 1, :], axis=1, keepdims=True) * scale
        s = jnp.where(pos < lens[me * 4 + j], sbuf[j % 2] * scale, -jnp.inf)
        top = jnp.maximum(jnp.max(s, axis=1, keepdims=True), s_new)
        w = jnp.exp(s - top)
        w_new = jnp.exp(s_new - top)
        inv = 1.0 / (jnp.sum(w, axis=1, keepdims=True) + w_new)
        return (w * inv).astype(BF16), (w_new * inv).astype(BF16).astype(F32)

    def mix(j, prob, p_new):
        hs = seq // 2
        acc = dot(prob[:, :hs], vbuf[j, :hs]) + dot(prob[:, hs:], vbuf[j, hs:])
        os_[j] = acc + p_new * vns[j:j + 1, :]

    s3 = one_hot_rows(32, 32, lambda r: ((r // 2) % 2) * 16 + (r % 2) * 8 + (r // 8) * 2 + (r // 4) % 2)

    sent(q_send.at[three], Q)
    sent(gu_recv, GU)
    sent(qkv.at[three], QP)

    def send_outputs(pair, i):
        o_bf = os_[2 * pair:2 * pair + 2].reshape(16, hd).astype(BF16)
        o_rows = dot(s3, jnp.concatenate([o_bf[:, :half], o_bf[:, half:]], axis=0))
        o_send[pair] = o_rows.reshape(4, 8, 128).astype(BF16)
        for yy in ypeers:
            for xx in (x3, x2, x1, xi):
                send(o_send.at[pair, yy], o_recv.at[pair, me], i, yy, xx)
        for xx in xpeers:
            send(o_send.at[pair, yi], o_recv.at[pair, me], i, yi, xx)
        o_recv[pair, me] = o_send[pair, yi]

    scores(0)
    scores(1)
    w0 = weights(0)
    loaded(VAL0, vbuf.at[pl.ds(0, 2)])
    mix(0, *w0)
    scores(2)
    mix(1, *weights(1))
    send_outputs(0, O1)
    recv(gux_recv, GUX)
    gu = gup[xi] + gu_recv[0] + gux_recv[...]
    gate = gu[0].astype(BF16).astype(F32)
    up_val = gu[1].astype(BF16).astype(F32)
    m_all[xi] = (gate * jax.nn.sigmoid(gate) * up_val).astype(BF16)
    for xx in (x2, x3, x1):
        send(m_all.at[xi], m_all.at[xi], M, yi, xx)
    loaded(VAL2, vbuf.at[2])
    loaded(VAL3, vbuf.at[3])
    scores(3)
    mix(2, *weights(2))
    w3 = weights(3)
    mix(3, *w3)
    send_outputs(1, O2)
    for j in range(4):
        voc = pl.ds(j * vb, vb)
        load(EMB, (emb_hbm.at[voc, pl.ds(0, hd)], vbuf.at[j, pl.ds(0, vb)]),
             (emb_hbm.at[voc, pl.ds(hd, hd)], vbuf.at[j, pl.ds(seq // 2, vb)]))
    s5 = one_hot_rows(16, 16, lambda r: ((r % 8) // 2) * 4 + (r // 8) * 2 + r % 2)
    resid[...] = dot(s5, hid[pl.ds(pl.multiple_of(yi * 16, 16), 16), :])
    loaded(WDO, wdo)
    recv(m_all.at[three], M)
    mdown[...] = sum([dot(m_all[i], wd[pl.ds(i * ffc, ffc)]) for i in range(4)])
    s4 = one_hot_rows(128, 128, lambda r: ((r % 32) // 2) * 8 + (r // 32) * 2 + r % 2)

    def products(pair, i):
        o_rows = jnp.concatenate([o_recv[pair, k].astype(F32) for k in range(16)], axis=0)
        a_all = dot(s4, o_rows.astype(BF16)).astype(BF16)
        attn = jnp.concatenate([a_all[k * 32:(k + 1) * 32] for k in range(4)], axis=1)
        bpart[pair] = (dot(attn, wo[...]) + mdown[pl.ds(pair * 32, 32)]).reshape(4, 8, wid)
        for yy in ypeers:
            send(bpart.at[pair, yy], b_recv.at[pair, yi], i, yy, xi)

    recv(o_recv.at[0, most], O1)
    products(0, B1)
    recv(o_recv.at[1, most], O2)
    products(1, B2)
    recv(b_recv.at[0, three], B1)
    recv(b_recv.at[1, three], B2)
    res = resid[...] + jnp.concatenate([
        (bpart[p, yi] + b_recv[p, ypeers[0]]) + (b_recv[p, ypeers[1]] + b_recv[p, ypeers[2]]) for p in range(2)], axis=0)

    mean_l = jnp.sum(res, axis=1, keepdims=True) * (1.0 / wid)
    dev = res - mean_l
    m2_l = jnp.sum(dev * dev, axis=1, keepdims=True)
    lane = lax.broadcasted_iota(jnp.int32, (16, 128), 1)
    s2_send[...] = jnp.where(lane < 64, mean_l, m2_l)
    sent(st_recv.at[three], ST)
    sent(gux, GUX)
    sent(m_all.at[three], M)
    for xx in xpeers:
        send(s2_send, s2_recv.at[xi], S2, yi, xx)
    recv(s2_recv.at[three], S2)
    parts = [s2_recv[xx] for xx in xpeers]
    means = [mean_l] + [p[:, 0:1] for p in parts]
    mu = (means[0] + means[1] + means[2] + means[3]) * 0.25
    m2 = m2_l + sum([p[:, 64:65] for p in parts]) + wid * sum([(m - mu) * (m - mu) for m in means])
    rstd = lax.rsqrt(m2 * (1.0 / (4 * wid)) + EPS)
    s6 = one_hot_rows(16, 16, lambda r: ((r // 2) % 2) * 8 + (r // 4) * 2 + r % 2)
    f_own = dot(s6, ((res - mu) * rstd * gf[...]).astype(BF16)).astype(BF16)
    fbuf[yi] = f_own
    for yy in ypeers:
        send(fbuf.at[yi], fbuf.at[yi], FN, yy, xi)
    loaded(EMB, vbuf.at[:, pl.ds(0, 2 * vb)])

    lsend1, hold, lsend2 = lbuf.at[0], lbuf.at[1], lbuf.at[2]

    def logit_part(f, xx, c0, cn):
        return dot_t(f[:, :hd], vbuf[xx, pl.ds(c0, cn)]) + dot_t(f[:, hd:], vbuf[xx, pl.ds(seq // 2 + c0, cn)])

    def cross(i, at):
        recv_chunk(lrecv1.at[at], l1_sem.at[i - 1])
        hold[at] = hold[at] + lrecv1[at]
        send(hold.at[at], xrecv.at[at], LX, yi, x2, lx_sem.at[i])

    def cross_blocks(f, slots, chunks, first):
        n = f.shape[0] // 16
        prev = None
        for i, (c0, cn) in enumerate(chunks):
            at = (slots, slice(None), pl.ds(c0, cn))
            if first + i == 0:
                hold[at] = logit_part(f, x2, c0, cn).reshape(n, 16, cn)
                send(hold.at[at], xrecv.at[at], LX, yi, x2, lx_sem.at[0])
                lsend1[at] = logit_part(f, x3, c0, cn).reshape(n, 16, cn)
                send(lsend1.at[at], drecv, L1, yi, x3, d_sem)
                continue
            lsend1[at] = logit_part(f, x3, c0, cn).reshape(n, 16, cn)
            send(lsend1.at[at], lrecv1.at[at], L1, yi, x1, l1_sem.at[first + i - 1])
            hold[at] = logit_part(f, x2, c0, cn).reshape(n, 16, cn)
            if prev is not None:
                cross(*prev)
            prev = (first + i, at)
        cross(*prev)

    slot_a = pl.ds(0, 1)
    slot_b = pl.ds(1, 3)
    na = len(chunks_a)
    cross_blocks(f_own, slot_a, chunks_a, 0)
    recv(fbuf.at[three], FN)
    f_rest = jnp.concatenate([fbuf[yy] for yy in ypeers], axis=0)
    cross_blocks(f_rest, slot_b, chunks_b, na)
    f_all = jnp.concatenate([f_own, f_rest], axis=0)
    for i, (c0, cn) in enumerate(chunks_c):
        at = (slice(None), slice(None), pl.ds(c0, cn))
        lsend2[at] = logit_part(f_all, x1, c0, cn).reshape(4, 16, cn)
        send(lsend2.at[at], lrecv2.at[at], L2, yi, x1, l2_sem.at[i])
        own[at] = logit_part(f_all, xi, c0, cn).reshape(4, 16, cn)
    recv_chunk(lrecv2, l2_sem.at[0]) if len(chunks_c) == 1 else [
        recv_chunk(lrecv2.at[:, :, pl.ds(c0, cn)], l2_sem.at[i]) for i, (c0, cn) in enumerate(chunks_c)]
    tops, totals = {}, {}
    order = [yi] + ypeers
    for d in range(4):
        tops[d] = jnp.full((16, 1), -jnp.inf, F32)
        totals[d] = jnp.zeros((16, 1), F32)
    for chunks, slots, ds, first in ((chunks_a, slot_a, (0,), 0), (chunks_b, slot_b, (1, 2, 3), na)):
        for i, (c0, cn) in enumerate(chunks):
            recv_chunk(xrecv.at[slots, :, pl.ds(c0, cn)], lx_sem.at[first + i])
            if first + i == 0:
                recv_chunk(drecv, d_sem)
            cs = pl.ds(c0, cn)
            for d in ds:
                row = pl.ds(pl.multiple_of(order[d] * 16, 16), 16)
                z = own[d, :, cs] + lrecv2[d, :, cs] + xrecv[d, :, cs]
                if first + i == 0:
                    z = z + drecv[0]
                if c0 + cn > vb:
                    z_out[row, c0:vb] = z[:, :vb - c0]
                    z = jnp.where(lax.broadcasted_iota(jnp.int32, (16, cn), 1) < vb - c0, z, -jnp.inf)
                else:
                    z_out[row, cs] = z
                m_new = jnp.maximum(tops[d], jnp.max(z, axis=1, keepdims=True))
                totals[d] = totals[d] * jnp.exp(tops[d] - m_new) + jnp.sum(jnp.exp(z - m_new), axis=1, keepdims=True)
                tops[d] = m_new
    lane = lax.broadcasted_iota(jnp.int32, (16, 128), 1)
    for d in range(4):
        lcol[order[d]] = jnp.where(lane == 0, tops[d], totals[d])

    stat = lcol[...].reshape(rows, 128)
    mine = jnp.concatenate([stat, stat], axis=0).T[0:2]
    l_send[...] = mine
    for yy in ypeers:
        for xx in (x3, x2, x1, xi):
            send(l_send, l_recv.at[me], LSE, yy, xx)
    for xx in xpeers:
        send(l_send, l_recv.at[me], LSE, yi, xx)
    l_recv[me] = mine
    sent(s2_recv.at[three], S2)
    sent(fbuf.at[three], FN)
    sent(o_recv.at[:, most], O1)
    sent(bpart.at[:, three], B1)
    sent(lbuf, L1)
    recv(l_recv.at[most], LSE)
    tops = [l_recv[i, 0:1, :] for i in range(16)]
    top = functools.reduce(jnp.maximum, tops)
    total = sum([l_recv[i, 1:2, :] * jnp.exp(tops[i] - top) for i in range(16)])
    log_norm = top + jnp.log(total)
    lr_out[...] = log_norm[:, :rows]
    ln_out[...] = jnp.broadcast_to(log_norm, (128, 128)).T[:rows, 0:1]
    sent(l_recv.at[most], LSE)


def finish_kernel(own_rows, kv, z, ln, lr, k_out, v_out, lp_out, ln_out, k_s, v_s, lp_s, sem):
    k_s[...] = kv[0].astype(BF16)[:own_rows]
    v_s[...] = kv[1].astype(BF16)[:own_rows]
    copies = [pltpu.make_async_copy(k_s, k_out, sem.at[0]), pltpu.make_async_copy(v_s, v_out, sem.at[1]),
              pltpu.make_async_copy(lr, ln_out, sem.at[2])]
    for cp in copies:
        cp.start()
    for i in range(z.shape[0] // 8):
        at = pl.ds(i * 8, 8)
        lp_s[at] = z[at] - ln[at]
        copies.append(pltpu.make_async_copy(lp_s.at[at], lp_out.at[at], sem.at[3 + i]))
        copies[-1].start()
    for cp in copies:
        cp.wait()


def solution(mesh):
    row_spec = P(("dp", "yax", "xax"))

    def local_step(hidden, cache_len, k_cache, v_cache, g_attn, w_query, w_key, w_value,
                   w_gate, w_up, w_out, w_down, g_final, embedding):
        rows, wid = hidden.shape
        own_rows, seq, hd = k_cache.shape
        ffc = w_gate.shape[1] // 4
        vb = embedding.shape[0] // 4
        inv_freq = np.power(ROPE_BASE, -2.0 * np.arange(hd // 2) / hd).astype(np.float32).reshape(1, hd // 2)
        vbp = -(-vb // 128) * 128
        def cut(step, start=0):
            return [(c, min(step, vbp - c)) for c in range(start, vbp, step)]

        chunks_a = [(0, 512)] + cut(768, 512)
        chunks_b, chunks_c = cut(768), [(0, vbp)]
        nx, nc = len(chunks_a) + len(chunks_b), len(chunks_c)
        sizes = (rows, wid, seq, hd, ffc, vb, chunks_a, chunks_b, chunks_c)
        any_spec = pl.BlockSpec(memory_space=pltpu.HBM)
        vmem = pl.BlockSpec(memory_space=pltpu.VMEM)
        v = pltpu.VMEM
        dma = pltpu.SemaphoreType.DMA
        scratch = [
            v((rows, wid), BF16), v((1, 2 * wid + hd // 2), F32), v((2, 24, hd // 2), F32),
            *[v((seq, hd), BF16)] * 5, v((4, seq, hd), BF16),
            v((2, wid, 2 * hd), BF16), v((4, 2, wid, ffc), BF16),
            v((4 * ffc + 2 * hd, wid), BF16),
            v((8, 128), F32), v((4, 8, 128), F32), v((4, 24, 2 * hd), F32), v((4, 24, 2 * hd), F32),
            v((4, 16, 128), BF16), v((4, 16, 128), BF16), v((4, 8, hd), F32), v((8, hd), F32), v((8, hd), F32),
            v((4, 8, hd), F32), v((2, 8, seq), F32), v((2, 4, 8, 128), BF16), v((2, 16, 8, 128), BF16),
            v((4, 2, rows, ffc), F32), v((2, 2, rows, ffc), F32), v((2, rows, ffc), F32), v((2, rows, ffc), F32),
            v((4, rows, ffc), BF16), v((rows, wid), F32), v((16, wid), F32), v((2, 4, 8, wid), F32), v((2, 4, 8, wid), F32),
            v((16, 128), F32), v((4, 16, 128), F32), v((4, 16, wid), BF16),
            v((3, 4, 16, vbp), F32), v((4, 16, vbp), F32), v((4, 16, vbp), F32), v((1, 16, chunks_a[0][1]), F32),
            v((4, 16, vbp), F32), v((4, 16, vbp), F32), v((4, 16, 128), F32),
            v((2, 128), F32), v((16, 2, 128), F32),
            dma((12,)), dma((6,)), dma((14,)), dma((nx - 1,)), dma((nx,)), dma((nc,)), dma(()), pltpu.SemaphoreType.REGULAR, pltpu.SemaphoreType.REGULAR,
        ]
        kv, z, ln, lr = pl.pallas_call(
            functools.partial(step_kernel, sizes),
            name="decode_step",
            out_shape=(v((2, 8, hd), F32), v((rows, vb), F32), v((rows, 1), F32), v((1, rows), F32)),
            in_specs=[pl.BlockSpec(memory_space=pltpu.SMEM)] + [any_spec] * 14,
            out_specs=(vmem, vmem, vmem, vmem),
            scratch_shapes=scratch,
            compiler_params=pltpu.CompilerParams(collective_id=0, has_side_effects=True,
                                                 vmem_limit_bytes=67043328 - 900 * 1024),
        )(cache_len, hidden, jnp.asarray(inv_freq), k_cache, v_cache, g_attn.reshape(1, wid), w_query, w_key, w_value,
          w_gate, w_up, w_out, w_down, g_final.reshape(1, wid), embedding)
        k_new, v_new, log_probs, log_norm = pl.pallas_call(
            functools.partial(finish_kernel, own_rows),
            name="finish_step",
            out_shape=(jax.ShapeDtypeStruct((own_rows, hd), BF16), jax.ShapeDtypeStruct((own_rows, hd), BF16),
                       jax.ShapeDtypeStruct((rows, vb), F32), jax.ShapeDtypeStruct((1, rows), F32)),
            in_specs=[vmem] * 4,
            out_specs=(any_spec,) * 4,
            scratch_shapes=[v((own_rows, hd), BF16), v((own_rows, hd), BF16), v((rows, vb), F32), dma((11,))],
            compiler_params=pltpu.CompilerParams(vmem_limit_bytes=4 * 1024 * 1024),
        )(kv, z, ln, lr)
        return k_new, v_new, log_probs, log_norm[0]

    in_specs = (P("dp", "xax"), P("dp"), row_spec, row_spec, P("xax"), P("xax", "yax"),
                P("xax", None), P("xax", None), P("xax", "yax"), P("xax", "yax"),
                P("yax", "xax"), P("yax", "xax"), P("xax"), P("yax", "xax"))
    out_specs = (row_spec, row_spec, P("dp", ("yax", "xax")), P("dp"))
    return jax.shard_map(local_step, mesh=mesh, in_specs=in_specs, out_specs=out_specs, check_vma=False)
```
